8 devices in a mesh: sp: 8 (over z, y, x, core).
Axes of the slice: x: 2, y: 2, z: 1, core: 2. Of those that a mesh axis runs over, the one named last changes fastest.
Arguments:
- x: bfloat16 [4096, 1024], P('sp')
- seg_ids: int32 [4096], P('sp')
- positions: int32 [4096], P('sp')
- grad_y: bfloat16 [4096, 1024], P('sp')
- norm1_gain: bfloat16 [1024], P('sp')
- w_q: bfloat16 [1024, 16, 64], P('sp')
- w_k: bfloat16 [1024, 16, 64], P('sp')
- w_v: bfloat16 [1024, 16, 64], P('sp')
- w_o: bfloat16 [16, 64, 1024], P('sp')
- norm2_gain: bfloat16 [1024], P('sp')
- w_gate: bfloat16 [1024, 2816], P('sp')
- w_up: bfloat16 [1024, 2816], P('sp')
- w_down: bfloat16 [2816, 1024], P('sp')
Outputs:
- output 1: bfloat16 [4096, 1024], P('sp')
- output 2: bfloat16 [4096, 1024], P('sp')
- output 3: float32 [1024], P('sp')
- output 4: float32 [1024, 16, 64], P('sp')
- output 5: float32 [1024, 16, 64], P('sp')
- output 6: float32 [1024, 16, 64], P('sp')
- output 7: float32 [16, 64, 1024], P('sp')
- output 8: float32 [1024], P('sp')
- output 9: float32 [1024, 2816], P('sp')
- output 10: float32 [1024, 2816], P('sp')
- output 11: float32 [2816, 1024], P('sp')
All inputs are finite; a program needn't handle non-finite values.
Results may differ from the reference program's by a relative error of at most 0.0158321.
Values are sent between devices in bfloat16 or wider.
A program may use at most 1 GiB of HBM per device.

```python
import jax
import jax.numpy as jnp
from jax import lax

D = 1024
HEADS = 16
KV_HEADS = 16
HEAD = 64
FF = 2816
SEQ = 4096
DOCS = 4
BLOCK = 256
NORM_EPS = 1e-5
ROPE_BASE = 10000.0
SCALE = HEAD ** -0.5


def doc_layout(key):
    cut_points = jax.random.permutation(key, SEQ - 1)[: DOCS - 1] + 1
    doc_starts = jnp.zeros((SEQ,), jnp.int32).at[cut_points].set(1)
    seg_ids = jnp.cumsum(doc_starts).astype(jnp.int32)
    tok_index = jnp.arange(SEQ, dtype=jnp.int32)
    first_index = lax.cummax(tok_index * doc_starts, axis=0)
    return seg_ids, (tok_index - first_index).astype(jnp.int32)


def normal_draw(key, shape, scale):
    return jax.random.normal(key, shape, jnp.float32) * scale


def setup_inputs(seed: int = 0) -> dict:
    keys = jax.random.split(jax.random.key(seed), 13)
    seg_ids, positions = doc_layout(keys[0])
    return {
        'x': normal_draw(keys[1], (SEQ, D), 1.0).astype(jnp.bfloat16),
        'seg_ids': seg_ids,
        'positions': positions,
        'grad_y': normal_draw(keys[2], (SEQ, D), 1.0).astype(jnp.bfloat16),
        'norm1_gain': (1.0 + normal_draw(keys[3], (D,), 0.5)).astype(jnp.bfloat16),
        'w_q': normal_draw(keys[4], (D, HEADS, HEAD), D ** -0.5).astype(jnp.bfloat16),
        'w_k': normal_draw(keys[5], (D, KV_HEADS, HEAD), D ** -0.5).astype(jnp.bfloat16),
        'w_v': normal_draw(keys[6], (D, KV_HEADS, HEAD), D ** -0.5).astype(jnp.bfloat16),
        'w_o': normal_draw(keys[7], (HEADS, HEAD, D), (HEADS * HEAD) ** -0.5).astype(jnp.bfloat16),
        'norm2_gain': (1.0 + normal_draw(keys[8], (D,), 0.5)).astype(jnp.bfloat16),
        'w_gate': normal_draw(keys[9], (D, FF), D ** -0.5).astype(jnp.bfloat16),
        'w_up': normal_draw(keys[10], (D, FF), D ** -0.5).astype(jnp.bfloat16),
        'w_down': normal_draw(keys[11], (FF, D), FF ** -0.5).astype(jnp.bfloat16),
    }


def to_bf16(t):
    return t.astype(jnp.bfloat16).astype(jnp.float32)


def rms_scale(t, gain):
    return t * lax.rsqrt(jnp.mean(t * t, axis=-1, keepdims=True) + NORM_EPS) * gain


def rope_tables(positions):
    half = HEAD // 2
    inv_freq = ROPE_BASE ** (-jnp.arange(half, dtype=jnp.float32) * 2.0 / HEAD)
    angle = positions.astype(jnp.float32)[:, None] * inv_freq[None, :]
    cos_t = jnp.cos(angle)
    sin_t = jnp.sin(angle)
    cos_full = jnp.concatenate([cos_t, cos_t], axis=-1)[:, None, :]
    sin_full = jnp.concatenate([sin_t, sin_t], axis=-1)[:, None, :]
    return cos_full, sin_full


def rotate(t, cos_full, sin_full):
    half = HEAD // 2
    return t * cos_full + jnp.concatenate([-t[..., half:], t[..., :half]], axis=-1) * sin_full


def head_attention(q_head, k_head, v_head, seg_ids):
    num_blocks = SEQ // BLOCK
    key_index = jnp.arange(SEQ)

    def one_block(block_args):
        q_block, block_id = block_args
        q_start = block_id * BLOCK
        q_index = q_start + jnp.arange(BLOCK)
        q_seg = lax.dynamic_slice(seg_ids, (q_start,), (BLOCK,))
        allowed = (key_index[None, :] <= q_index[:, None]) & (seg_ids[None, :] == q_seg[:, None])
        logits = jnp.dot(q_block, k_head.T, preferred_element_type=jnp.float32) * SCALE
        attn_probs = jax.nn.softmax(jnp.where(allowed, logits, -1e30), axis=-1)
        return to_bf16(jnp.dot(to_bf16(attn_probs), v_head, preferred_element_type=jnp.float32))

    attended = lax.map(jax.checkpoint(one_block), (q_head.reshape(num_blocks, BLOCK, HEAD), jnp.arange(num_blocks)))
    return attended.reshape(SEQ, HEAD)


def layer_forward(x_wide, seg_ids, positions, g_attn, w_q, w_k, w_v, w_o, g_mlp, w_gate, w_up, w_down):
    cos_full, sin_full = rope_tables(positions)
    u_norm = to_bf16(rms_scale(x_wide, g_attn))
    q_all = to_bf16(rotate(jnp.einsum('td,dhe->the', u_norm, w_q), cos_full, sin_full))
    k_all = to_bf16(rotate(jnp.einsum('td,dhe->the', u_norm, w_k), cos_full, sin_full))
    v_all = to_bf16(jnp.einsum('td,dhe->the', u_norm, w_v))
    group = HEADS // KV_HEADS
    k_rep = jnp.repeat(k_all, group, axis=1)
    v_rep = jnp.repeat(v_all, group, axis=1)
    attended = lax.map(lambda head_args: head_attention(head_args[0], head_args[1], head_args[2], seg_ids),
                       (q_all.transpose(1, 0, 2), k_rep.transpose(1, 0, 2), v_rep.transpose(1, 0, 2)))
    o_all = attended.transpose(1, 0, 2)
    h_res = to_bf16(x_wide + jnp.einsum('the,hed->td', o_all, w_o))
    z_norm = to_bf16(rms_scale(h_res, g_mlp))
    gate_pre = jnp.dot(z_norm, w_gate, preferred_element_type=jnp.float32)
    up_pre = jnp.dot(z_norm, w_up, preferred_element_type=jnp.float32)
    mlp_act = to_bf16(jax.nn.silu(gate_pre) * up_pre)
    return to_bf16(h_res + jnp.dot(mlp_act, w_down, preferred_element_type=jnp.float32))


def reference(x, seg_ids, positions, grad_y, norm1_gain, w_q, w_k, w_v, w_o, norm2_gain, w_gate, w_up, w_down):
    def forward(x_wide, g_attn, wq_full, wk_full, wv_full, wo_full, g_mlp, wgate_full, wup_full, wdown_full):
        return layer_forward(x_wide, seg_ids, positions, g_attn, wq_full, wk_full, wv_full, wo_full,
                             g_mlp, wgate_full, wup_full, wdown_full)

    primals = tuple(t.astype(jnp.float32) for t in (x, norm1_gain, w_q, w_k, w_v, w_o, norm2_gain, w_gate, w_up, w_down))
    y_out, pullback = jax.vjp(forward, *primals)
    grads = pullback(grad_y.astype(jnp.float32))
    return (y_out.astype(jnp.bfloat16), grads[0].astype(jnp.bfloat16), grads[1], grads[2], grads[3],
            grads[4], grads[5], grads[6], grads[7], grads[8], grads[9])
```

```python
import jax
import jax.numpy as jnp
from jax import lax
from jax.experimental import pallas as pl
from jax.experimental.pallas import tpu as pltpu
from jax.sharding import PartitionSpec as P

NORM_EPS = 1e-5
ROPE_BASE = 10000.0
SEQ = 4096
D = 1024
HD = 64
FF = 2816
NDEV = 8
TOK = SEQ // NDEV
LANES = 128
BQ = 256
BK = 512
NQ = SEQ // BQ
NEG = -1e30
F32 = jnp.float32
BF16 = jnp.bfloat16


def dot_nt(a, b):
    return lax.dot_general(a, b, (((1,), (1,)), ((), ())), preferred_element_type=F32)


def dot_tn(a, b):
    return lax.dot_general(a, b, (((0,), (0,)), ((), ())), preferred_element_type=F32)


def head_pair(t):
    lane = lax.broadcasted_iota(jnp.int32, (1, LANES), 1)
    low = (lane < HD).astype(F32).astype(BF16)
    high = (lane >= HD).astype(F32).astype(BF16)
    return jnp.concatenate([t * low, t * high], axis=0)


def rope_back_tile(t, cos_t, sin_t):
    lane = lax.broadcasted_iota(jnp.int32, t.shape, 1)
    first_half = lax.rem(lane, HD) < HD // 2
    rotated = jnp.where(first_half, -pltpu.roll(t, LANES - HD // 2, 1), pltpu.roll(t, HD // 2, 1))
    return t * cos_t - rotated * sin_t


def attn_fwd_kernel(lo_ref, start_ref, q_ref, k_ref, v_ref, o_ref, lse_ref, acc_ref):
    q_iota = lax.rem(lax.broadcasted_iota(jnp.int32, (1, 2 * BQ), 1), BQ)

    def q_block(i, _):
        q_start = pl.multiple_of(i * BQ, BQ)
        q2 = head_pair(q_ref[pl.ds(q_start, BQ), :])
        first = start_ref[pl.ds(i, 1), :]
        q_index = q_start + q_iota
        acc_ref[...] = jnp.zeros_like(acc_ref)

        def k_block(j, carry):
            m_old, l_old = carry
            k_start = pl.multiple_of(j * BK, BK)
            k = k_ref[pl.ds(k_start, BK), :]
            v = v_ref[pl.ds(k_start, BK), :]
            s = dot_nt(k, q2)
            k_index = k_start + lax.broadcasted_iota(jnp.int32, s.shape, 0)
            s = jnp.where((k_index >= first) & (k_index <= q_index), s, NEG)
            m_new = jnp.maximum(m_old, jnp.max(s, axis=0, keepdims=True))
            p = jnp.exp(s - m_new)
            alpha = jnp.exp(m_old - m_new)
            l_new = alpha * l_old + jnp.sum(p, axis=0, keepdims=True)
            acc_ref[...] = acc_ref[...] * alpha + dot_tn(v, p.astype(BF16))
            return m_new, l_new

        init = (jnp.full((1, 2 * BQ), NEG, F32), jnp.zeros((1, 2 * BQ), F32))
        m_fin, l_fin = lax.fori_loop(lo_ref[i], (q_start + BQ - 1) // BK + 1, k_block, init)
        lse_ref[pl.ds(i, 1), :] = m_fin + jnp.log(l_fin)
        out = acc_ref[...] * (1.0 / l_fin)
        out = jnp.concatenate([out[:HD, :BQ], out[HD:, BQ:]], axis=0)
        o_ref[pl.ds(q_start, BQ), :] = out.T.astype(BF16)
        return 0

    lax.fori_loop(0, NQ, q_block, 0)


def attn_bwd_kernel(lo_ref, start_ref, lse_ref, q_ref, k_ref, v_ref, o_ref, do_ref, cos_ref, sin_ref,
                    out_ref, dk_acc, dv_acc, dq_acc):
    q_iota = lax.rem(lax.broadcasted_iota(jnp.int32, (1, 2 * BQ), 1), BQ)
    dk_acc[...] = jnp.zeros_like(dk_acc)
    dv_acc[...] = jnp.zeros_like(dv_acc)

    def q_block(i, _):
        q_start = pl.multiple_of(i * BQ, BQ)
        q2 = head_pair(q_ref[pl.ds(q_start, BQ), :])
        do = do_ref[pl.ds(q_start, BQ), :]
        do2 = head_pair(do)
        prod = (do.astype(F32) * o_ref[pl.ds(q_start, BQ), :].astype(F32)).T
        delta = jnp.concatenate([jnp.sum(prod[:HD], axis=0, keepdims=True),
                                 jnp.sum(prod[HD:], axis=0, keepdims=True)], axis=1)
        first = start_ref[pl.ds(i, 1), :]
        lse = lse_ref[pl.ds(i, 1), :]
        q_index = q_start + q_iota
        dq_acc[...] = jnp.zeros_like(dq_acc)

        def k_block(j, _):
            k_start = pl.multiple_of(j * BK, BK)
            k = k_ref[pl.ds(k_start, BK), :]
            v = v_ref[pl.ds(k_start, BK), :]
            s = dot_nt(k, q2)
            k_index = k_start + lax.broadcasted_iota(jnp.int32, s.shape, 0)
            s = jnp.where((k_index >= first) & (k_index <= q_index), s, NEG)
            p = jnp.exp(s - lse)
            dp = dot_nt(v, do2).astype(BF16).astype(F32)
            ds = (p * (dp - delta)).astype(BF16)
            dv_acc[pl.ds(k_start, BK), :] += jnp.dot(p.astype(BF16), do2, preferred_element_type=F32)
            dk_acc[pl.ds(k_start, BK), :] += jnp.dot(ds, q2, preferred_element_type=F32)
            dq_acc[...] += dot_tn(k, ds)
            return 0

        lax.fori_loop(lo_ref[i], (q_start + BQ - 1) // BK + 1, k_block, 0)
        dq = jnp.concatenate([dq_acc[:HD, :BQ], dq_acc[HD:, BQ:]], axis=0).T * (HD ** -0.5)
        rows = pl.ds(q_start, BQ)
        dq = dq.astype(BF16).astype(F32)
        out_ref[rows, 0:LANES] = rope_back_tile(dq, cos_ref[rows, :], sin_ref[rows, :]).astype(BF16)
        return 0

    lax.fori_loop(0, NQ, q_block, 0)

    def finish(i, _):
        rows = pl.ds(pl.multiple_of(i * BQ, BQ), BQ)
        dk = dk_acc[rows, :].astype(BF16).astype(F32)
        out_ref[rows, LANES:2 * LANES] = rope_back_tile(dk, cos_ref[rows, :], sin_ref[rows, :]).astype(BF16)
        out_ref[rows, 2 * LANES:3 * LANES] = dv_acc[rows, :].astype(BF16)
        return 0

    lax.fori_loop(0, NQ, finish, 0)


VMEM_SPEC = pl.BlockSpec(memory_space=pltpu.VMEM)
SMEM_SPEC = pl.BlockSpec(memory_space=pltpu.SMEM)


def attn_forward(lo, start, q, k, v):
    return pl.pallas_call(
        attn_fwd_kernel,
        out_shape=(jax.ShapeDtypeStruct((SEQ, LANES), BF16), jax.ShapeDtypeStruct((NQ, 2 * BQ), F32)),
        in_specs=[SMEM_SPEC] + [VMEM_SPEC] * 4,
        out_specs=(VMEM_SPEC, VMEM_SPEC),
        scratch_shapes=[pltpu.VMEM((LANES, 2 * BQ), F32)],
        compiler_params=pltpu.CompilerParams(vmem_limit_bytes=40 * 1024 * 1024),
        cost_estimate=pl.CostEstimate(flops=20_000_000_000, bytes_accessed=5_000_000, transcendentals=20_000_000),
        name='attn_fwd',
    )(lo, start, q, k, v)


def attn_backward(lo, start, lse, q, k, v, o, do, cos_t, sin_t):
    return pl.pallas_call(
        attn_bwd_kernel,
        out_shape=jax.ShapeDtypeStruct((SEQ, 3 * LANES), BF16),
        in_specs=[SMEM_SPEC] + [VMEM_SPEC] * 9,
        out_specs=VMEM_SPEC,
        scratch_shapes=[pltpu.VMEM((SEQ, LANES), F32), pltpu.VMEM((SEQ, LANES), F32),
                        pltpu.VMEM((LANES, 2 * BQ), F32)],
        compiler_params=pltpu.CompilerParams(vmem_limit_bytes=48 * 1024 * 1024),
        cost_estimate=pl.CostEstimate(flops=50_000_000_000, bytes_accessed=12_000_000, transcendentals=20_000_000),
        name='attn_bwd',
    )(lo, start, lse, q, k, v, o, do, cos_t, sin_t)


def rms_back(grad_out, normed, inv_rms):
    mean_term = jnp.mean(grad_out * normed, axis=-1, keepdims=True)
    return inv_rms * (grad_out - normed * mean_term)


def rotate_columns(w):
    rows = w.shape[0]
    halves = w.reshape(rows, 2, 2, HD // 2)
    return jnp.concatenate([-halves[:, :, 1:], halves[:, :, :1]], axis=2).reshape(rows, LANES)


def solution(mesh):
    row_spec = P('sp', None)
    cube_spec = P('sp', None, None)
    vec_spec = P('sp')

    def gather(t):
        return lax.all_gather(t, 'sp', axis=0, tiled=True)

    def scatter_sum(t):
        return lax.psum_scatter(t, 'sp', scatter_dimension=0, tiled=True)

    def exchange(t):
        return lax.all_to_all(t, 'sp', 0, 0)

    def local_layer(x, seg_ids, positions, grad_y, norm1_gain, w_q, w_k, w_v, w_o, norm2_gain, w_gate, w_up, w_down):
        x_all = gather(x)
        small = jnp.concatenate([norm1_gain.astype(F32), norm2_gain.astype(F32), positions.astype(F32)])
        small = gather(small[None, :])
        gain1 = small[:, :128].reshape(D)
        gain2 = small[:, 128:256].reshape(D)
        pos_all = small[:, 256:].reshape(SEQ)
        start_all = jnp.arange(SEQ, dtype=jnp.int32) - pos_all.astype(jnp.int32)
        lo = start_all[::BQ] // BK
        start2 = start_all.reshape(NQ, BQ)
        start2 = jnp.concatenate([start2, start2], axis=1)

        half = HD // 2
        inv_freq = ROPE_BASE ** (-jnp.arange(half, dtype=F32) * 2.0 / HD)
        angle = pos_all[:, None] * jnp.tile(inv_freq, 4)[None, :]
        cos_t = jnp.cos(angle)
        sin_t = jnp.sin(angle)

        w_in = jnp.concatenate([t.reshape(LANES, NDEV, LANES) for t in (w_q, w_k, w_v)], axis=2)
        w_own = exchange(w_in.transpose(1, 0, 2)).reshape(D, 3 * LANES)
        w_q_own, w_k_own = w_own[:, :LANES], w_own[:, LANES:2 * LANES]
        w_ext = jnp.concatenate([w_own, rotate_columns(w_q_own), rotate_columns(w_k_own)], axis=1)

        xa = x_all.astype(F32)
        inv_all = lax.rsqrt(jnp.mean(xa * xa, axis=-1, keepdims=True) + NORM_EPS)
        u_all = (xa * inv_all * gain1).astype(BF16)
        proj = jnp.dot(u_all, w_ext, preferred_element_type=F32)
        q = (proj[:, :LANES] * cos_t + proj[:, 3 * LANES:4 * LANES] * sin_t).astype(BF16) * BF16(HD ** -0.5)
        k = (proj[:, LANES:2 * LANES] * cos_t + proj[:, 4 * LANES:] * sin_t).astype(BF16)
        v = proj[:, 2 * LANES:3 * LANES].astype(BF16)
        o_own, lse = attn_forward(lo, start2, q, k, v)
        o_loc = exchange(o_own.reshape(NDEV, TOK, LANES)).transpose(1, 0, 2).reshape(TOK, D)

        wo_full = gather(w_o.reshape(LANES, D))
        wgu_full = gather(jnp.concatenate([w_gate, w_up], axis=1))
        wd_full = gather(w_down)
        win_full = gather(w_in.reshape(LANES, 3 * D))

        x_wide = x.astype(F32)
        h_res = (x_wide + jnp.dot(o_loc, wo_full, preferred_element_type=F32)).astype(BF16)
        h_wide = h_res.astype(F32)
        inv_rms2 = lax.rsqrt(jnp.mean(h_wide * h_wide, axis=-1, keepdims=True) + NORM_EPS)
        normed2 = h_wide * inv_rms2
        z_norm = (normed2 * gain2).astype(BF16)
        gate_up = jnp.dot(z_norm, wgu_full, preferred_element_type=F32)
        gate_pre, up_pre = gate_up[:, :FF], gate_up[:, FF:]
        gate_sig = jax.nn.sigmoid(gate_pre)
        gate_act = gate_pre * gate_sig
        mlp_act = (gate_act * up_pre).astype(BF16)
        grad_wdown = scatter_sum(jnp.einsum('tf,td->fd', mlp_act, grad_y, preferred_element_type=F32))

        grad_act = dot_nt(grad_y, wd_full).astype(BF16).astype(F32)
        grad_gate = (grad_act * up_pre * gate_sig * (1.0 + gate_pre * (1.0 - gate_sig))).astype(BF16)
        grad_up = (grad_act * gate_act).astype(BF16)
        grad_gu = jnp.concatenate([grad_gate, grad_up], axis=1)
        grad_wgu = scatter_sum(dot_tn(z_norm, grad_gu))
        grad_z = dot_nt(grad_gu, wgu_full).astype(BF16).astype(F32)
        grad_gain2 = jnp.sum(grad_z * normed2, axis=0)
        grad_h = (grad_y.astype(F32) + rms_back(grad_z * gain2, normed2, inv_rms2)).astype(BF16)
        grad_o = dot_nt(grad_h, wo_full).astype(BF16)
        grad_o = exchange(grad_o.reshape(TOK, NDEV, LANES).transpose(1, 0, 2)).reshape(SEQ, LANES)
        grad_wo = scatter_sum(dot_tn(o_loc, grad_h))
        y = (h_wide + jnp.dot(mlp_act, wd_full, preferred_element_type=F32)).astype(BF16)

        d_qkv = attn_backward(lo, start2, lse, q, k, v, o_own, grad_o, cos_t, sin_t)
        d_loc = exchange(d_qkv.reshape(NDEV, TOK, 3 * LANES)).transpose(1, 0, 2).reshape(TOK, 3 * D)
        grad_win = exchange(dot_tn(u_all, d_qkv).reshape(NDEV, LANES, 3 * LANES))
        grad_u = dot_nt(d_loc, win_full).astype(BF16).astype(F32)
        inv_rms1 = lax.rsqrt(jnp.mean(x_wide * x_wide, axis=-1, keepdims=True) + NORM_EPS)
        normed1 = x_wide * inv_rms1
        grad_gain1 = jnp.sum(grad_u * normed1, axis=0)
        grad_x = (grad_h.astype(F32) + rms_back(grad_u * gain1, normed1, inv_rms1)).astype(BF16)
        grad_gains = scatter_sum(jnp.concatenate([grad_gain1.reshape(NDEV, 128), grad_gain2.reshape(NDEV, 128)], axis=1))
        grad_q, grad_k, grad_v = (grad_win[:, :, n * LANES:(n + 1) * LANES].transpose(1, 0, 2).reshape(LANES, 16, HD)
                                  for n in range(3))
        return (y, grad_x, grad_gains[0, :128], grad_q, grad_k, grad_v, grad_wo.reshape(2, HD, D),
                grad_gains[0, 128:], grad_wgu[:, :FF], grad_wgu[:, FF:], grad_wdown)

    return jax.shard_map(
        local_layer, mesh=mesh,
        in_specs=(row_spec, vec_spec, vec_spec, row_spec, vec_spec, cube_spec, cube_spec, cube_spec, cube_spec,
                  vec_spec, row_spec, row_spec, row_spec),
        out_specs=(row_spec, row_spec, vec_spec, cube_spec, cube_spec, cube_spec, cube_spec, vec_spec,
                   row_spec, row_spec, row_spec),
        check_vma=False)
```

```python
import jax
import jax.numpy as jnp
from jax import lax
from jax.experimental import pallas as pl
from jax.experimental.pallas import tpu as pltpu
from jax.sharding import PartitionSpec as P

NORM_EPS = 1e-5
ROPE_BASE = 10000.0
SEQ = 4096
D = 1024
HD = 64
FF = 2816
NDEV = 8
TOK = SEQ // NDEV
LANES = 128
BQ = 256
BK = 512
NQ = SEQ // BQ
NEG = -1e30
F32 = jnp.float32
BF16 = jnp.bfloat16


def dot_nt(a, b):
    return lax.dot_general(a, b, (((1,), (1,)), ((), ())), preferred_element_type=F32)


def dot_tn(a, b):
    return lax.dot_general(a, b, (((0,), (0,)), ((), ())), preferred_element_type=F32)


def head_pair(t):
    lane = lax.broadcasted_iota(jnp.int32, (1, LANES), 1)
    low = (lane < HD).astype(F32).astype(BF16)
    high = (lane >= HD).astype(F32).astype(BF16)
    return jnp.concatenate([t * low, t * high], axis=0)


def rope_back_tile(t, cos_t, sin_t):
    lane = lax.broadcasted_iota(jnp.int32, t.shape, 1)
    first_half = lax.rem(lane, HD) < HD // 2
    rotated = jnp.where(first_half, -pltpu.roll(t, LANES - HD // 2, 1), pltpu.roll(t, HD // 2, 1))
    return t * cos_t - rotated * sin_t


def attn_fwd_kernel(lo_ref, start_ref, q_ref, k_ref, v_ref, o_ref, lse_ref, acc_ref):
    q_iota = lax.rem(lax.broadcasted_iota(jnp.int32, (1, 2 * BQ), 1), BQ)

    def q_block(i, _):
        q_start = pl.multiple_of(i * BQ, BQ)
        q2 = head_pair(q_ref[pl.ds(q_start, BQ), :])
        first = start_ref[pl.ds(i, 1), :]
        q_index = q_start + q_iota
        acc_ref[...] = jnp.zeros_like(acc_ref)

        def k_block(j, carry):
            m_old, l_old = carry
            k_start = pl.multiple_of(j * BK, BK)
            k = k_ref[pl.ds(k_start, BK), :]
            v = v_ref[pl.ds(k_start, BK), :]
            s = dot_nt(k, q2)
            k_index = k_start + lax.broadcasted_iota(jnp.int32, s.shape, 0)
            s = jnp.where((k_index >= first) & (k_index <= q_index), s, NEG)
            m_new = jnp.maximum(m_old, jnp.max(s, axis=0, keepdims=True))
            p = jnp.exp(s - m_new)
            alpha = jnp.exp(m_old - m_new)
            l_new = alpha * l_old + jnp.sum(p, axis=0, keepdims=True)
            acc_ref[...] = acc_ref[...] * alpha + dot_tn(v, p.astype(BF16))
            return m_new, l_new

        init = (jnp.full((1, 2 * BQ), NEG, F32), jnp.zeros((1, 2 * BQ), F32))
        m_fin, l_fin = lax.fori_loop(lo_ref[i], (q_start + BQ - 1) // BK + 1, k_block, init)
        lse_ref[pl.ds(i, 1), :] = m_fin + jnp.log(l_fin)
        out = acc_ref[...] * (1.0 / l_fin)
        out = jnp.concatenate([out[:HD, :BQ], out[HD:, BQ:]], axis=0)
        o_ref[pl.ds(q_start, BQ), :] = out.T.astype(BF16)
        return 0

    lax.fori_loop(0, NQ, q_block, 0)


def attn_bwd_kernel(lo_ref, start_ref, lse_ref, q_ref, k_ref, v_ref, o_ref, do_ref, cos_ref, sin_ref,
                    out_ref, dk_acc, dv_acc, dq_acc):
    q_iota = lax.rem(lax.broadcasted_iota(jnp.int32, (1, 2 * BQ), 1), BQ)
    dk_acc[...] = jnp.zeros_like(dk_acc)
    dv_acc[...] = jnp.zeros_like(dv_acc)

    def q_block(i, _):
        q_start = pl.multiple_of(i * BQ, BQ)
        q2 = head_pair(q_ref[pl.ds(q_start, BQ), :])
        do = do_ref[pl.ds(q_start, BQ), :]
        do2 = head_pair(do)
        prod = (do.astype(F32) * o_ref[pl.ds(q_start, BQ), :].astype(F32)).T
        delta = jnp.concatenate([jnp.sum(prod[:HD], axis=0, keepdims=True),
                                 jnp.sum(prod[HD:], axis=0, keepdims=True)], axis=1)
        first = start_ref[pl.ds(i, 1), :]
        lse = lse_ref[pl.ds(i, 1), :]
        q_index = q_start + q_iota
        dq_acc[...] = jnp.zeros_like(dq_acc)

        def k_block(j, _):
            k_start = pl.multiple_of(j * BK, BK)
            k = k_ref[pl.ds(k_start, BK), :]
            v = v_ref[pl.ds(k_start, BK), :]
            s = dot_nt(k, q2)
            k_index = k_start + lax.broadcasted_iota(jnp.int32, s.shape, 0)
            s = jnp.where((k_index >= first) & (k_index <= q_index), s, NEG)
            p = jnp.exp(s - lse)
            dp = dot_nt(v, do2).astype(BF16).astype(F32)
            ds = (p * (dp - delta)).astype(BF16)
            dv_acc[pl.ds(k_start, BK), :] += jnp.dot(p.astype(BF16), do2, preferred_element_type=F32)
            dk_acc[pl.ds(k_start, BK), :] += jnp.dot(ds, q2, preferred_element_type=F32)
            dq_acc[...] += dot_tn(k, ds)
            return 0

        lax.fori_loop(lo_ref[i], (q_start + BQ - 1) // BK + 1, k_block, 0)
        dq = jnp.concatenate([dq_acc[:HD, :BQ], dq_acc[HD:, BQ:]], axis=0).T * (HD ** -0.5)
        rows = pl.ds(q_start, BQ)
        dq = dq.astype(BF16).astype(F32)
        out_ref[rows, 0:LANES] = rope_back_tile(dq, cos_ref[rows, :], sin_ref[rows, :]).astype(BF16)
        return 0

    lax.fori_loop(0, NQ, q_block, 0)

    def finish(i, _):
        rows = pl.ds(pl.multiple_of(i * BQ, BQ), BQ)
        dk = dk_acc[rows, :].astype(BF16).astype(F32)
        out_ref[rows, LANES:2 * LANES] = rope_back_tile(dk, cos_ref[rows, :], sin_ref[rows, :]).astype(BF16)
        out_ref[rows, 2 * LANES:3 * LANES] = dv_acc[rows, :].astype(BF16)
        return 0

    lax.fori_loop(0, NQ, finish, 0)


VMEM_SPEC = pl.BlockSpec(memory_space=pltpu.VMEM)
SMEM_SPEC = pl.BlockSpec(memory_space=pltpu.SMEM)


def attn_forward(lo, start, q, k, v):
    return pl.pallas_call(
        attn_fwd_kernel,
        out_shape=(jax.ShapeDtypeStruct((SEQ, LANES), BF16), jax.ShapeDtypeStruct((NQ, 2 * BQ), F32)),
        in_specs=[SMEM_SPEC] + [VMEM_SPEC] * 4,
        out_specs=(VMEM_SPEC, VMEM_SPEC),
        scratch_shapes=[pltpu.VMEM((LANES, 2 * BQ), F32)],
        compiler_params=pltpu.CompilerParams(vmem_limit_bytes=40 * 1024 * 1024),
        cost_estimate=pl.CostEstimate(flops=20_000_000_000, bytes_accessed=5_000_000, transcendentals=20_000_000),
        name='attn_fwd',
    )(lo, start, q, k, v)


def attn_backward(lo, start, lse, q, k, v, o, do, cos_t, sin_t):
    return pl.pallas_call(
        attn_bwd_kernel,
        out_shape=jax.ShapeDtypeStruct((SEQ, 3 * LANES), BF16),
        in_specs=[SMEM_SPEC] + [VMEM_SPEC] * 9,
        out_specs=VMEM_SPEC,
        scratch_shapes=[pltpu.VMEM((SEQ, LANES), F32), pltpu.VMEM((SEQ, LANES), F32),
                        pltpu.VMEM((LANES, 2 * BQ), F32)],
        compiler_params=pltpu.CompilerParams(vmem_limit_bytes=48 * 1024 * 1024),
        cost_estimate=pl.CostEstimate(flops=50_000_000_000, bytes_accessed=12_000_000, transcendentals=20_000_000),
        name='attn_bwd',
    )(lo, start, lse, q, k, v, o, do, cos_t, sin_t)


def head_kernel(x_ref, w_ref, small_ref, freq_ref, u_hbm, q_ref, k_ref, v_ref, cos_ref, sin_ref, all_small,
                x_buf, w_buf, w_ext, u_buf, small_send, small_recv, w_send, w_recv, x_send, x_recv, u_sem):
    me = lax.axis_index('sp')
    core = lax.rem(me, 2)
    x_pos = lax.rem(me // 2, 2)
    y_pos = me // 4
    step_c, step_x, step_y = 1 - 2 * core, 2 - 4 * x_pos, 4 - 8 * y_pos
    mate, near_x, near_y, diag = me + step_c, me + step_x, me + step_y, me + step_x + step_y

    barrier = pltpu.get_barrier_semaphore()
    for n in range(1, NDEV):
        pl.semaphore_signal(barrier, inc=1, device_id=(lax.rem(me + n, NDEV),), device_id_type=pl.DeviceIdType.MESH)
    pl.semaphore_wait(barrier, NDEV - 1)

    def remote(src, dst, send_sem, recv_sem, dev):
        return pltpu.make_async_remote_copy(src_ref=src, dst_ref=dst, send_sem=send_sem, recv_sem=recv_sem,
                                            device_id=(dev,), device_id_type=pl.DeviceIdType.MESH)

    def half(ref, h):
        return ref.at[pl.ds(h * (TOK // 2), TOK // 2), :]

    def x_copy(slot, src_dev, h, target, from_ref=None):
        source = half(x_buf.at[src_dev], h) if from_ref is None else half(from_ref, h)
        return remote(source, half(x_buf.at[src_dev], h), x_send.at[slot], x_recv.at[slot], target)

    smalls = [remote(small_ref, all_small.at[me], small_send.at[n - 1], small_recv.at[n - 1], lax.rem(me + n, NDEV))
              for n in range(1, NDEV)]
    weights = [remote(w_ref.at[lax.rem(me + n, NDEV)], w_buf.at[me], w_send.at[n - 1], w_recv.at[n - 1],
                      lax.rem(me + n, NDEV)) for n in range(1, NDEV)]
    for c in smalls:
        c.start()
    for c in weights:
        c.start()
    own = [x_copy(0, me, 0, near_x, x_ref), x_copy(3, me, 1, near_y, x_ref),
           x_copy(1, me, 1, near_x, x_ref), x_copy(2, me, 0, near_y, x_ref),
           x_copy(12, me, 0, mate, x_ref), x_copy(13, me, 1, mate, x_ref)]
    for c in own:
        c.start()

    all_small[me] = small_ref[...]
    w_buf[me] = w_ref[me]
    for c in smalls + weights:
        c.wait_recv()

    lane = lax.broadcasted_iota(jnp.int32, (LANES, LANES), 1)
    first_half = lax.rem(lane, HD) < HD // 2

    def build(i, _):
        rows = pl.ds(pl.multiple_of(i * LANES, LANES), LANES)
        w_ext[rows, 0:3 * LANES] = w_buf[i]
        for n in range(2):
            t = w_buf[i, :, n * LANES:(n + 1) * LANES].astype(F32)
            rot = jnp.where(first_half, -pltpu.roll(t, LANES - HD // 2, 1), pltpu.roll(t, HD // 2, 1))
            w_ext[rows, (3 + n) * LANES:(4 + n) * LANES] = rot.astype(BF16)
        return 0

    lax.fori_loop(0, NDEV, build, 0)
    gain1 = jnp.concatenate([all_small[n, 0:1, :] for n in range(NDEV)], axis=1)

    def process(order, src_ref, src_dev, h):
        def part(i, _):
            local = pl.ds(pl.multiple_of(h * (TOK // 2) + i * LANES, LANES), LANES)
            rows = pl.ds(pl.multiple_of(src_dev * TOK + h * (TOK // 2) + i * LANES, LANES), LANES)
            xv = src_ref[local, :].astype(F32)
            inv = lax.rsqrt(jnp.mean(xv * xv, axis=-1, keepdims=True) + NORM_EPS)
            u = (xv * inv * gain1).astype(BF16)
            u_buf[rows, :] = u
            proj = jnp.dot(u, w_ext[...], preferred_element_type=F32)
            angle = freq_ref[...] * all_small[src_dev, pl.ds(2 + 2 * h + i, 1), :]
            cos4, sin4 = jnp.cos(angle), jnp.sin(angle)
            cos_v = jnp.concatenate([cos4] * 4, axis=0).T
            sin_v = jnp.concatenate([sin4] * 4, axis=0).T
            cos_ref[rows, :] = cos_v
            sin_ref[rows, :] = sin_v
            q = (proj[:, :LANES] * cos_v + proj[:, 3 * LANES:4 * LANES] * sin_v).astype(BF16).astype(F32)
            q_ref[rows, :] = (q * (HD ** -0.5)).astype(BF16)
            k_ref[rows, :] = (proj[:, LANES:2 * LANES] * cos_v + proj[:, 4 * LANES:] * sin_v).astype(BF16)
            v_ref[rows, :] = proj[:, 2 * LANES:3 * LANES].astype(BF16)
            return 0

        lax.fori_loop(0, 2, part, 0)
        u_rows = pl.ds(pl.multiple_of(src_dev * TOK + h * (TOK // 2), TOK // 2), TOK // 2)
        out = pltpu.make_async_copy(u_buf.at[u_rows, :], u_hbm.at[u_rows, :], u_sem.at[order])
        out.start()
        return out

    pending = []
    copies = list(own)

    def arrive(slot, src_dev, h):
        x_copy(slot, src_dev, h, mate).wait_recv()

    def pass_on(slot, src_dev, h, target):
        c = x_copy(slot, src_dev, h, target)
        c.start()
        copies.append(c)

    def work(src_ref, src_dev, h):
        pending.append(process(len(pending), src_ref, src_dev, h))

    work(x_ref, me, 0)
    work(x_ref, me, 1)
    arrivals = [(0, near_x, 0, 5, 4), (3, near_y, 1, 5, 5), (1, near_x, 1, None, None), (2, near_y, 0, None, None),
                (4, diag, 0, None, None), (5, diag, 1, None, None)]
    late = [(12, mate, 0), (13, mate, 1)]
    for slot, src_dev, h, _, relay in arrivals:
        arrive(slot, src_dev, h)
        if relay == 4:
            pass_on(4, src_dev, h, near_y)
        elif relay == 5:
            pass_on(5, src_dev, h, near_x)
        pass_on(6 + slot, src_dev, h, mate)
        work(x_buf.at[src_dev], src_dev, h)
        mate_slot, mate_src, mate_h = late.pop(0)
        arrive(mate_slot, mate_src, mate_h)
        work(x_buf.at[mate_src], mate_src, mate_h)
        late.append((6 + slot, src_dev + step_c, h))
    for slot, src_dev, h in late:
        arrive(slot, src_dev, h)
        work(x_buf.at[src_dev], src_dev, h)
    for c in pending:
        c.wait()
    for c in smalls + weights + copies:
        c.wait_send()


def head_stage(x, w_pieces, small, freq):
    dma = pltpu.SemaphoreType.DMA
    return pl.pallas_call(
        head_kernel,
        out_shape=(jax.ShapeDtypeStruct((SEQ, D), BF16),) + tuple(jax.ShapeDtypeStruct((SEQ, LANES), BF16) for _ in range(3))
        + tuple(jax.ShapeDtypeStruct((SEQ, LANES), F32) for _ in range(2))
        + (jax.ShapeDtypeStruct((NDEV, 8, LANES), F32),),
        in_specs=[VMEM_SPEC] * 4,
        out_specs=(pl.BlockSpec(memory_space=pl.ANY),) + (VMEM_SPEC,) * 6,
        scratch_shapes=[pltpu.VMEM((NDEV, TOK, D), BF16), pltpu.VMEM((NDEV, LANES, 3 * LANES), BF16),
                        pltpu.VMEM((D, 5 * LANES), BF16), pltpu.VMEM((SEQ, D), BF16),
                        dma((NDEV - 1,)), dma((NDEV - 1,)), dma((NDEV - 1,)), dma((NDEV - 1,)),
                        dma((14,)), dma((14,)), dma((16,))],
        compiler_params=pltpu.CompilerParams(collective_id=0, has_side_effects=True,
                                             vmem_limit_bytes=48 * 1024 * 1024),
        cost_estimate=pl.CostEstimate(flops=40_000_000_000, bytes_accessed=30_000_000, transcendentals=1_000_000),
        name='head_stage',
    )(x, w_pieces, small, freq)


def rms_back(grad_out, normed, inv_rms):
    mean_term = jnp.mean(grad_out * normed, axis=-1, keepdims=True)
    return inv_rms * (grad_out - normed * mean_term)


def solution(mesh):
    row_spec = P('sp', None)
    cube_spec = P('sp', None, None)
    vec_spec = P('sp')

    def gather(t):
        return lax.all_gather(t, 'sp', axis=0, tiled=True)

    def scatter_sum(t):
        return lax.psum_scatter(t, 'sp', scatter_dimension=0, tiled=True)

    def exchange(t):
        return lax.all_to_all(t, 'sp', 0, 0)

    def local_layer(x, seg_ids, positions, grad_y, norm1_gain, w_q, w_k, w_v, w_o, norm2_gain, w_gate, w_up, w_down):
        half = HD // 2
        inv_freq = (ROPE_BASE ** (-jnp.arange(half, dtype=F32) * 2.0 / HD))[:, None]
        freq = jnp.broadcast_to(inv_freq, (half, LANES))
        small = jnp.concatenate([norm1_gain.astype(F32)[None, :], norm2_gain.astype(F32)[None, :],
                                 positions.astype(F32).reshape(4, LANES), jnp.zeros((2, LANES), F32)])
        w_in = jnp.concatenate([t.reshape(LANES, NDEV, LANES) for t in (w_q, w_k, w_v)], axis=2)
        u_all, q, k, v, cos_t, sin_t, small = head_stage(x, w_in.transpose(1, 0, 2), small, freq)
        gain1 = small[:, 0].reshape(D)
        gain2 = small[:, 1].reshape(D)
        start_all = jnp.arange(SEQ, dtype=jnp.int32) - small[:, 2:6].reshape(SEQ).astype(jnp.int32)
        lo = start_all[::BQ] // BK
        start2 = start_all.reshape(NQ, BQ)
        start2 = jnp.concatenate([start2, start2], axis=1)
        o_own, lse = attn_forward(lo, start2, q, k, v)
        o_loc = exchange(o_own.reshape(NDEV, TOK, LANES)).transpose(1, 0, 2).reshape(TOK, D)

        wo_full = gather(w_o.reshape(LANES, D))
        wgu_full = gather(jnp.concatenate([w_gate, w_up], axis=1))
        wd_full = gather(w_down)
        win_full = gather(w_in.reshape(LANES, 3 * D))

        x_wide = x.astype(F32)
        h_res = (x_wide + jnp.dot(o_loc, wo_full, preferred_element_type=F32)).astype(BF16)
        h_wide = h_res.astype(F32)
        inv_rms2 = lax.rsqrt(jnp.mean(h_wide * h_wide, axis=-1, keepdims=True) + NORM_EPS)
        normed2 = h_wide * inv_rms2
        z_norm = (normed2 * gain2).astype(BF16)
        gate_up = jnp.dot(z_norm, wgu_full, preferred_element_type=F32)
        gate_pre, up_pre = gate_up[:, :FF], gate_up[:, FF:]
        gate_sig = jax.nn.sigmoid(gate_pre)
        gate_act = gate_pre * gate_sig
        mlp_act = (gate_act * up_pre).astype(BF16)
        grad_wdown = scatter_sum(jnp.einsum('tf,td->fd', mlp_act, grad_y, preferred_element_type=F32))

        grad_act = dot_nt(grad_y, wd_full).astype(BF16).astype(F32)
        grad_gate = (grad_act * up_pre * gate_sig * (1.0 + gate_pre * (1.0 - gate_sig))).astype(BF16)
        grad_up = (grad_act * gate_act).astype(BF16)
        grad_gu = jnp.concatenate([grad_gate, grad_up], axis=1)
        grad_wgu = scatter_sum(dot_tn(z_norm, grad_gu))
        grad_z = dot_nt(grad_gu, wgu_full).astype(BF16).astype(F32)
        grad_gain2 = jnp.sum(grad_z * normed2, axis=0)
        grad_h = (grad_y.astype(F32) + rms_back(grad_z * gain2, normed2, inv_rms2)).astype(BF16)
        grad_o = dot_nt(grad_h, wo_full).astype(BF16)
        grad_o = exchange(grad_o.reshape(TOK, NDEV, LANES).transpose(1, 0, 2)).reshape(SEQ, LANES)
        grad_wo = scatter_sum(dot_tn(o_loc, grad_h))
        y = (h_wide + jnp.dot(mlp_act, wd_full, preferred_element_type=F32)).astype(BF16)

        d_qkv = attn_backward(lo, start2, lse, q, k, v, o_own, grad_o, cos_t, sin_t)
        d_loc = exchange(d_qkv.reshape(NDEV, TOK, 3 * LANES)).transpose(1, 0, 2).reshape(TOK, 3 * D)
        grad_win = exchange(dot_tn(u_all, d_qkv).reshape(NDEV, LANES, 3 * LANES))
        grad_u = dot_nt(d_loc, win_full).astype(BF16).astype(F32)
        inv_rms1 = lax.rsqrt(jnp.mean(x_wide * x_wide, axis=-1, keepdims=True) + NORM_EPS)
        normed1 = x_wide * inv_rms1
        grad_gain1 = jnp.sum(grad_u * normed1, axis=0)
        grad_x = (grad_h.astype(F32) + rms_back(grad_u * gain1, normed1, inv_rms1)).astype(BF16)
        grad_gains = scatter_sum(jnp.concatenate([grad_gain1.reshape(NDEV, 128), grad_gain2.reshape(NDEV, 128)], axis=1))
        grad_q, grad_k, grad_v = (grad_win[:, :, n * LANES:(n + 1) * LANES].transpose(1, 0, 2).reshape(LANES, 16, HD)
                                  for n in range(3))
        return (y, grad_x, grad_gains[0, :128], grad_q, grad_k, grad_v, grad_wo.reshape(2, HD, D),
                grad_gains[0, 128:], grad_wgu[:, :FF], grad_wgu[:, FF:], grad_wdown)

    return jax.shard_map(
        local_layer, mesh=mesh,
        in_specs=(row_spec, vec_spec, vec_spec, row_spec, vec_spec, cube_spec, cube_spec, cube_spec, cube_spec,
                  vec_spec, row_spec, row_spec, row_spec),
        out_specs=(row_spec, row_spec, vec_spec, cube_spec, cube_spec, cube_spec, cube_spec, vec_spec,
                   row_spec, row_spec, row_spec),
        check_vma=False)
```

```python
import jax
import jax.numpy as jnp
from jax import lax
from jax.experimental import pallas as pl
from jax.experimental.pallas import tpu as pltpu
from jax.sharding import PartitionSpec as P

NORM_EPS = 1e-5
ROPE_BASE = 10000.0
SEQ = 4096
D = 1024
HD = 64
FF = 2816
NDEV = 8
TOK = SEQ // NDEV
LANES = 128
BQ = 256
BK = 512
NQ = SEQ // BQ
NEG = -1e30
F32 = jnp.float32
BF16 = jnp.bfloat16


def dot_nt(a, b):
    return lax.dot_general(a, b, (((1,), (1,)), ((), ())), preferred_element_type=F32)


def dot_tn(a, b):
    return lax.dot_general(a, b, (((0,), (0,)), ((), ())), preferred_element_type=F32)


def head_pair(t):
    lane = lax.broadcasted_iota(jnp.int32, (1, LANES), 1)
    low = (lane < HD).astype(F32).astype(BF16)
    high = (lane >= HD).astype(F32).astype(BF16)
    return jnp.concatenate([t * low, t * high], axis=0)


def rope_back_tile(t, cos_t, sin_t):
    lane = lax.broadcasted_iota(jnp.int32, t.shape, 1)
    first_half = lax.rem(lane, HD) < HD // 2
    rotated = jnp.where(first_half, -pltpu.roll(t, LANES - HD // 2, 1), pltpu.roll(t, HD // 2, 1))
    return t * cos_t - rotated * sin_t


def attn_fwd_kernel(lo_ref, start_ref, q_ref, k_ref, v_ref, o_ref, lse_ref, acc_ref):
    q_iota = lax.rem(lax.broadcasted_iota(jnp.int32, (1, 2 * BQ), 1), BQ)

    def q_block(i, _):
        q_start = pl.multiple_of(i * BQ, BQ)
        q2 = head_pair(q_ref[pl.ds(q_start, BQ), :])
        first = start_ref[pl.ds(i, 1), :]
        q_index = q_start + q_iota
        acc_ref[...] = jnp.zeros_like(acc_ref)

        def k_block(j, carry):
            m_old, l_old = carry
            k_start = pl.multiple_of(j * BK, BK)
            k = k_ref[pl.ds(k_start, BK), :]
            v = v_ref[pl.ds(k_start, BK), :]
            s = dot_nt(k, q2)
            k_index = k_start + lax.broadcasted_iota(jnp.int32, s.shape, 0)
            s = jnp.where((k_index >= first) & (k_index <= q_index), s, NEG)
            m_new = jnp.maximum(m_old, jnp.max(s, axis=0, keepdims=True))
            p = jnp.exp(s - m_new)
            alpha = jnp.exp(m_old - m_new)
            l_new = alpha * l_old + jnp.sum(p, axis=0, keepdims=True)
            acc_ref[...] = acc_ref[...] * alpha + dot_tn(v, p.astype(BF16))
            return m_new, l_new

        init = (jnp.full((1, 2 * BQ), NEG, F32), jnp.zeros((1, 2 * BQ), F32))
        m_fin, l_fin = lax.fori_loop(lo_ref[i], (q_start + BQ - 1) // BK + 1, k_block, init)
        lse_ref[pl.ds(i, 1), :] = m_fin + jnp.log(l_fin)
        out = acc_ref[...] * (1.0 / l_fin)
        out = jnp.concatenate([out[:HD, :BQ], out[HD:, BQ:]], axis=0)
        o_ref[pl.ds(q_start, BQ), :] = out.T.astype(BF16)
        return 0

    lax.fori_loop(0, NQ, q_block, 0)


def attn_bwd_kernel(lo_ref, start_ref, lse_ref, q_ref, k_ref, v_ref, o_ref, do_ref, cos_ref, sin_ref,
                    out_ref, dk_acc, dv_acc, dq_acc):
    q_iota = lax.rem(lax.broadcasted_iota(jnp.int32, (1, 2 * BQ), 1), BQ)
    dk_acc[...] = jnp.zeros_like(dk_acc)
    dv_acc[...] = jnp.zeros_like(dv_acc)

    def q_block(i, _):
        q_start = pl.multiple_of(i * BQ, BQ)
        q2 = head_pair(q_ref[pl.ds(q_start, BQ), :])
        do = do_ref[pl.ds(q_start, BQ), :]
        do2 = head_pair(do)
        prod = (do.astype(F32) * o_ref[pl.ds(q_start, BQ), :].astype(F32)).T
        delta = jnp.concatenate([jnp.sum(prod[:HD], axis=0, keepdims=True),
                                 jnp.sum(prod[HD:], axis=0, keepdims=True)], axis=1)
        first = start_ref[pl.ds(i, 1), :]
        lse = lse_ref[pl.ds(i, 1), :]
        q_index = q_start + q_iota
        dq_acc[...] = jnp.zeros_like(dq_acc)

        def k_block(j, _):
            k_start = pl.multiple_of(j * BK, BK)
            k = k_ref[pl.ds(k_start, BK), :]
            v = v_ref[pl.ds(k_start, BK), :]
            s = dot_nt(k, q2)
            k_index = k_start + lax.broadcasted_iota(jnp.int32, s.shape, 0)
            s = jnp.where((k_index >= first) & (k_index <= q_index), s, NEG)
            p = jnp.exp(s - lse)
            dp = dot_nt(v, do2).astype(BF16).astype(F32)
            ds = (p * (dp - delta)).astype(BF16)
            dv_acc[pl.ds(k_start, BK), :] += jnp.dot(p.astype(BF16), do2, preferred_element_type=F32)
            dk_acc[pl.ds(k_start, BK), :] += jnp.dot(ds, q2, preferred_element_type=F32)
            dq_acc[...] += dot_tn(k, ds)
            return 0

        lax.fori_loop(lo_ref[i], (q_start + BQ - 1) // BK + 1, k_block, 0)
        dq = jnp.concatenate([dq_acc[:HD, :BQ], dq_acc[HD:, BQ:]], axis=0).T * (HD ** -0.5)
        rows = pl.ds(q_start, BQ)
        dq = dq.astype(BF16).astype(F32)
        out_ref[rows, 0:LANES] = rope_back_tile(dq, cos_ref[rows, :], sin_ref[rows, :]).astype(BF16)
        return 0

    lax.fori_loop(0, NQ, q_block, 0)

    def finish(i, _):
        rows = pl.ds(pl.multiple_of(i * BQ, BQ), BQ)
        dk = dk_acc[rows, :].astype(BF16).astype(F32)
        out_ref[rows, LANES:2 * LANES] = rope_back_tile(dk, cos_ref[rows, :], sin_ref[rows, :]).astype(BF16)
        out_ref[rows, 2 * LANES:3 * LANES] = dv_acc[rows, :].astype(BF16)
        return 0

    lax.fori_loop(0, NQ, finish, 0)


VMEM_SPEC = pl.BlockSpec(memory_space=pltpu.VMEM)
SMEM_SPEC = pl.BlockSpec(memory_space=pltpu.SMEM)


def attn_forward(lo, start, q, k, v):
    return pl.pallas_call(
        attn_fwd_kernel,
        out_shape=(jax.ShapeDtypeStruct((SEQ, LANES), BF16), jax.ShapeDtypeStruct((NQ, 2 * BQ), F32)),
        in_specs=[SMEM_SPEC] + [VMEM_SPEC] * 4,
        out_specs=(VMEM_SPEC, VMEM_SPEC),
        scratch_shapes=[pltpu.VMEM((LANES, 2 * BQ), F32)],
        compiler_params=pltpu.CompilerParams(vmem_limit_bytes=40 * 1024 * 1024),
        cost_estimate=pl.CostEstimate(flops=20_000_000_000, bytes_accessed=5_000_000, transcendentals=20_000_000),
        name='attn_fwd',
    )(lo, start, q, k, v)


def attn_backward(lo, start, lse, q, k, v, o, do, cos_t, sin_t):
    return pl.pallas_call(
        attn_bwd_kernel,
        out_shape=jax.ShapeDtypeStruct((SEQ, 3 * LANES), BF16),
        in_specs=[SMEM_SPEC] + [VMEM_SPEC] * 9,
        out_specs=VMEM_SPEC,
        scratch_shapes=[pltpu.VMEM((SEQ, LANES), F32), pltpu.VMEM((SEQ, LANES), F32),
                        pltpu.VMEM((LANES, 2 * BQ), F32)],
        compiler_params=pltpu.CompilerParams(vmem_limit_bytes=48 * 1024 * 1024),
        cost_estimate=pl.CostEstimate(flops=50_000_000_000, bytes_accessed=12_000_000, transcendentals=20_000_000),
        name='attn_bwd',
    )(lo, start, lse, q, k, v, o, do, cos_t, sin_t)


def head_kernel(x_ref, w_ref, small_ref, freq_ref, u_hbm, q_ref, k_ref, v_ref, cos_ref, sin_ref, all_small,
                x_buf, w_buf, w_ext, u_buf, small_send, small_recv, w_send, w_recv, x_send, x_recv, u_sem):
    me = lax.axis_index('sp')
    core = lax.rem(me, 2)
    x_pos = lax.rem(me // 2, 2)
    y_pos = me // 4
    step_c, step_x, step_y = 1 - 2 * core, 2 - 4 * x_pos, 4 - 8 * y_pos
    mate, near_x, near_y, diag = me + step_c, me + step_x, me + step_y, me + step_x + step_y

    barrier = pltpu.get_barrier_semaphore()
    for n in range(1, NDEV):
        pl.semaphore_signal(barrier, inc=1, device_id=(lax.rem(me + n, NDEV),), device_id_type=pl.DeviceIdType.MESH)
    pl.semaphore_wait(barrier, NDEV - 1)

    def remote(src, dst, send_sem, recv_sem, dev):
        return pltpu.make_async_remote_copy(src_ref=src, dst_ref=dst, send_sem=send_sem, recv_sem=recv_sem,
                                            device_id=(dev,), device_id_type=pl.DeviceIdType.MESH)

    def half(ref, h):
        return ref.at[pl.ds(h * (TOK // 2), TOK // 2), :]

    def x_copy(slot, src_dev, h, target, from_ref=None):
        source = half(x_buf.at[src_dev], h) if from_ref is None else half(from_ref, h)
        return remote(source, half(x_buf.at[src_dev], h), x_send.at[slot], x_recv.at[slot], target)

    smalls = [remote(small_ref, all_small.at[me], small_send.at[n - 1], small_recv.at[n - 1], lax.rem(me + n, NDEV))
              for n in range(1, NDEV)]
    weights = [remote(w_ref.at[lax.rem(me + n, NDEV)], w_buf.at[me], w_send.at[n - 1], w_recv.at[n - 1],
                      lax.rem(me + n, NDEV)) for n in range(1, NDEV)]
    for c in smalls:
        c.start()
    for c in weights:
        c.start()
    own = [x_copy(0, me, 0, near_x, x_ref), x_copy(3, me, 1, near_y, x_ref),
           x_copy(1, me, 1, near_x, x_ref), x_copy(2, me, 0, near_y, x_ref),
           x_copy(12, me, 0, mate, x_ref), x_copy(13, me, 1, mate, x_ref)]
    for c in own:
        c.start()

    all_small[me] = small_ref[...]
    w_buf[me] = w_ref[me]
    for c in smalls + weights:
        c.wait_recv()

    lane = lax.broadcasted_iota(jnp.int32, (LANES, LANES), 1)
    first_half = lax.rem(lane, HD) < HD // 2

    def build(i, _):
        rows = pl.ds(pl.multiple_of(i * LANES, LANES), LANES)
        w_ext[rows, 0:3 * LANES] = w_buf[i]
        for n in range(2):
            t = w_buf[i, :, n * LANES:(n + 1) * LANES].astype(F32)
            rot = jnp.where(first_half, -pltpu.roll(t, LANES - HD // 2, 1), pltpu.roll(t, HD // 2, 1))
            w_ext[rows, (3 + n) * LANES:(4 + n) * LANES] = rot.astype(BF16)
        return 0

    lax.fori_loop(0, NDEV, build, 0)
    gain1 = jnp.concatenate([all_small[n, 0:1, :] for n in range(NDEV)], axis=1)

    def process(order, src_ref, src_dev, h):
        def part(i, _):
            local = pl.ds(pl.multiple_of(h * (TOK // 2) + i * LANES, LANES), LANES)
            rows = pl.ds(pl.multiple_of(src_dev * TOK + h * (TOK // 2) + i * LANES, LANES), LANES)
            xv = src_ref[local, :].astype(F32)
            inv = lax.rsqrt(jnp.mean(xv * xv, axis=-1, keepdims=True) + NORM_EPS)
            u = (xv * inv * gain1).astype(BF16)
            u_buf[rows, :] = u
            proj = jnp.dot(u, w_ext[...], preferred_element_type=F32)
            angle = freq_ref[...] * all_small[src_dev, pl.ds(2 + 2 * h + i, 1), :]
            cos4, sin4 = jnp.cos(angle), jnp.sin(angle)
            cos_v = jnp.concatenate([cos4] * 4, axis=0).T
            sin_v = jnp.concatenate([sin4] * 4, axis=0).T
            cos_ref[rows, :] = cos_v
            sin_ref[rows, :] = sin_v
            q = (proj[:, :LANES] * cos_v + proj[:, 3 * LANES:4 * LANES] * sin_v).astype(BF16).astype(F32)
            q_ref[rows, :] = (q * (HD ** -0.5)).astype(BF16)
            k_ref[rows, :] = (proj[:, LANES:2 * LANES] * cos_v + proj[:, 4 * LANES:] * sin_v).astype(BF16)
            v_ref[rows, :] = proj[:, 2 * LANES:3 * LANES].astype(BF16)
            return 0

        lax.fori_loop(0, 2, part, 0)
        u_rows = pl.ds(pl.multiple_of(src_dev * TOK + h * (TOK // 2), TOK // 2), TOK // 2)
        out = pltpu.make_async_copy(u_buf.at[u_rows, :], u_hbm.at[u_rows, :], u_sem.at[order])
        out.start()
        return out

    pending = []
    copies = list(own)

    def arrive(slot, src_dev, h):
        x_copy(slot, src_dev, h, mate).wait_recv()

    def pass_on(slot, src_dev, h, target):
        c = x_copy(slot, src_dev, h, target)
        c.start()
        copies.append(c)

    def work(src_ref, src_dev, h):
        pending.append(process(len(pending), src_ref, src_dev, h))

    work(x_ref, me, 0)
    work(x_ref, me, 1)
    arrivals = [(0, near_x, 0, 5, 4), (3, near_y, 1, 5, 5), (1, near_x, 1, None, None), (2, near_y, 0, None, None),
                (4, diag, 0, None, None), (5, diag, 1, None, None)]
    late = [(12, mate, 0), (13, mate, 1)]
    for slot, src_dev, h, _, relay in arrivals:
        arrive(slot, src_dev, h)
        if relay == 4:
            pass_on(4, src_dev, h, near_y)
        elif relay == 5:
            pass_on(5, src_dev, h, near_x)
        pass_on(6 + slot, src_dev, h, mate)
        work(x_buf.at[src_dev], src_dev, h)
        mate_slot, mate_src, mate_h = late.pop(0)
        arrive(mate_slot, mate_src, mate_h)
        work(x_buf.at[mate_src], mate_src, mate_h)
        late.append((6 + slot, src_dev + step_c, h))
    for slot, src_dev, h in late:
        arrive(slot, src_dev, h)
        work(x_buf.at[src_dev], src_dev, h)
    for c in pending:
        c.wait()
    for c in smalls + weights + copies:
        c.wait_send()


def head_stage(x, w_pieces, small, freq):
    dma = pltpu.SemaphoreType.DMA
    return pl.pallas_call(
        head_kernel,
        out_shape=(jax.ShapeDtypeStruct((SEQ, D), BF16),) + tuple(jax.ShapeDtypeStruct((SEQ, LANES), BF16) for _ in range(3))
        + tuple(jax.ShapeDtypeStruct((SEQ, LANES), F32) for _ in range(2))
        + (jax.ShapeDtypeStruct((NDEV, 8, LANES), F32),),
        in_specs=[VMEM_SPEC] * 4,
        out_specs=(pl.BlockSpec(memory_space=pl.ANY),) + (VMEM_SPEC,) * 6,
        scratch_shapes=[pltpu.VMEM((NDEV, TOK, D), BF16), pltpu.VMEM((NDEV, LANES, 3 * LANES), BF16),
                        pltpu.VMEM((D, 5 * LANES), BF16), pltpu.VMEM((SEQ, D), BF16),
                        dma((NDEV - 1,)), dma((NDEV - 1,)), dma((NDEV - 1,)), dma((NDEV - 1,)),
                        dma((14,)), dma((14,)), dma((16,))],
        compiler_params=pltpu.CompilerParams(collective_id=0, has_side_effects=True,
                                             vmem_limit_bytes=48 * 1024 * 1024),
        cost_estimate=pl.CostEstimate(flops=40_000_000_000, bytes_accessed=30_000_000, transcendentals=1_000_000),
        name='head_stage',
    )(x, w_pieces, small, freq)


COLS = D // 2
DN_ROWS = FF // NDEV
OUT_ROWS = DN_ROWS + LANES


def tail_kernel(mt_ref, gy_ref, ot_ref, gh_ref, gw_ref, d_ref, x_ref, gain_ref, gg2_ref, win_hbm,
                dn_out, wo_out, gw_out, gx_out, gain_out,
                mt_mate, gy_mate, ot_mate, gh_mate, part, box, d_buf, win_buf, gain_mine, gain_buf,
                mate_send, mate_recv, rs_send, rs_recv, d_send, d_recv, gw_send, gw_recv, gg_send, gg_recv, win_sem):
    me = lax.axis_index('sp')
    core = lax.rem(me, 2)
    x_pos = lax.rem(me // 2, 2)
    y_pos = me // 4
    step_c, step_x, step_y = 1 - 2 * core, 2 - 4 * x_pos, 4 - 8 * y_pos
    mate, near_x, near_y, diag = me + step_c, me + step_x, me + step_y, me + step_x + step_y

    win_copy = pltpu.make_async_copy(win_hbm, win_buf, win_sem)
    win_copy.start()

    barrier = pltpu.get_barrier_semaphore()
    for n in range(1, NDEV):
        pl.semaphore_signal(barrier, inc=1, device_id=(lax.rem(me + n, NDEV),), device_id_type=pl.DeviceIdType.MESH)
    pl.semaphore_wait(barrier, NDEV - 1)

    def remote(src, dst, send_sem, recv_sem, dev):
        return pltpu.make_async_remote_copy(src_ref=src, dst_ref=dst, send_sem=send_sem, recv_sem=recv_sem,
                                            device_id=(dev,), device_id_type=pl.DeviceIdType.MESH)

    def to_peers(src, dst, send_sem, recv_sem):
        return [remote(src.at[lax.rem(me + n, NDEV)], dst.at[me], send_sem.at[n - 1], recv_sem.at[n - 1],
                       lax.rem(me + n, NDEV)) for n in range(1, NDEV)]

    def dn_rows(dev):
        return pl.ds(pl.multiple_of(dev * DN_ROWS, 32), DN_ROWS)

    def wo_rows(dev):
        return pl.ds(pl.multiple_of(dev * LANES, LANES), LANES)

    swaps = []
    for q in range(NDEV // 2):
        dest = 2 * q + 1 - core
        swaps.append(remote(mt_ref.at[dn_rows(dest), :], mt_mate.at[q], mate_send.at[q], mate_recv.at[q], mate))
        swaps.append(remote(ot_ref.at[wo_rows(dest), :], ot_mate.at[q], mate_send.at[4 + q], mate_recv.at[4 + q], mate))
    swaps.append(remote(gy_ref, gy_mate, mate_send.at[8], mate_recv.at[8], mate))
    swaps.append(remote(gh_ref, gh_mate, mate_send.at[9], mate_recv.at[9], mate))
    for c in swaps:
        c.start()
    d_moves = to_peers(d_ref, d_buf, d_send, d_recv)
    gw_moves = to_peers(gw_ref, gw_out, gw_send, gw_recv)
    gg_moves = to_peers(gain_mine, gain_buf, gg_send, gg_recv)
    for c in d_moves:
        c.start()
    d_buf[me] = d_ref[me]
    gw_out[me] = gw_ref[me]
    for c in swaps:
        c.wait_recv()

    def compute(rel, dev, col):
        chip = dev // 2
        cols = pl.ds(col * COLS, COLS)
        part[rel, col, 0:DN_ROWS, :] = (
            jnp.dot(mt_ref[dn_rows(dev), :], gy_ref[:, cols], preferred_element_type=F32)
            + jnp.dot(mt_mate[chip], gy_mate[:, cols], preferred_element_type=F32))
        part[rel, col, DN_ROWS:OUT_ROWS, :] = (
            jnp.dot(ot_ref[wo_rows(dev), :], gh_ref[:, cols], preferred_element_type=F32)
            + jnp.dot(ot_mate[chip], gh_mate[:, cols], preferred_element_type=F32))

    moves = [remote(part.at[3, 0], box.at[0], rs_send.at[0], rs_recv.at[0], near_x),
             remote(part.at[3, 1], box.at[1], rs_send.at[1], rs_recv.at[1], near_y),
             remote(part.at[1, 0], box.at[2], rs_send.at[2], rs_recv.at[2], near_x),
             remote(part.at[2, 1], box.at[3], rs_send.at[3], rs_recv.at[3], near_y),
             remote(part.at[2, 0], box.at[4], rs_send.at[4], rs_recv.at[4], near_y),
             remote(part.at[1, 1], box.at[5], rs_send.at[5], rs_recv.at[5], near_x)]
    compute(3, diag, 0)
    moves[0].start()
    compute(3, diag, 1)
    moves[1].start()
    compute(1, near_x, 0)
    moves[2].start()
    compute(2, near_y, 1)
    moves[3].start()
    for c in gw_moves:
        c.start()
    compute(2, near_y, 0)
    compute(1, near_x, 1)
    compute(0, me, 0)
    compute(0, me, 1)

    def add_box(rel, col, n):
        def rows_add(i, _):
            rows = pl.ds(pl.multiple_of(i * 32, 32), 32)
            part[rel, col, rows, :] += box[n, rows, :]
            return 0
        lax.fori_loop(0, OUT_ROWS // 32, rows_add, 0)

    moves[0].wait_recv()
    add_box(2, 0, 0)
    moves[4].start()
    moves[1].wait_recv()
    add_box(1, 1, 1)
    moves[5].start()

    for c in d_moves:
        c.wait_recv()
    win_copy.wait()
    gain1 = gain_ref[...]

    def grad_rows(i, acc):
        rows = pl.ds(pl.multiple_of(i * LANES, LANES), LANES)
        gu = dot_nt(d_buf[0, rows, :], win_buf[:, 0:3 * LANES])
        for g in range(1, NDEV):
            gu = gu + dot_nt(d_buf[g, rows, :], win_buf[:, g * 3 * LANES:(g + 1) * 3 * LANES])
        gu = gu.astype(BF16).astype(F32)
        xv = x_ref[rows, :].astype(F32)
        inv = lax.rsqrt(jnp.mean(xv * xv, axis=-1, keepdims=True) + NORM_EPS)
        normed = xv * inv
        acc = acc + jnp.sum(gu * normed, axis=0, keepdims=True)
        scaled = gu * gain1
        mean_term = jnp.mean(scaled * normed, axis=-1, keepdims=True)
        gx_out[rows, :] = (gh_ref[rows, :].astype(F32) + inv * (scaled - normed * mean_term)).astype(BF16)
        return acc

    gg1 = lax.fori_loop(0, TOK // LANES, grad_rows, jnp.zeros((1, D), F32))
    gg2 = gg2_ref[...]
    for n in range(NDEV):
        piece = slice(n * LANES, (n + 1) * LANES)
        gain_mine[n] = jnp.concatenate([gg1[:, piece], gg2[:, piece], jnp.zeros((6, LANES), F32)], axis=0)
    for c in gg_moves:
        c.start()
    gain_buf[me] = gain_mine[me]

    moves[2].wait_recv()
    add_box(0, 0, 2)
    moves[3].wait_recv()
    add_box(0, 1, 3)
    for c in gg_moves:
        c.wait_recv()
    total = gain_buf[0]
    for n in range(1, NDEV):
        total = total + gain_buf[n]
    gain_out[...] = total
    for col in range(2):
        moves[4 + col].wait_recv()

        def finish(i, _):
            rows = pl.ds(pl.multiple_of(i * 32, 32), 32)
            dn_out[rows, col * COLS:(col + 1) * COLS] = part[0, col, rows, :] + box[4 + col, rows, :]
            return 0

        lax.fori_loop(0, DN_ROWS // 32, finish, 0)
        wo_out[:, col * COLS:(col + 1) * COLS] = part[0, col, DN_ROWS:OUT_ROWS, :] + box[4 + col, DN_ROWS:OUT_ROWS, :]
    for c in gw_moves:
        c.wait_recv()
    for c in swaps + d_moves + gw_moves + gg_moves + moves:
        c.wait_send()


def tail_stage(m_t, grad_y, o_t, grad_h, grad_win, d_qkv, x, gain1, gg2, win_full):
    dma = pltpu.SemaphoreType.DMA
    peers = (NDEV - 1,)
    return pl.pallas_call(
        tail_kernel,
        out_shape=(jax.ShapeDtypeStruct((DN_ROWS, D), F32), jax.ShapeDtypeStruct((LANES, D), F32),
                   jax.ShapeDtypeStruct((NDEV, LANES, 3 * LANES), F32), jax.ShapeDtypeStruct((TOK, D), BF16),
                   jax.ShapeDtypeStruct((8, LANES), F32)),
        in_specs=[VMEM_SPEC] * 9 + [pl.BlockSpec(memory_space=pl.ANY)],
        out_specs=(VMEM_SPEC,) * 5,
        scratch_shapes=[pltpu.VMEM((4, DN_ROWS, TOK), BF16), pltpu.VMEM((TOK, D), BF16),
                        pltpu.VMEM((4, LANES, TOK), BF16), pltpu.VMEM((TOK, D), BF16),
                        pltpu.VMEM((4, 2, OUT_ROWS, COLS), F32), pltpu.VMEM((6, OUT_ROWS, COLS), F32),
                        pltpu.VMEM((NDEV, TOK, 3 * LANES), BF16), pltpu.VMEM((D, 3 * D), BF16),
                        pltpu.VMEM((NDEV, 8, LANES), F32), pltpu.VMEM((NDEV, 8, LANES), F32),
                        dma((10,)), dma((10,)), dma((6,)), dma((6,)), dma(peers), dma(peers),
                        dma(peers), dma(peers), dma(peers), dma(peers), dma],
        compiler_params=pltpu.CompilerParams(collective_id=1, has_side_effects=True,
                                             vmem_limit_bytes=60 * 1024 * 1024),
        cost_estimate=pl.CostEstimate(flops=60_000_000_000, bytes_accessed=60_000_000, transcendentals=1_000),
        name='tail_stage',
    )(m_t, grad_y, o_t, grad_h, grad_win, d_qkv, x, gain1, gg2, win_full)


def rms_back(grad_out, normed, inv_rms):
    mean_term = jnp.mean(grad_out * normed, axis=-1, keepdims=True)
    return inv_rms * (grad_out - normed * mean_term)


def solution(mesh):
    row_spec = P('sp', None)
    cube_spec = P('sp', None, None)
    vec_spec = P('sp')

    def gather(t):
        return lax.all_gather(t, 'sp', axis=0, tiled=True)

    def scatter_sum(t):
        return lax.psum_scatter(t, 'sp', scatter_dimension=0, tiled=True)

    def exchange(t):
        return lax.all_to_all(t, 'sp', 0, 0)

    def local_layer(x, seg_ids, positions, grad_y, norm1_gain, w_q, w_k, w_v, w_o, norm2_gain, w_gate, w_up, w_down):
        half = HD // 2
        inv_freq = (ROPE_BASE ** (-jnp.arange(half, dtype=F32) * 2.0 / HD))[:, None]
        freq = jnp.broadcast_to(inv_freq, (half, LANES))
        small = jnp.concatenate([norm1_gain.astype(F32)[None, :], norm2_gain.astype(F32)[None, :],
                                 positions.astype(F32).reshape(4, LANES), jnp.zeros((2, LANES), F32)])
        w_in = jnp.concatenate([t.reshape(LANES, NDEV, LANES) for t in (w_q, w_k, w_v)], axis=2)
        u_all, q, k, v, cos_t, sin_t, small = head_stage(x, w_in.transpose(1, 0, 2), small, freq)
        gain1 = small[:, 0].reshape(D)
        gain2 = small[:, 1].reshape(D)
        start_all = jnp.arange(SEQ, dtype=jnp.int32) - small[:, 2:6].reshape(SEQ).astype(jnp.int32)
        lo = start_all[::BQ] // BK
        start2 = start_all.reshape(NQ, BQ)
        start2 = jnp.concatenate([start2, start2], axis=1)
        o_own, lse = attn_forward(lo, start2, q, k, v)
        o_heads = exchange(o_own.reshape(NDEV, TOK, LANES))
        o_loc = o_heads.transpose(1, 0, 2).reshape(TOK, D)
        o_t = o_heads.transpose(0, 2, 1).reshape(D, TOK)

        wo_full = gather(w_o.reshape(LANES, D))
        wgu_full = gather(jnp.concatenate([w_gate, w_up], axis=1))
        wd_full = gather(w_down)
        win_full = gather(w_in.reshape(LANES, 3 * D))

        x_wide = x.astype(F32)
        h_res = (x_wide + jnp.dot(o_loc, wo_full, preferred_element_type=F32)).astype(BF16)
        h_wide = h_res.astype(F32)
        inv_rms2 = lax.rsqrt(jnp.mean(h_wide * h_wide, axis=-1, keepdims=True) + NORM_EPS)
        normed2 = h_wide * inv_rms2
        z_norm = (normed2 * gain2).astype(BF16)
        gate_up = jnp.dot(z_norm, wgu_full, preferred_element_type=F32)
        gate_pre, up_pre = gate_up[:, :FF], gate_up[:, FF:]
        gate_sig = jax.nn.sigmoid(gate_pre)
        gate_act = gate_pre * gate_sig
        mlp_act = (gate_act * up_pre).astype(BF16)

        grad_act = dot_nt(grad_y, wd_full).astype(BF16).astype(F32)
        grad_gate = (grad_act * up_pre * gate_sig * (1.0 + gate_pre * (1.0 - gate_sig))).astype(BF16)
        grad_up = (grad_act * gate_act).astype(BF16)
        grad_gu = jnp.concatenate([grad_gate, grad_up], axis=1)
        grad_wgu = scatter_sum(dot_tn(z_norm, grad_gu))
        grad_z = dot_nt(grad_gu, wgu_full).astype(BF16).astype(F32)
        grad_gain2 = jnp.sum(grad_z * normed2, axis=0, keepdims=True)
        grad_h = (grad_y.astype(F32) + rms_back(grad_z * gain2, normed2, inv_rms2)).astype(BF16)
        grad_o = dot_nt(grad_h, wo_full).astype(BF16)
        grad_o = exchange(grad_o.reshape(TOK, NDEV, LANES).transpose(1, 0, 2)).reshape(SEQ, LANES)
        y = (h_wide + jnp.dot(mlp_act, wd_full, preferred_element_type=F32)).astype(BF16)

        d_qkv = attn_backward(lo, start2, lse, q, k, v, o_own, grad_o, cos_t, sin_t)
        grad_win = dot_tn(u_all, d_qkv).reshape(NDEV, LANES, 3 * LANES)
        grad_wdown, grad_wo, grad_win, grad_x, grad_gains = tail_stage(
            mlp_act.T, grad_y, o_t, grad_h, grad_win, d_qkv.reshape(NDEV, TOK, 3 * LANES), x,
            gain1[None, :], grad_gain2, win_full)
        grad_q, grad_k, grad_v = (grad_win[:, :, n * LANES:(n + 1) * LANES].transpose(1, 0, 2).reshape(LANES, 16, HD)
                                  for n in range(3))
        return (y, grad_x, grad_gains[0], grad_q, grad_k, grad_v, grad_wo.reshape(2, HD, D),
                grad_gains[1], grad_wgu[:, :FF], grad_wgu[:, FF:], grad_wdown)

    return jax.shard_map(
        local_layer, mesh=mesh,
        in_specs=(row_spec, vec_spec, vec_spec, row_spec, vec_spec, cube_spec, cube_spec, cube_spec, cube_spec,
                  vec_spec, row_spec, row_spec, row_spec),
        out_specs=(row_spec, row_spec, vec_spec, cube_spec, cube_spec, cube_spec, cube_spec, vec_spec,
                   row_spec, row_spec, row_spec),
        check_vma=False)
```

```python
import jax
import jax.numpy as jnp
from jax import lax
from jax.experimental import pallas as pl
from jax.experimental.pallas import tpu as pltpu
from jax.sharding import PartitionSpec as P


NORM_EPS = 1e-5
ROPE_BASE = 10000.0
SEQ = 4096
D = 1024
HD = 64
FF = 2816
NDEV = 8
TOK = SEQ // NDEV
LANES = 128
BQ = 256
BK = 512
NQ = SEQ // BQ
NEG = -1e30
F32 = jnp.float32
BF16 = jnp.bfloat16


def dot_nt(a, b):
    return lax.dot_general(a, b, (((1,), (1,)), ((), ())), preferred_element_type=F32)


def dot_tn(a, b):
    return lax.dot_general(a, b, (((0,), (0,)), ((), ())), preferred_element_type=F32)


def head_pair(t):
    lane = lax.broadcasted_iota(jnp.int32, (1, LANES), 1)
    low = (lane < HD).astype(F32).astype(BF16)
    high = (lane >= HD).astype(F32).astype(BF16)
    return jnp.concatenate([t * low, t * high], axis=0)


def rope_back_tile(t, cos_t, sin_t):
    lane = lax.broadcasted_iota(jnp.int32, t.shape, 1)
    first_half = lax.rem(lane, HD) < HD // 2
    rotated = jnp.where(first_half, -pltpu.roll(t, LANES - HD // 2, 1), pltpu.roll(t, HD // 2, 1))
    return t * cos_t - rotated * sin_t


def attn_fwd_kernel(lo_ref, start_ref, q_ref, k_ref, v_ref, o_ref, lse_ref, acc_ref):
    q_iota = lax.rem(lax.broadcasted_iota(jnp.int32, (1, 2 * BQ), 1), BQ)

    def q_block(i, _):
        q_start = pl.multiple_of(i * BQ, BQ)
        q2 = head_pair(q_ref[pl.ds(q_start, BQ), :])
        first = start_ref[pl.ds(i, 1), :]
        q_index = q_start + q_iota
        acc_ref[...] = jnp.zeros_like(acc_ref)

        def k_block(j, carry):
            m_old, l_old = carry
            k_start = pl.multiple_of(j * BK, BK)
            k = k_ref[pl.ds(k_start, BK), :]
            v = v_ref[pl.ds(k_start, BK), :]
            s = dot_nt(k, q2)
            k_index = k_start + lax.broadcasted_iota(jnp.int32, s.shape, 0)
            s = jnp.where((k_index >= first) & (k_index <= q_index), s, NEG)
            m_new = jnp.maximum(m_old, jnp.max(s, axis=0, keepdims=True))
            p = jnp.exp(s - m_new)
            alpha = jnp.exp(m_old - m_new)
            l_new = alpha * l_old + jnp.sum(p, axis=0, keepdims=True)
            acc_ref[...] = acc_ref[...] * alpha + dot_tn(v, p.astype(BF16))
            return m_new, l_new

        init = (jnp.full((1, 2 * BQ), NEG, F32), jnp.zeros((1, 2 * BQ), F32))
        m_fin, l_fin = lax.fori_loop(lax.div(lo_ref[i, 0], BK), (q_start + BQ - 1) // BK + 1, k_block, init)
        lse_ref[pl.ds(i, 1), :] = m_fin + jnp.log(l_fin)
        out = acc_ref[...] * (1.0 / l_fin)
        out = jnp.concatenate([out[:HD, :BQ], out[HD:, BQ:]], axis=0)
        o_ref[pl.ds(q_start, BQ), :] = out.T.astype(BF16)
        return 0

    lax.fori_loop(0, NQ, q_block, 0)


def attn_bwd_kernel(lo_ref, start_ref, lse_ref, q_ref, k_ref, v_ref, o_ref, do_ref, cos_ref, sin_ref,
                    out_ref, dk_acc, dv_acc, dq_acc):
    q_iota = lax.rem(lax.broadcasted_iota(jnp.int32, (1, 2 * BQ), 1), BQ)
    dk_acc[...] = jnp.zeros_like(dk_acc)
    dv_acc[...] = jnp.zeros_like(dv_acc)

    def q_block(i, _):
        q_start = pl.multiple_of(i * BQ, BQ)
        q2 = head_pair(q_ref[pl.ds(q_start, BQ), :])
        do = do_ref[pl.ds(q_start, BQ), :]
        do2 = head_pair(do)
        prod = (do.astype(F32) * o_ref[pl.ds(q_start, BQ), :].astype(F32)).T
        delta = jnp.concatenate([jnp.sum(prod[:HD], axis=0, keepdims=True),
                                 jnp.sum(prod[HD:], axis=0, keepdims=True)], axis=1)
        first = start_ref[pl.ds(i, 1), :]
        lse = lse_ref[pl.ds(i, 1), :]
        q_index = q_start + q_iota
        dq_acc[...] = jnp.zeros_like(dq_acc)

        def k_block(j, _):
            k_start = pl.multiple_of(j * BK, BK)
            k = k_ref[pl.ds(k_start, BK), :]
            v = v_ref[pl.ds(k_start, BK), :]
            s = dot_nt(k, q2)
            k_index = k_start + lax.broadcasted_iota(jnp.int32, s.shape, 0)
            s = jnp.where((k_index >= first) & (k_index <= q_index), s, NEG)
            p = jnp.exp(s - lse)
            dp = dot_nt(v, do2).astype(BF16).astype(F32)
            ds = (p * (dp - delta)).astype(BF16)
            dv_acc[pl.ds(k_start, BK), :] += jnp.dot(p.astype(BF16), do2, preferred_element_type=F32)
            dk_acc[pl.ds(k_start, BK), :] += jnp.dot(ds, q2, preferred_element_type=F32)
            dq_acc[...] += dot_tn(k, ds)
            return 0

        lax.fori_loop(lax.div(lo_ref[i, 0], BK), (q_start + BQ - 1) // BK + 1, k_block, 0)
        dq = jnp.concatenate([dq_acc[:HD, :BQ], dq_acc[HD:, BQ:]], axis=0).T * (HD ** -0.5)
        rows = pl.ds(q_start, BQ)
        dq = dq.astype(BF16).astype(F32)
        out_ref[rows, 0:LANES] = rope_back_tile(dq, cos_ref[rows, :], sin_ref[rows, :]).astype(BF16)
        return 0

    lax.fori_loop(0, NQ, q_block, 0)

    def finish(i, _):
        rows = pl.ds(pl.multiple_of(i * BQ, BQ), BQ)
        dk = dk_acc[rows, :].astype(BF16).astype(F32)
        out_ref[rows, LANES:2 * LANES] = rope_back_tile(dk, cos_ref[rows, :], sin_ref[rows, :]).astype(BF16)
        out_ref[rows, 2 * LANES:3 * LANES] = dv_acc[rows, :].astype(BF16)
        return 0

    lax.fori_loop(0, NQ, finish, 0)


VMEM_SPEC = pl.BlockSpec(memory_space=pltpu.VMEM)
SMEM_SPEC = pl.BlockSpec(memory_space=pltpu.SMEM)


def attn_forward(start, q, k, v):
    return pl.pallas_call(
        attn_fwd_kernel,
        out_shape=(jax.ShapeDtypeStruct((SEQ, LANES), BF16), jax.ShapeDtypeStruct((NQ, 2 * BQ), F32)),
        in_specs=[SMEM_SPEC] + [VMEM_SPEC] * 4,
        out_specs=(VMEM_SPEC, VMEM_SPEC),
        scratch_shapes=[pltpu.VMEM((LANES, 2 * BQ), F32)],
        compiler_params=pltpu.CompilerParams(vmem_limit_bytes=40 * 1024 * 1024),
        cost_estimate=pl.CostEstimate(flops=20_000_000_000, bytes_accessed=5_000_000, transcendentals=20_000_000),
        name='attn_fwd',
    )(start, start, q, k, v)


def attn_backward(start, lse, q, k, v, o, do, cos_t, sin_t):
    return pl.pallas_call(
        attn_bwd_kernel,
        out_shape=jax.ShapeDtypeStruct((SEQ, 3 * LANES), BF16),
        in_specs=[SMEM_SPEC] + [VMEM_SPEC] * 9,
        out_specs=VMEM_SPEC,
        scratch_shapes=[pltpu.VMEM((SEQ, LANES), F32), pltpu.VMEM((SEQ, LANES), F32),
                        pltpu.VMEM((LANES, 2 * BQ), F32)],
        compiler_params=pltpu.CompilerParams(vmem_limit_bytes=48 * 1024 * 1024),
        cost_estimate=pl.CostEstimate(flops=50_000_000_000, bytes_accessed=12_000_000, transcendentals=20_000_000),
        name='attn_bwd',
    )(start, start, lse, q, k, v, o, do, cos_t, sin_t)


def head_kernel(x_ref, w_ref, small_ref, freq_ref, wo_ref, u_hbm, q_ref, k_ref, v_ref, cos_ref, sin_ref, all_small,
                start_ref, wo_out, x_buf, w_buf, w_ext, u_buf, small_send, small_recv, w_send, w_recv, x_send, x_recv,
                wo_send, wo_recv, u_sem):
    me = lax.axis_index('sp')
    core = lax.rem(me, 2)
    x_pos = lax.rem(me // 2, 2)
    y_pos = me // 4
    step_c, step_x, step_y = 1 - 2 * core, 2 - 4 * x_pos, 4 - 8 * y_pos
    mate, near_x, near_y, diag = me + step_c, me + step_x, me + step_y, me + step_x + step_y

    barrier = pltpu.get_barrier_semaphore()
    for n in range(1, NDEV):
        pl.semaphore_signal(barrier, inc=1, device_id=(lax.rem(me + n, NDEV),), device_id_type=pl.DeviceIdType.MESH)
    pl.semaphore_wait(barrier, NDEV - 1)

    def remote(src, dst, send_sem, recv_sem, dev):
        return pltpu.make_async_remote_copy(src_ref=src, dst_ref=dst, send_sem=send_sem, recv_sem=recv_sem,
                                            device_id=(dev,), device_id_type=pl.DeviceIdType.MESH)

    def half(ref, h):
        rows = ref.shape[0] // 2
        return ref.at[pl.ds(h * rows, rows), :]

    def x_copy(slot, src_dev, h, target, from_ref=None):
        source = half(x_buf.at[src_dev], h) if from_ref is None else half(from_ref, h)
        return remote(source, half(x_buf.at[src_dev], h), x_send.at[slot], x_recv.at[slot], target)

    def wo_copy(slot, src_dev, h, target, from_ref=None):
        source = half(wo_out.at[src_dev], h) if from_ref is None else half(from_ref, h)
        return remote(source, half(wo_out.at[src_dev], h), wo_send.at[slot], wo_recv.at[slot], target)

    def first_sends(copy, from_ref):
        return [copy(0, me, 0, near_x, from_ref), copy(3, me, 1, near_y, from_ref),
                copy(1, me, 1, near_x, from_ref), copy(2, me, 0, near_y, from_ref),
                copy(12, me, 0, mate, from_ref), copy(13, me, 1, mate, from_ref)]

    smalls = [remote(small_ref, all_small.at[me], small_send.at[n - 1], small_recv.at[n - 1], lax.rem(me + n, NDEV))
              for n in range(1, NDEV)]
    weights = [remote(w_ref.at[lax.rem(me + n, NDEV)], w_buf.at[me], w_send.at[n - 1], w_recv.at[n - 1],
                      lax.rem(me + n, NDEV)) for n in range(1, NDEV)]
    for c in smalls:
        c.start()
    for c in weights:
        c.start()
    own = first_sends(x_copy, x_ref)
    for c in own:
        c.start()

    all_small[me] = small_ref[...]
    w_buf[me] = w_ref[me]
    for c in smalls + weights:
        c.wait_recv()

    lane = lax.broadcasted_iota(jnp.int32, (LANES, LANES), 1)
    first_half = lax.rem(lane, HD) < HD // 2

    def build(i, _):
        rows = pl.ds(pl.multiple_of(i * LANES, LANES), LANES)
        w_ext[rows, 0:3 * LANES] = w_buf[i]
        for n in range(2):
            t = w_buf[i, :, n * LANES:(n + 1) * LANES].astype(F32)
            rot = jnp.where(first_half, -pltpu.roll(t, LANES - HD // 2, 1), pltpu.roll(t, HD // 2, 1))
            w_ext[rows, (3 + n) * LANES:(4 + n) * LANES] = rot.astype(BF16)
        return 0

    lax.fori_loop(0, NDEV, build, 0)
    gain1 = jnp.concatenate([all_small[n, 0:1, :] for n in range(NDEV)], axis=1)

    def process(order, src_ref, src_dev, h):
        def part(i, _):
            local = pl.ds(pl.multiple_of(h * (TOK // 2) + i * LANES, LANES), LANES)
            rows = pl.ds(pl.multiple_of(src_dev * TOK + h * (TOK // 2) + i * LANES, LANES), LANES)
            xv = src_ref[local, :].astype(F32)
            inv = lax.rsqrt(jnp.mean(xv * xv, axis=-1, keepdims=True) + NORM_EPS)
            u = (xv * inv * gain1).astype(BF16)
            u_buf[rows, :] = u
            proj = jnp.dot(u, w_ext[...], preferred_element_type=F32)
            angle = freq_ref[...] * all_small[src_dev, pl.ds(2 + 2 * h + i, 1), :]
            cos4, sin4 = jnp.cos(angle), jnp.sin(angle)
            cos_v = jnp.concatenate([cos4] * 4, axis=0).T
            sin_v = jnp.concatenate([sin4] * 4, axis=0).T
            cos_ref[rows, :] = cos_v
            sin_ref[rows, :] = sin_v
            q = (proj[:, :LANES] * cos_v + proj[:, 3 * LANES:4 * LANES] * sin_v).astype(BF16).astype(F32)
            q_ref[rows, :] = (q * (HD ** -0.5)).astype(BF16)
            k_ref[rows, :] = (proj[:, LANES:2 * LANES] * cos_v + proj[:, 4 * LANES:] * sin_v).astype(BF16)
            v_ref[rows, :] = proj[:, 2 * LANES:3 * LANES].astype(BF16)
            return 0

        lax.fori_loop(0, 2, part, 0)
        u_rows = pl.ds(pl.multiple_of(src_dev * TOK + h * (TOK // 2), TOK // 2), TOK // 2)
        out = pltpu.make_async_copy(u_buf.at[u_rows, :], u_hbm.at[u_rows, :], u_sem.at[order])
        out.start()
        return out

    pending = []
    copies = list(own)

    def arrive(copy, slot, src_dev, h):
        copy(slot, src_dev, h, mate).wait_recv()

    def pass_on(copy, slot, src_dev, h, target):
        c = copy(slot, src_dev, h, target)
        c.start()
        copies.append(c)

    def relay(copy, slot, src_dev, h):
        arrive(copy, slot, src_dev, h)
        if slot == 0:
            pass_on(copy, 4, src_dev, h, near_y)
        elif slot == 3:
            pass_on(copy, 5, src_dev, h, near_x)
        pass_on(copy, 6 + slot, src_dev, h, mate)

    def work(src_ref, src_dev, h):
        pending.append(process(len(pending), src_ref, src_dev, h))

    work(x_ref, me, 0)
    work(x_ref, me, 1)
    arrivals = [(0, near_x, 0), (3, near_y, 1), (1, near_x, 1), (2, near_y, 0), (4, diag, 0), (5, diag, 1)]
    late = [(12, mate, 0), (13, mate, 1)]
    for n, (slot, src_dev, h) in enumerate(arrivals):
        relay(x_copy, slot, src_dev, h)
        if n == 1:
            wo_own = first_sends(wo_copy, wo_ref)
            for c in wo_own:
                c.start()
            copies += wo_own
            wo_out[me] = wo_ref[...]
        if n >= 4:
            relay(wo_copy, *arrivals[n - 4])
        work(x_buf.at[src_dev], src_dev, h)
        mate_slot, mate_src, mate_h = late.pop(0)
        arrive(x_copy, mate_slot, mate_src, mate_h)
        work(x_buf.at[mate_src], mate_src, mate_h)
        late.append((6 + slot, src_dev + step_c, h))
    for n, (slot, src_dev, h) in enumerate(late):
        if n < 2:
            relay(wo_copy, *arrivals[n + 2])
        arrive(x_copy, slot, src_dev, h)
        work(x_buf.at[src_dev], src_dev, h)
    for n in range(NDEV):
        for h in range(2):
            row = jnp.concatenate([all_small[n, 2 + 2 * h:3 + 2 * h, :], all_small[n, 3 + 2 * h:4 + 2 * h, :]], axis=1)
            index = n * TOK + h * BQ + lax.broadcasted_iota(jnp.int32, (1, BQ), 1)
            first = index - row.astype(jnp.int32)
            start_ref[2 * n + h:2 * n + h + 1, :] = jnp.concatenate([first, first], axis=1)
    relay(wo_copy, *arrivals[4])
    relay(wo_copy, *arrivals[5])
    for slot, src_dev, h in [(12, mate, 0), (13, mate, 1)] + [(6 + m, d + step_c, h) for m, d, h in arrivals]:
        arrive(wo_copy, slot, src_dev, h)
    for c in pending:
        c.wait()
    for c in smalls + weights + copies:
        c.wait_send()


def head_stage(x, w_pieces, small, freq, w_o):
    dma = pltpu.SemaphoreType.DMA
    return pl.pallas_call(
        head_kernel,
        out_shape=(jax.ShapeDtypeStruct((SEQ, D), BF16),) + tuple(jax.ShapeDtypeStruct((SEQ, LANES), BF16) for _ in range(3))
        + tuple(jax.ShapeDtypeStruct((SEQ, LANES), F32) for _ in range(2))
        + (jax.ShapeDtypeStruct((NDEV, 8, LANES), F32), jax.ShapeDtypeStruct((NQ, 2 * BQ), jnp.int32),
           jax.ShapeDtypeStruct((NDEV, LANES, D), BF16)),
        in_specs=[VMEM_SPEC] * 5,
        out_specs=(pl.BlockSpec(memory_space=pl.ANY),) + (VMEM_SPEC,) * 8,
        scratch_shapes=[pltpu.VMEM((NDEV, TOK, D), BF16), pltpu.VMEM((NDEV, LANES, 3 * LANES), BF16),
                        pltpu.VMEM((D, 5 * LANES), BF16), pltpu.VMEM((SEQ, D), BF16),
                        dma((NDEV - 1,)), dma((NDEV - 1,)), dma((NDEV - 1,)), dma((NDEV - 1,)),
                        dma((14,)), dma((14,)), dma((14,)), dma((14,)), dma((16,))],
        compiler_params=pltpu.CompilerParams(collective_id=0, has_side_effects=True,
                                             vmem_limit_bytes=48 * 1024 * 1024),
        cost_estimate=pl.CostEstimate(flops=40_000_000_000, bytes_accessed=30_000_000, transcendentals=1_000_000),
        name='head_stage',
    )(x, w_pieces, small, freq, w_o)


COLS = D // 2
DN_ROWS = FF // NDEV
OUT_ROWS = DN_ROWS + LANES


def tail_kernel(mt_ref, gy_ref, ot_ref, gh_ref, d_ref, x_ref, h_ref, gz_ref, gain_ref, u_hbm, win_hbm,
                dn_out, wo_out, gw_out, gx_out, gain_out,
                mt_mate, gy_mate, ot_mate, gh_mate, part, box, d_buf, win_buf, u_buf, gw_mine, gain_mine, gain_buf,
                mate_send, mate_recv, rs_send, rs_recv, d_send, d_recv, gw_send, gw_recv, gg_send, gg_recv, win_sem, u_sem):
    me = lax.axis_index('sp')
    core = lax.rem(me, 2)
    x_pos = lax.rem(me // 2, 2)
    y_pos = me // 4
    step_c, step_x, step_y = 1 - 2 * core, 2 - 4 * x_pos, 4 - 8 * y_pos
    mate, near_x, near_y, diag = me + step_c, me + step_x, me + step_y, me + step_x + step_y

    win_copy = pltpu.make_async_copy(win_hbm, win_buf, win_sem)
    win_copy.start()
    u_copy = pltpu.make_async_copy(u_hbm, u_buf, u_sem)
    u_copy.start()

    barrier = pltpu.get_barrier_semaphore()
    for n in range(1, NDEV):
        pl.semaphore_signal(barrier, inc=1, device_id=(lax.rem(me + n, NDEV),), device_id_type=pl.DeviceIdType.MESH)
    pl.semaphore_wait(barrier, NDEV - 1)

    def remote(src, dst, send_sem, recv_sem, dev):
        return pltpu.make_async_remote_copy(src_ref=src, dst_ref=dst, send_sem=send_sem, recv_sem=recv_sem,
                                            device_id=(dev,), device_id_type=pl.DeviceIdType.MESH)

    def to_peers(src, dst, send_sem, recv_sem):
        return [remote(src.at[lax.rem(me + n, NDEV)], dst.at[me], send_sem.at[n - 1], recv_sem.at[n - 1],
                       lax.rem(me + n, NDEV)) for n in range(1, NDEV)]

    def dn_rows(dev):
        return pl.ds(pl.multiple_of(dev * DN_ROWS, 32), DN_ROWS)

    def wo_rows(dev):
        return pl.ds(pl.multiple_of(dev * LANES, LANES), LANES)

    swaps = []
    for q in range(NDEV // 2):
        dest = 2 * q + 1 - core
        swaps.append(remote(mt_ref.at[dn_rows(dest), :], mt_mate.at[q], mate_send.at[q], mate_recv.at[q], mate))
        swaps.append(remote(ot_ref.at[wo_rows(dest), :], ot_mate.at[q], mate_send.at[4 + q], mate_recv.at[4 + q], mate))
    swaps.append(remote(gy_ref, gy_mate, mate_send.at[8], mate_recv.at[8], mate))
    swaps.append(remote(gh_ref, gh_mate, mate_send.at[9], mate_recv.at[9], mate))
    for c in swaps:
        c.start()
    d_moves = to_peers(d_ref, d_buf, d_send, d_recv)
    gw_moves = to_peers(gw_mine, gw_out, gw_send, gw_recv)
    gg_moves = to_peers(gain_mine, gain_buf, gg_send, gg_recv)
    for c in d_moves:
        c.start()
    d_buf[me] = d_ref[me]
    for c in swaps:
        c.wait_recv()

    def compute(rel, dev, col):
        chip = dev // 2
        cols = pl.ds(col * COLS, COLS)
        part[rel, col, 0:DN_ROWS, :] = (
            jnp.dot(mt_ref[dn_rows(dev), :], gy_ref[:, cols], preferred_element_type=F32)
            + jnp.dot(mt_mate[chip], gy_mate[:, cols], preferred_element_type=F32))
        part[rel, col, DN_ROWS:OUT_ROWS, :] = (
            jnp.dot(ot_ref[wo_rows(dev), :], gh_ref[:, cols], preferred_element_type=F32)
            + jnp.dot(ot_mate[chip], gh_mate[:, cols], preferred_element_type=F32))

    moves = [remote(part.at[3, 0], box.at[0], rs_send.at[0], rs_recv.at[0], near_x),
             remote(part.at[3, 1], box.at[1], rs_send.at[1], rs_recv.at[1], near_y),
             remote(part.at[1, 0], box.at[2], rs_send.at[2], rs_recv.at[2], near_x),
             remote(part.at[2, 1], box.at[3], rs_send.at[3], rs_recv.at[3], near_y),
             remote(part.at[2, 0], box.at[4], rs_send.at[4], rs_recv.at[4], near_y),
             remote(part.at[1, 1], box.at[5], rs_send.at[5], rs_recv.at[5], near_x)]
    compute(3, diag, 0)
    moves[0].start()
    compute(3, diag, 1)
    moves[1].start()
    compute(1, near_x, 0)
    moves[2].start()
    compute(2, near_y, 1)
    moves[3].start()
    compute(2, near_y, 0)
    compute(1, near_x, 1)
    u_copy.wait()

    def grad_win_piece(n, _):
        cols = pl.ds(pl.multiple_of(n * LANES, LANES), LANES)
        total = dot_tn(u_buf[0:TOK, cols], d_ref[0])
        for g in range(1, NDEV):
            total = total + dot_tn(u_buf[g * TOK:(g + 1) * TOK, cols], d_ref[g])
        gw_mine[n] = total
        return 0

    lax.fori_loop(0, NDEV, grad_win_piece, 0)
    for c in gw_moves:
        c.start()
    gw_out[me] = gw_mine[me]
    compute(0, me, 0)
    compute(0, me, 1)

    def add_box(rel, col, n):
        def rows_add(i, _):
            rows = pl.ds(pl.multiple_of(i * 32, 32), 32)
            part[rel, col, rows, :] += box[n, rows, :]
            return 0

        lax.fori_loop(0, OUT_ROWS // 32, rows_add, 0)

    moves[0].wait_recv()
    add_box(2, 0, 0)
    moves[4].start()
    moves[1].wait_recv()
    add_box(1, 1, 1)
    moves[5].start()

    for c in d_moves:
        c.wait_recv()
    win_copy.wait()
    gain1 = gain_ref[...]

    def grad_rows(i, carry):
        acc, acc2 = carry
        rows = pl.ds(pl.multiple_of(i * LANES, LANES), LANES)
        gu = dot_nt(d_buf[0, rows, :], win_buf[:, 0:3 * LANES])
        for g in range(1, NDEV):
            gu = gu + dot_nt(d_buf[g, rows, :], win_buf[:, g * 3 * LANES:(g + 1) * 3 * LANES])
        gu = gu.astype(BF16).astype(F32)
        xv = x_ref[rows, :].astype(F32)
        inv = lax.rsqrt(jnp.mean(xv * xv, axis=-1, keepdims=True) + NORM_EPS)
        normed = xv * inv
        acc = acc + jnp.sum(gu * normed, axis=0, keepdims=True)
        scaled = gu * gain1
        mean_term = jnp.mean(scaled * normed, axis=-1, keepdims=True)
        gx_out[rows, :] = (gh_ref[rows, :].astype(F32) + inv * (scaled - normed * mean_term)).astype(BF16)
        hv = h_ref[rows, :].astype(F32)
        normed2 = hv * lax.rsqrt(jnp.mean(hv * hv, axis=-1, keepdims=True) + NORM_EPS)
        acc2 = acc2 + jnp.sum(gz_ref[rows, :].astype(F32) * normed2, axis=0, keepdims=True)
        return acc, acc2

    gg1, gg2 = lax.fori_loop(0, TOK // LANES, grad_rows, (jnp.zeros((1, D), F32), jnp.zeros((1, D), F32)))
    for n in range(NDEV):
        piece = slice(n * LANES, (n + 1) * LANES)
        gain_mine[n] = jnp.concatenate([gg1[:, piece], gg2[:, piece], jnp.zeros((6, LANES), F32)], axis=0)
    for c in gg_moves:
        c.start()
    gain_buf[me] = gain_mine[me]

    moves[2].wait_recv()
    add_box(0, 0, 2)
    moves[3].wait_recv()
    add_box(0, 1, 3)
    for c in gg_moves:
        c.wait_recv()
    total = gain_buf[0]
    for n in range(1, NDEV):
        total = total + gain_buf[n]
    gain_out[...] = total
    for col in range(2):
        moves[4 + col].wait_recv()

        def finish(i, _):
            rows = pl.ds(pl.multiple_of(i * 32, 32), 32)
            dn_out[rows, col * COLS:(col + 1) * COLS] = part[0, col, rows, :] + box[4 + col, rows, :]
            return 0

        lax.fori_loop(0, DN_ROWS // 32, finish, 0)
        wo_out[:, col * COLS:(col + 1) * COLS] = part[0, col, DN_ROWS:OUT_ROWS, :] + box[4 + col, DN_ROWS:OUT_ROWS, :]
    for c in gw_moves:
        c.wait_recv()
    for c in swaps + d_moves + gw_moves + gg_moves + moves:
        c.wait_send()


def tail_stage(m_t, grad_y, o_t, grad_h, d_qkv, x, h_res, grad_z, gain1, u_all, win_full):
    dma = pltpu.SemaphoreType.DMA
    peers = (NDEV - 1,)
    return pl.pallas_call(
        tail_kernel,
        out_shape=(jax.ShapeDtypeStruct((DN_ROWS, D), F32), jax.ShapeDtypeStruct((LANES, D), F32),
                   jax.ShapeDtypeStruct((NDEV, LANES, 3 * LANES), F32), jax.ShapeDtypeStruct((TOK, D), BF16),
                   jax.ShapeDtypeStruct((8, LANES), F32)),
        in_specs=[VMEM_SPEC] * 9 + [pl.BlockSpec(memory_space=pl.ANY)] * 2,
        out_specs=(VMEM_SPEC,) * 5,
        scratch_shapes=[pltpu.VMEM((4, DN_ROWS, TOK), BF16), pltpu.VMEM((TOK, D), BF16),
                        pltpu.VMEM((4, LANES, TOK), BF16), pltpu.VMEM((TOK, D), BF16),
                        pltpu.VMEM((4, 2, OUT_ROWS, COLS), F32), pltpu.VMEM((6, OUT_ROWS, COLS), F32),
                        pltpu.VMEM((NDEV, TOK, 3 * LANES), BF16), pltpu.VMEM((D, 3 * D), BF16),
                        pltpu.VMEM((SEQ, D), BF16), pltpu.VMEM((NDEV, LANES, 3 * LANES), F32),
                        pltpu.VMEM((NDEV, 8, LANES), F32), pltpu.VMEM((NDEV, 8, LANES), F32),
                        dma((10,)), dma((10,)), dma((6,)), dma((6,)), dma(peers), dma(peers),
                        dma(peers), dma(peers), dma(peers), dma(peers), dma, dma],
        compiler_params=pltpu.CompilerParams(collective_id=1, has_side_effects=True,
                                             vmem_limit_bytes=60 * 1024 * 1024),
        cost_estimate=pl.CostEstimate(flops=60_000_000_000, bytes_accessed=60_000_000, transcendentals=1_000),
        name='tail_stage',
    )(m_t, grad_y, o_t, grad_h, d_qkv, x, h_res, grad_z, gain1, u_all, win_full)


def rms_back(grad_out, normed, inv_rms):
    mean_term = jnp.mean(grad_out * normed, axis=-1, keepdims=True)
    return inv_rms * (grad_out - normed * mean_term)


def solution(mesh):
    row_spec = P('sp', None)
    cube_spec = P('sp', None, None)
    vec_spec = P('sp')

    def gather(t):
        return lax.all_gather(t, 'sp', axis=0, tiled=True)

    def scatter_sum(t):
        return lax.psum_scatter(t, 'sp', scatter_dimension=0, tiled=True)

    def exchange(t):
        return lax.all_to_all(t, 'sp', 0, 0)

    def local_layer(x, seg_ids, positions, grad_y, norm1_gain, w_q, w_k, w_v, w_o, norm2_gain, w_gate, w_up, w_down):
        half = HD // 2
        inv_freq = (ROPE_BASE ** (-jnp.arange(half, dtype=F32) * 2.0 / HD))[:, None]
        freq = jnp.broadcast_to(inv_freq, (half, LANES))
        small = jnp.concatenate([norm1_gain.astype(F32)[None, :], norm2_gain.astype(F32)[None, :],
                                 positions.astype(F32).reshape(4, LANES), jnp.zeros((2, LANES), F32)])
        w_in = jnp.concatenate([t.reshape(LANES, NDEV, LANES) for t in (w_q, w_k, w_v)], axis=2)
        u_all, q, k, v, cos_t, sin_t, small, start2, wo_full = head_stage(
            x, w_in.transpose(1, 0, 2), small, freq, w_o.reshape(LANES, D))
        wo_full = wo_full.reshape(D, D)
        gain1 = small[:, 0].reshape(1, D)
        gain2 = small[:, 1].reshape(D)
        o_own, lse = attn_forward(start2, q, k, v)
        o_heads = exchange(o_own.reshape(NDEV, TOK, LANES))
        o_loc = o_heads.transpose(1, 0, 2).reshape(TOK, D)
        o_t = o_heads.transpose(0, 2, 1).reshape(D, TOK)

        wd_full = gather(w_down)
        wgu_full = gather(jnp.concatenate([w_gate, w_up], axis=1))
        win_full = gather(w_in.reshape(LANES, 3 * D))

        x_wide = x.astype(F32)
        h_res = (x_wide + jnp.dot(o_loc, wo_full, preferred_element_type=F32)).astype(BF16)
        h_wide = h_res.astype(F32)
        inv_rms2 = lax.rsqrt(jnp.mean(h_wide * h_wide, axis=-1, keepdims=True) + NORM_EPS)
        normed2 = h_wide * inv_rms2
        z_norm = (normed2 * gain2).astype(BF16)
        gate_up = jnp.dot(z_norm, wgu_full, preferred_element_type=F32)
        gate_pre, up_pre = gate_up[:, :FF], gate_up[:, FF:]
        gate_sig = jax.nn.sigmoid(gate_pre)
        gate_act = gate_pre * gate_sig
        mlp_act = (gate_act * up_pre).astype(BF16)

        grad_act = dot_nt(grad_y, wd_full).astype(BF16).astype(F32)
        grad_gate = (grad_act * up_pre * gate_sig * (1.0 + gate_pre * (1.0 - gate_sig))).astype(BF16)
        grad_up = (grad_act * gate_act).astype(BF16)
        grad_gu = jnp.concatenate([grad_gate, grad_up], axis=1)
        grad_wgu = scatter_sum(dot_tn(z_norm, grad_gu))
        grad_z_b = lax.optimization_barrier(dot_nt(grad_gu, wgu_full).astype(BF16))
        grad_z = grad_z_b.astype(F32)
        grad_h = (grad_y.astype(F32) + rms_back(grad_z * gain2, normed2, inv_rms2)).astype(BF16)
        grad_o = dot_nt(grad_h, wo_full).astype(BF16)
        grad_o = exchange(grad_o.reshape(TOK, NDEV, LANES).transpose(1, 0, 2)).reshape(SEQ, LANES)
        y = (h_wide + jnp.dot(mlp_act, wd_full, preferred_element_type=F32)).astype(BF16)

        d_qkv = attn_backward(start2, lse, q, k, v, o_own, grad_o, cos_t, sin_t)
        grad_wdown, grad_wo, grad_win, grad_x, grad_gains = tail_stage(
            mlp_act.T, grad_y, o_t, grad_h, d_qkv.reshape(NDEV, TOK, 3 * LANES), x, h_res, grad_z_b,
            gain1, u_all, win_full)
        grad_q, grad_k, grad_v = (grad_win[:, :, n * LANES:(n + 1) * LANES].transpose(1, 0, 2).reshape(LANES, 16, HD)
                                  for n in range(3))
        return (y, grad_x, grad_gains[0], grad_q, grad_k, grad_v, grad_wo.reshape(2, HD, D),
                grad_gains[1], grad_wgu[:, :FF], grad_wgu[:, FF:], grad_wdown)

    return jax.shard_map(
        local_layer, mesh=mesh,
        in_specs=(row_spec, vec_spec, vec_spec, row_spec, vec_spec, cube_spec, cube_spec, cube_spec, cube_spec,
                  vec_spec, row_spec, row_spec, row_spec),
        out_specs=(row_spec, row_spec, vec_spec, cube_spec, cube_spec, cube_spec, cube_spec, vec_spec,
                   row_spec, row_spec, row_spec),
        check_vma=False)
```

```python
import jax
import jax.numpy as jnp
from jax import lax
from jax.experimental import pallas as pl
from jax.experimental.pallas import tpu as pltpu
from jax.sharding import PartitionSpec as P


NORM_EPS = 1e-5
ROPE_BASE = 10000.0
SEQ = 4096
D = 1024
HD = 64
FF = 2816
NDEV = 8
TOK = SEQ // NDEV
LANES = 128
BQ = 256
BK = 512
NQ = SEQ // BQ
NEG = -1e30
F32 = jnp.float32
BF16 = jnp.bfloat16


def dot_nt(a, b):
    return lax.dot_general(a, b, (((1,), (1,)), ((), ())), preferred_element_type=F32)


def dot_tn(a, b):
    return lax.dot_general(a, b, (((0,), (0,)), ((), ())), preferred_element_type=F32)


def head_pair(t):
    lane = lax.broadcasted_iota(jnp.int32, (1, LANES), 1)
    low = (lane < HD).astype(F32).astype(BF16)
    high = (lane >= HD).astype(F32).astype(BF16)
    return jnp.concatenate([t * low, t * high], axis=0)


def rope_back_tile(t, cos_t, sin_t):
    lane = lax.broadcasted_iota(jnp.int32, t.shape, 1)
    first_half = lax.rem(lane, HD) < HD // 2
    rotated = jnp.where(first_half, -pltpu.roll(t, LANES - HD // 2, 1), pltpu.roll(t, HD // 2, 1))
    return t * cos_t - rotated * sin_t


def attn_fwd_kernel(lo_ref, start_ref, q_ref, k_ref, v_ref, o_ref, lse_ref, acc_ref):
    q_iota = lax.rem(lax.broadcasted_iota(jnp.int32, (1, 2 * BQ), 1), BQ)

    def q_block(i, _):
        q_start = pl.multiple_of(i * BQ, BQ)
        q2 = head_pair(q_ref[pl.ds(q_start, BQ), :])
        first = start_ref[pl.ds(i, 1), :]
        q_index = q_start + q_iota
        acc_ref[...] = jnp.zeros_like(acc_ref)

        def k_block(j, carry):
            m_old, l_old = carry
            k_start = pl.multiple_of(j * BK, BK)
            k = k_ref[pl.ds(k_start, BK), :]
            v = v_ref[pl.ds(k_start, BK), :]
            s = dot_nt(k, q2)
            k_index = k_start + lax.broadcasted_iota(jnp.int32, s.shape, 0)
            s = jnp.where((k_index >= first) & (k_index <= q_index), s, NEG)
            m_new = jnp.maximum(m_old, jnp.max(s, axis=0, keepdims=True))
            p = jnp.exp(s - m_new)
            alpha = jnp.exp(m_old - m_new)
            l_new = alpha * l_old + jnp.sum(p, axis=0, keepdims=True)
            acc_ref[...] = acc_ref[...] * alpha + dot_tn(v, p.astype(BF16))
            return m_new, l_new

        init = (jnp.full((1, 2 * BQ), NEG, F32), jnp.zeros((1, 2 * BQ), F32))
        m_fin, l_fin = lax.fori_loop(lax.div(lo_ref[i, 0], BK), (q_start + BQ - 1) // BK + 1, k_block, init)
        lse_ref[pl.ds(i, 1), :] = m_fin + jnp.log(l_fin)
        out = acc_ref[...] * (1.0 / l_fin)
        out = jnp.concatenate([out[:HD, :BQ], out[HD:, BQ:]], axis=0)
        o_ref[pl.ds(q_start, BQ), :] = out.T.astype(BF16)
        return 0

    lax.fori_loop(0, NQ, q_block, 0)


def attn_bwd_kernel(lo_ref, start_ref, lse_ref, q_ref, k_ref, v_ref, o_ref, do_ref, cos_ref, sin_ref,
                    out_ref, dk_acc, dv_acc, dq_acc):
    q_iota = lax.rem(lax.broadcasted_iota(jnp.int32, (1, 2 * BQ), 1), BQ)
    dk_acc[...] = jnp.zeros_like(dk_acc)
    dv_acc[...] = jnp.zeros_like(dv_acc)

    def q_block(i, _):
        q_start = pl.multiple_of(i * BQ, BQ)
        q2 = head_pair(q_ref[pl.ds(q_start, BQ), :])
        do = do_ref[pl.ds(q_start, BQ), :]
        do2 = head_pair(do)
        prod = (do.astype(F32) * o_ref[pl.ds(q_start, BQ), :].astype(F32)).T
        delta = jnp.concatenate([jnp.sum(prod[:HD], axis=0, keepdims=True),
                                 jnp.sum(prod[HD:], axis=0, keepdims=True)], axis=1)
        first = start_ref[pl.ds(i, 1), :]
        lse = lse_ref[pl.ds(i, 1), :]
        q_index = q_start + q_iota
        dq_acc[...] = jnp.zeros_like(dq_acc)

        def k_block(j, _):
            k_start = pl.multiple_of(j * BK, BK)
            k = k_ref[pl.ds(k_start, BK), :]
            v = v_ref[pl.ds(k_start, BK), :]
            s = dot_nt(k, q2)
            k_index = k_start + lax.broadcasted_iota(jnp.int32, s.shape, 0)
            s = jnp.where((k_index >= first) & (k_index <= q_index), s, NEG)
            p = jnp.exp(s - lse)
            dp = dot_nt(v, do2).astype(BF16).astype(F32)
            ds = (p * (dp - delta)).astype(BF16)
            dv_acc[pl.ds(k_start, BK), :] += jnp.dot(p.astype(BF16), do2, preferred_element_type=F32)
            dk_acc[pl.ds(k_start, BK), :] += jnp.dot(ds, q2, preferred_element_type=F32)
            dq_acc[...] += dot_tn(k, ds)
            return 0

        lax.fori_loop(lax.div(lo_ref[i, 0], BK), (q_start + BQ - 1) // BK + 1, k_block, 0)
        dq = jnp.concatenate([dq_acc[:HD, :BQ], dq_acc[HD:, BQ:]], axis=0).T * (HD ** -0.5)
        rows = pl.ds(q_start, BQ)
        dq = dq.astype(BF16).astype(F32)
        out_ref[rows, 0:LANES] = rope_back_tile(dq, cos_ref[rows, :], sin_ref[rows, :]).astype(BF16)
        return 0

    lax.fori_loop(0, NQ, q_block, 0)

    def finish(i, _):
        rows = pl.ds(pl.multiple_of(i * BQ, BQ), BQ)
        dk = dk_acc[rows, :].astype(BF16).astype(F32)
        out_ref[rows, LANES:2 * LANES] = rope_back_tile(dk, cos_ref[rows, :], sin_ref[rows, :]).astype(BF16)
        out_ref[rows, 2 * LANES:3 * LANES] = dv_acc[rows, :].astype(BF16)
        return 0

    lax.fori_loop(0, NQ, finish, 0)


VMEM_SPEC = pl.BlockSpec(memory_space=pltpu.VMEM)
SMEM_SPEC = pl.BlockSpec(memory_space=pltpu.SMEM)


def attn_forward(start, q, k, v):
    return pl.pallas_call(
        attn_fwd_kernel,
        out_shape=(jax.ShapeDtypeStruct((SEQ, LANES), BF16), jax.ShapeDtypeStruct((NQ, 2 * BQ), F32)),
        in_specs=[SMEM_SPEC] + [VMEM_SPEC] * 4,
        out_specs=(VMEM_SPEC, VMEM_SPEC),
        scratch_shapes=[pltpu.VMEM((LANES, 2 * BQ), F32)],
        compiler_params=pltpu.CompilerParams(vmem_limit_bytes=40 * 1024 * 1024),
        cost_estimate=pl.CostEstimate(flops=20_000_000_000, bytes_accessed=5_000_000, transcendentals=20_000_000),
        name='attn_fwd',
    )(start, start, q, k, v)


def attn_backward(start, lse, q, k, v, o, do, cos_t, sin_t):
    return pl.pallas_call(
        attn_bwd_kernel,
        out_shape=jax.ShapeDtypeStruct((SEQ, 3 * LANES), BF16),
        in_specs=[SMEM_SPEC] + [VMEM_SPEC] * 9,
        out_specs=VMEM_SPEC,
        scratch_shapes=[pltpu.VMEM((SEQ, LANES), F32), pltpu.VMEM((SEQ, LANES), F32),
                        pltpu.VMEM((LANES, 2 * BQ), F32)],
        compiler_params=pltpu.CompilerParams(vmem_limit_bytes=48 * 1024 * 1024),
        cost_estimate=pl.CostEstimate(flops=50_000_000_000, bytes_accessed=12_000_000, transcendentals=20_000_000),
        name='attn_bwd',
    )(start, start, lse, q, k, v, o, do, cos_t, sin_t)


def head_kernel(x_ref, w_ref, small_ref, freq_ref, wo_ref, u_hbm, q_ref, k_ref, v_ref, cos_ref, sin_ref, all_small,
                start_ref, wo_out, x_buf, w_buf, w_ext, u_buf, small_send, small_recv, w_send, w_recv, x_send, x_recv,
                wo_send, wo_recv, u_sem):
    me = lax.axis_index('sp')
    core = lax.rem(me, 2)
    x_pos = lax.rem(me // 2, 2)
    y_pos = me // 4
    step_c, step_x, step_y = 1 - 2 * core, 2 - 4 * x_pos, 4 - 8 * y_pos
    mate, near_x, near_y, diag = me + step_c, me + step_x, me + step_y, me + step_x + step_y

    barrier = pltpu.get_barrier_semaphore()
    for n in range(1, NDEV):
        pl.semaphore_signal(barrier, inc=1, device_id=(lax.rem(me + n, NDEV),), device_id_type=pl.DeviceIdType.MESH)
    pl.semaphore_wait(barrier, NDEV - 1)

    def remote(src, dst, send_sem, recv_sem, dev):
        return pltpu.make_async_remote_copy(src_ref=src, dst_ref=dst, send_sem=send_sem, recv_sem=recv_sem,
                                            device_id=(dev,), device_id_type=pl.DeviceIdType.MESH)

    def half(ref, h):
        rows = ref.shape[0] // 2
        return ref.at[pl.ds(h * rows, rows), :]

    def x_copy(slot, src_dev, h, target, from_ref=None):
        source = half(x_buf.at[src_dev], h) if from_ref is None else half(from_ref, h)
        return remote(source, half(x_buf.at[src_dev], h), x_send.at[slot], x_recv.at[slot], target)

    def wo_copy(slot, src_dev, h, target, from_ref=None):
        source = half(wo_out.at[src_dev], h) if from_ref is None else half(from_ref, h)
        return remote(source, half(wo_out.at[src_dev], h), wo_send.at[slot], wo_recv.at[slot], target)

    def first_sends(copy, from_ref):
        return [copy(0, me, 0, near_x, from_ref), copy(3, me, 1, near_y, from_ref),
                copy(1, me, 1, near_x, from_ref), copy(2, me, 0, near_y, from_ref),
                copy(12, me, 0, mate, from_ref), copy(13, me, 1, mate, from_ref)]

    smalls = [remote(small_ref, all_small.at[me], small_send.at[n - 1], small_recv.at[n - 1], lax.rem(me + n, NDEV))
              for n in range(1, NDEV)]
    weights = [remote(w_ref.at[lax.rem(me + n, NDEV)], w_buf.at[me], w_send.at[n - 1], w_recv.at[n - 1],
                      lax.rem(me + n, NDEV)) for n in range(1, NDEV)]
    for c in smalls:
        c.start()
    for c in weights:
        c.start()
    own = first_sends(x_copy, x_ref)
    for c in own:
        c.start()

    all_small[me] = small_ref[...]
    w_buf[me] = w_ref[me]
    for c in smalls + weights:
        c.wait_recv()

    lane = lax.broadcasted_iota(jnp.int32, (LANES, LANES), 1)
    first_half = lax.rem(lane, HD) < HD // 2

    def build(i, _):
        rows = pl.ds(pl.multiple_of(i * LANES, LANES), LANES)
        w_ext[rows, 0:3 * LANES] = w_buf[i]
        for n in range(2):
            t = w_buf[i, :, n * LANES:(n + 1) * LANES].astype(F32)
            rot = jnp.where(first_half, -pltpu.roll(t, LANES - HD // 2, 1), pltpu.roll(t, HD // 2, 1))
            w_ext[rows, (3 + n) * LANES:(4 + n) * LANES] = rot.astype(BF16)
        return 0

    lax.fori_loop(0, NDEV, build, 0)
    gain1 = jnp.concatenate([all_small[n, 0:1, :] for n in range(NDEV)], axis=1)

    def process(order, src_ref, src_dev, h):
        def part(i, _):
            local = pl.ds(pl.multiple_of(h * (TOK // 2) + i * LANES, LANES), LANES)
            rows = pl.ds(pl.multiple_of(src_dev * TOK + h * (TOK // 2) + i * LANES, LANES), LANES)
            xv = src_ref[local, :].astype(F32)
            inv = lax.rsqrt(jnp.mean(xv * xv, axis=-1, keepdims=True) + NORM_EPS)
            u = (xv * inv * gain1).astype(BF16)
            u_buf[rows, :] = u
            proj = jnp.dot(u, w_ext[...], preferred_element_type=F32)
            angle = freq_ref[...] * all_small[src_dev, pl.ds(2 + 2 * h + i, 1), :]
            cos4, sin4 = jnp.cos(angle), jnp.sin(angle)
            cos_v = jnp.concatenate([cos4] * 4, axis=0).T
            sin_v = jnp.concatenate([sin4] * 4, axis=0).T
            cos_ref[rows, :] = cos_v
            sin_ref[rows, :] = sin_v
            q = (proj[:, :LANES] * cos_v + proj[:, 3 * LANES:4 * LANES] * sin_v).astype(BF16).astype(F32)
            q_ref[rows, :] = (q * (HD ** -0.5)).astype(BF16)
            k_ref[rows, :] = (proj[:, LANES:2 * LANES] * cos_v + proj[:, 4 * LANES:] * sin_v).astype(BF16)
            v_ref[rows, :] = proj[:, 2 * LANES:3 * LANES].astype(BF16)
            return 0

        lax.fori_loop(0, 2, part, 0)
        u_rows = pl.ds(pl.multiple_of(src_dev * TOK + h * (TOK // 2), TOK // 2), TOK // 2)
        out = pltpu.make_async_copy(u_buf.at[u_rows, :], u_hbm.at[u_rows, :], u_sem.at[order])
        out.start()
        return out

    pending = []
    copies = list(own)

    def arrive(copy, slot, src_dev, h):
        copy(slot, src_dev, h, mate).wait_recv()

    def pass_on(copy, slot, src_dev, h, target):
        c = copy(slot, src_dev, h, target)
        c.start()
        copies.append(c)

    def relay(copy, slot, src_dev, h):
        arrive(copy, slot, src_dev, h)
        if slot == 0:
            pass_on(copy, 4, src_dev, h, near_y)
        elif slot == 3:
            pass_on(copy, 5, src_dev, h, near_x)
        pass_on(copy, 6 + slot, src_dev, h, mate)

    def work(src_ref, src_dev, h):
        pending.append(process(len(pending), src_ref, src_dev, h))

    work(x_ref, me, 0)
    work(x_ref, me, 1)
    arrivals = [(0, near_x, 0), (3, near_y, 1), (1, near_x, 1), (2, near_y, 0), (4, diag, 0), (5, diag, 1)]
    late = [(12, mate, 0), (13, mate, 1)]
    for n, (slot, src_dev, h) in enumerate(arrivals):
        relay(x_copy, slot, src_dev, h)
        if n == 1:
            wo_own = first_sends(wo_copy, wo_ref)
            for c in wo_own:
                c.start()
            copies += wo_own
            wo_out[me] = wo_ref[...]
        if n >= 4:
            relay(wo_copy, *arrivals[n - 4])
        work(x_buf.at[src_dev], src_dev, h)
        mate_slot, mate_src, mate_h = late.pop(0)
        arrive(x_copy, mate_slot, mate_src, mate_h)
        work(x_buf.at[mate_src], mate_src, mate_h)
        late.append((6 + slot, src_dev + step_c, h))
    for n, (slot, src_dev, h) in enumerate(late):
        if n < 2:
            relay(wo_copy, *arrivals[n + 2])
        arrive(x_copy, slot, src_dev, h)
        work(x_buf.at[src_dev], src_dev, h)
    for n in range(NDEV):
        for h in range(2):
            row = jnp.concatenate([all_small[n, 2 + 2 * h:3 + 2 * h, :], all_small[n, 3 + 2 * h:4 + 2 * h, :]], axis=1)
            index = n * TOK + h * BQ + lax.broadcasted_iota(jnp.int32, (1, BQ), 1)
            first = index - row.astype(jnp.int32)
            start_ref[2 * n + h:2 * n + h + 1, :] = jnp.concatenate([first, first], axis=1)
    relay(wo_copy, *arrivals[4])
    relay(wo_copy, *arrivals[5])
    for slot, src_dev, h in [(12, mate, 0), (13, mate, 1)] + [(6 + m, d + step_c, h) for m, d, h in arrivals]:
        arrive(wo_copy, slot, src_dev, h)
    for c in pending:
        c.wait()
    for c in smalls + weights + copies:
        c.wait_send()


def head_stage(x, w_pieces, small, freq, w_o):
    dma = pltpu.SemaphoreType.DMA
    return pl.pallas_call(
        head_kernel,
        out_shape=(jax.ShapeDtypeStruct((SEQ, D), BF16),) + tuple(jax.ShapeDtypeStruct((SEQ, LANES), BF16) for _ in range(3))
        + tuple(jax.ShapeDtypeStruct((SEQ, LANES), F32) for _ in range(2))
        + (jax.ShapeDtypeStruct((NDEV, 8, LANES), F32), jax.ShapeDtypeStruct((NQ, 2 * BQ), jnp.int32),
           jax.ShapeDtypeStruct((NDEV, LANES, D), BF16)),
        in_specs=[VMEM_SPEC] * 5,
        out_specs=(pl.BlockSpec(memory_space=pl.ANY),) + (VMEM_SPEC,) * 8,
        scratch_shapes=[pltpu.VMEM((NDEV, TOK, D), BF16), pltpu.VMEM((NDEV, LANES, 3 * LANES), BF16),
                        pltpu.VMEM((D, 5 * LANES), BF16), pltpu.VMEM((SEQ, D), BF16),
                        dma((NDEV - 1,)), dma((NDEV - 1,)), dma((NDEV - 1,)), dma((NDEV - 1,)),
                        dma((14,)), dma((14,)), dma((14,)), dma((14,)), dma((16,))],
        compiler_params=pltpu.CompilerParams(collective_id=0, has_side_effects=True,
                                             vmem_limit_bytes=48 * 1024 * 1024),
        cost_estimate=pl.CostEstimate(flops=40_000_000_000, bytes_accessed=30_000_000, transcendentals=1_000_000),
        name='head_stage',
    )(x, w_pieces, small, freq, w_o)


COLS = D // 2
DN_ROWS = FF // NDEV
OUT_ROWS = DN_ROWS + LANES


def tail_kernel(mt_ref, gy_ref, ot_ref, gh_ref, d_ref, x_ref, h_ref, gz_ref, gain_ref, u_hbm, win_hbm,
                dn_out, wo_out, gw_out, gx_out, gain_out,
                mt_mate, gy_mate, ot_mate, gh_mate, part, box, d_buf, win_buf, u_buf, gw_mine, gain_mine, gain_buf,
                mate_send, mate_recv, rs_send, rs_recv, d_send, d_recv, gw_send, gw_recv, gg_send, gg_recv, win_sem, u_sem):
    me = lax.axis_index('sp')
    core = lax.rem(me, 2)
    x_pos = lax.rem(me // 2, 2)
    y_pos = me // 4
    step_c, step_x, step_y = 1 - 2 * core, 2 - 4 * x_pos, 4 - 8 * y_pos
    mate, near_x, near_y, diag = me + step_c, me + step_x, me + step_y, me + step_x + step_y

    win_copy = pltpu.make_async_copy(win_hbm, win_buf, win_sem)
    win_copy.start()
    u_copy = pltpu.make_async_copy(u_hbm, u_buf, u_sem)
    u_copy.start()

    barrier = pltpu.get_barrier_semaphore()
    for n in range(1, NDEV):
        pl.semaphore_signal(barrier, inc=1, device_id=(lax.rem(me + n, NDEV),), device_id_type=pl.DeviceIdType.MESH)
    pl.semaphore_wait(barrier, NDEV - 1)

    def remote(src, dst, send_sem, recv_sem, dev):
        return pltpu.make_async_remote_copy(src_ref=src, dst_ref=dst, send_sem=send_sem, recv_sem=recv_sem,
                                            device_id=(dev,), device_id_type=pl.DeviceIdType.MESH)

    def to_peers(src, dst, send_sem, recv_sem):
        return [remote(src.at[lax.rem(me + n, NDEV)], dst.at[me], send_sem.at[n - 1], recv_sem.at[n - 1],
                       lax.rem(me + n, NDEV)) for n in range(1, NDEV)]

    def dn_rows(dev):
        return pl.ds(pl.multiple_of(dev * DN_ROWS, 32), DN_ROWS)

    def wo_rows(dev):
        return pl.ds(pl.multiple_of(dev * LANES, LANES), LANES)

    swaps = []
    for q in range(NDEV // 2):
        dest = 2 * q + 1 - core
        swaps.append(remote(mt_ref.at[dn_rows(dest), :], mt_mate.at[q], mate_send.at[q], mate_recv.at[q], mate))
        swaps.append(remote(ot_ref.at[wo_rows(dest), :], ot_mate.at[q], mate_send.at[4 + q], mate_recv.at[4 + q], mate))
    swaps.append(remote(gy_ref, gy_mate, mate_send.at[8], mate_recv.at[8], mate))
    swaps.append(remote(gh_ref, gh_mate, mate_send.at[9], mate_recv.at[9], mate))
    for c in swaps:
        c.start()
    d_moves = to_peers(d_ref, d_buf, d_send, d_recv)
    gw_moves = to_peers(gw_mine, gw_out, gw_send, gw_recv)
    gg_moves = to_peers(gain_mine, gain_buf, gg_send, gg_recv)
    for c in d_moves:
        c.start()
    d_buf[me] = d_ref[me]
    for c in swaps:
        c.wait_recv()

    def compute(rel, dev, col):
        chip = dev // 2
        cols = pl.ds(col * COLS, COLS)
        part[rel, col, 0:DN_ROWS, :] = (
            jnp.dot(mt_ref[dn_rows(dev), :], gy_ref[:, cols], preferred_element_type=F32)
            + jnp.dot(mt_mate[chip], gy_mate[:, cols], preferred_element_type=F32))
        part[rel, col, DN_ROWS:OUT_ROWS, :] = (
            jnp.dot(ot_ref[wo_rows(dev), :], gh_ref[:, cols], preferred_element_type=F32)
            + jnp.dot(ot_mate[chip], gh_mate[:, cols], preferred_element_type=F32))

    moves = [remote(part.at[3, 0], box.at[0], rs_send.at[0], rs_recv.at[0], near_x),
             remote(part.at[3, 1], box.at[1], rs_send.at[1], rs_recv.at[1], near_y),
             remote(part.at[1, 0], box.at[2], rs_send.at[2], rs_recv.at[2], near_x),
             remote(part.at[2, 1], box.at[3], rs_send.at[3], rs_recv.at[3], near_y),
             remote(part.at[2, 0], box.at[4], rs_send.at[4], rs_recv.at[4], near_y),
             remote(part.at[1, 1], box.at[5], rs_send.at[5], rs_recv.at[5], near_x)]
    compute(3, diag, 0)
    moves[0].start()
    compute(3, diag, 1)
    moves[1].start()
    compute(1, near_x, 0)
    moves[2].start()
    compute(2, near_y, 1)
    moves[3].start()
    compute(2, near_y, 0)
    compute(1, near_x, 1)
    u_copy.wait()

    def grad_win_piece(n, _):
        cols = pl.ds(pl.multiple_of(n * LANES, LANES), LANES)
        total = dot_tn(u_buf[0:TOK, cols], d_ref[0])
        for g in range(1, NDEV):
            total = total + dot_tn(u_buf[g * TOK:(g + 1) * TOK, cols], d_ref[g])
        gw_mine[n] = total
        return 0

    lax.fori_loop(0, NDEV, grad_win_piece, 0)
    for c in gw_moves:
        c.start()
    gw_out[me] = gw_mine[me]
    compute(0, me, 0)
    compute(0, me, 1)

    def add_box(rel, col, n):
        def rows_add(i, _):
            rows = pl.ds(pl.multiple_of(i * 32, 32), 32)
            part[rel, col, rows, :] += box[n, rows, :]
            return 0

        lax.fori_loop(0, OUT_ROWS // 32, rows_add, 0)

    moves[0].wait_recv()
    add_box(2, 0, 0)
    moves[4].start()
    moves[1].wait_recv()
    add_box(1, 1, 1)
    moves[5].start()

    for c in d_moves:
        c.wait_recv()
    win_copy.wait()
    gain1 = gain_ref[...]

    def grad_rows(i, carry):
        acc, acc2 = carry
        rows = pl.ds(pl.multiple_of(i * LANES, LANES), LANES)
        gu = dot_nt(d_buf[0, rows, :], win_buf[:, 0:3 * LANES])
        for g in range(1, NDEV):
            gu = gu + dot_nt(d_buf[g, rows, :], win_buf[:, g * 3 * LANES:(g + 1) * 3 * LANES])
        gu = gu.astype(BF16).astype(F32)
        xv = x_ref[rows, :].astype(F32)
        inv = lax.rsqrt(jnp.mean(xv * xv, axis=-1, keepdims=True) + NORM_EPS)
        normed = xv * inv
        acc = acc + jnp.sum(gu * normed, axis=0, keepdims=True)
        scaled = gu * gain1
        mean_term = jnp.mean(scaled * normed, axis=-1, keepdims=True)
        gx_out[rows, :] = (gh_ref[rows, :].astype(F32) + inv * (scaled - normed * mean_term)).astype(BF16)
        hv = h_ref[rows, :].astype(F32)
        normed2 = hv * lax.rsqrt(jnp.mean(hv * hv, axis=-1, keepdims=True) + NORM_EPS)
        acc2 = acc2 + jnp.sum(gz_ref[rows, :].astype(F32) * normed2, axis=0, keepdims=True)
        return acc, acc2

    gg1, gg2 = lax.fori_loop(0, TOK // LANES, grad_rows, (jnp.zeros((1, D), F32), jnp.zeros((1, D), F32)))
    for n in range(NDEV):
        piece = slice(n * LANES, (n + 1) * LANES)
        gain_mine[n] = jnp.concatenate([gg1[:, piece], gg2[:, piece], jnp.zeros((6, LANES), F32)], axis=0)
    for c in gg_moves:
        c.start()
    gain_buf[me] = gain_mine[me]

    moves[2].wait_recv()
    add_box(0, 0, 2)
    moves[3].wait_recv()
    add_box(0, 1, 3)
    for c in gg_moves:
        c.wait_recv()
    total = gain_buf[0]
    for n in range(1, NDEV):
        total = total + gain_buf[n]
    gain_out[...] = total
    for col in range(2):
        moves[4 + col].wait_recv()

        def finish(i, _):
            rows = pl.ds(pl.multiple_of(i * 32, 32), 32)
            dn_out[rows, col * COLS:(col + 1) * COLS] = part[0, col, rows, :] + box[4 + col, rows, :]
            return 0

        lax.fori_loop(0, DN_ROWS // 32, finish, 0)
        wo_out[:, col * COLS:(col + 1) * COLS] = part[0, col, DN_ROWS:OUT_ROWS, :] + box[4 + col, DN_ROWS:OUT_ROWS, :]
    for c in gw_moves:
        c.wait_recv()
    for c in swaps + d_moves + gw_moves + gg_moves + moves:
        c.wait_send()


def tail_stage(m_t, grad_y, o_t, grad_h, d_qkv, x, h_res, grad_z, gain1, u_all, win_full):
    dma = pltpu.SemaphoreType.DMA
    peers = (NDEV - 1,)
    return pl.pallas_call(
        tail_kernel,
        out_shape=(jax.ShapeDtypeStruct((DN_ROWS, D), F32), jax.ShapeDtypeStruct((LANES, D), F32),
                   jax.ShapeDtypeStruct((NDEV, LANES, 3 * LANES), F32), jax.ShapeDtypeStruct((TOK, D), BF16),
                   jax.ShapeDtypeStruct((8, LANES), F32)),
        in_specs=[VMEM_SPEC] * 9 + [pl.BlockSpec(memory_space=pl.ANY)] * 2,
        out_specs=(VMEM_SPEC,) * 5,
        scratch_shapes=[pltpu.VMEM((4, DN_ROWS, TOK), BF16), pltpu.VMEM((TOK, D), BF16),
                        pltpu.VMEM((4, LANES, TOK), BF16), pltpu.VMEM((TOK, D), BF16),
                        pltpu.VMEM((4, 2, OUT_ROWS, COLS), F32), pltpu.VMEM((6, OUT_ROWS, COLS), F32),
                        pltpu.VMEM((NDEV, TOK, 3 * LANES), BF16), pltpu.VMEM((D, 3 * D), BF16),
                        pltpu.VMEM((SEQ, D), BF16), pltpu.VMEM((NDEV, LANES, 3 * LANES), F32),
                        pltpu.VMEM((NDEV, 8, LANES), F32), pltpu.VMEM((NDEV, 8, LANES), F32),
                        dma((10,)), dma((10,)), dma((6,)), dma((6,)), dma(peers), dma(peers),
                        dma(peers), dma(peers), dma(peers), dma(peers), dma, dma],
        compiler_params=pltpu.CompilerParams(collective_id=1, has_side_effects=True,
                                             vmem_limit_bytes=60 * 1024 * 1024),
        cost_estimate=pl.CostEstimate(flops=60_000_000_000, bytes_accessed=60_000_000, transcendentals=1_000),
        name='tail_stage',
    )(m_t, grad_y, o_t, grad_h, d_qkv, x, h_res, grad_z, gain1, u_all, win_full)


def pair_grad_kernel(z_ref, g_ref, out_hbm, z_mate, g_mate, zt, acc, z_send, z_recv, g_send, g_recv, out_sem):
    me = lax.axis_index('sp')
    core = lax.rem(me, 2)
    mate = me + 1 - 2 * core
    blocks = g_ref.shape[1] // COLS
    barrier = pltpu.get_barrier_semaphore()
    pl.semaphore_signal(barrier, inc=1, device_id=(mate,), device_id_type=pl.DeviceIdType.MESH)
    pl.semaphore_wait(barrier, 1)

    def swap(src, dst, send_sem, recv_sem):
        return pltpu.make_async_remote_copy(src_ref=src, dst_ref=dst, send_sem=send_sem, recv_sem=recv_sem,
                                            device_id=(mate,), device_id_type=pl.DeviceIdType.MESH)

    def block(b):
        return pl.ds(pl.multiple_of(b * COLS, COLS), COLS)

    def g_swap(b):
        return swap(g_ref.at[:, block(b)], g_mate.at[:, block(b)], g_send.at[b], g_recv.at[b])

    def out_copy(b):
        slot = lax.rem(b, 2)
        return pltpu.make_async_copy(acc.at[slot], out_hbm.at[:, block(b)], out_sem.at[slot])

    z_swap = swap(z_ref, z_mate, z_send, z_recv)
    z_swap.start()

    def start_swap(b, _):
        g_swap(b).start()
        return 0

    lax.fori_loop(0, blocks, start_swap, 0)

    def dest_cols(q):
        return pl.ds(pl.multiple_of((2 * q + core) * LANES, LANES), LANES)

    for q in range(NDEV // 2):
        zt[q * LANES:(q + 1) * LANES, 0:TOK] = z_ref[:, dest_cols(q)].T
    z_swap.wait_recv()
    for q in range(NDEV // 2):
        zt[q * LANES:(q + 1) * LANES, TOK:2 * TOK] = z_mate[:, dest_cols(q)].T

    def one_block(b, _):
        slot = lax.rem(b, 2)

        @pl.when(b >= 2)
        def _():
            out_copy(b - 2).wait()

        g_swap(b).wait_recv()
        acc[slot] = (jnp.dot(zt[:, 0:TOK], g_ref[:, block(b)], preferred_element_type=F32)
                     + jnp.dot(zt[:, TOK:2 * TOK], g_mate[:, block(b)], preferred_element_type=F32))
        out_copy(b).start()
        return 0

    lax.fori_loop(0, blocks, one_block, 0)
    out_copy(blocks - 2).wait()
    out_copy(blocks - 1).wait()

    def end_swap(b, _):
        g_swap(b).wait_send()
        return 0

    lax.fori_loop(0, blocks, end_swap, 0)
    z_swap.wait_send()


def pair_grad(z, grad_gu):
    dma = pltpu.SemaphoreType.DMA
    width = grad_gu.shape[1]
    blocks = width // COLS
    return pl.pallas_call(
        pair_grad_kernel,
        out_shape=jax.ShapeDtypeStruct((D // 2, width), F32),
        in_specs=[VMEM_SPEC] * 2,
        out_specs=pl.BlockSpec(memory_space=pl.ANY),
        scratch_shapes=[pltpu.VMEM((TOK, D), BF16), pltpu.VMEM((TOK, width), BF16),
                        pltpu.VMEM((D // 2, 2 * TOK), BF16), pltpu.VMEM((2, D // 2, COLS), F32),
                        dma, dma, dma((blocks,)), dma((blocks,)), dma((2,))],
        compiler_params=pltpu.CompilerParams(collective_id=2, has_side_effects=True,
                                             vmem_limit_bytes=60 * 1024 * 1024),
        cost_estimate=pl.CostEstimate(flops=6_000_000_000, bytes_accessed=20_000_000, transcendentals=0),
        name='pair_grad',
    )(z, grad_gu)


def rms_back(grad_out, normed, inv_rms):
    mean_term = jnp.mean(grad_out * normed, axis=-1, keepdims=True)
    return inv_rms * (grad_out - normed * mean_term)


def solution(mesh):
    row_spec = P('sp', None)
    cube_spec = P('sp', None, None)
    vec_spec = P('sp')

    def gather(t):
        return lax.all_gather(t, 'sp', axis=0, tiled=True)

    def exchange(t):
        return lax.all_to_all(t, 'sp', 0, 0)

    def local_layer(x, seg_ids, positions, grad_y, norm1_gain, w_q, w_k, w_v, w_o, norm2_gain, w_gate, w_up, w_down):
        half = HD // 2
        inv_freq = (ROPE_BASE ** (-jnp.arange(half, dtype=F32) * 2.0 / HD))[:, None]
        freq = jnp.broadcast_to(inv_freq, (half, LANES))
        small = jnp.concatenate([norm1_gain.astype(F32)[None, :], norm2_gain.astype(F32)[None, :],
                                 positions.astype(F32).reshape(4, LANES), jnp.zeros((2, LANES), F32)])
        w_in = jnp.concatenate([t.reshape(LANES, NDEV, LANES) for t in (w_q, w_k, w_v)], axis=2)
        u_all, q, k, v, cos_t, sin_t, small, start2, wo_full = head_stage(
            x, w_in.transpose(1, 0, 2), small, freq, w_o.reshape(LANES, D))
        wo_full = wo_full.reshape(D, D)
        gain1 = small[:, 0].reshape(1, D)
        gain2 = small[:, 1].reshape(D)
        o_own, lse = attn_forward(start2, q, k, v)
        o_heads = exchange(o_own.reshape(NDEV, TOK, LANES))
        o_loc = o_heads.transpose(1, 0, 2).reshape(TOK, D)
        o_t = o_heads.transpose(0, 2, 1).reshape(D, TOK)

        wd_full = gather(w_down)
        wgu_full = gather(jnp.concatenate([w_gate, w_up], axis=1))
        win_full = gather(w_in.reshape(LANES, 3 * D))

        x_wide = x.astype(F32)
        h_res = (x_wide + jnp.dot(o_loc, wo_full, preferred_element_type=F32)).astype(BF16)
        h_wide = h_res.astype(F32)
        inv_rms2 = lax.rsqrt(jnp.mean(h_wide * h_wide, axis=-1, keepdims=True) + NORM_EPS)
        normed2 = h_wide * inv_rms2
        z_norm = (normed2 * gain2).astype(BF16)
        gate_up = jnp.dot(z_norm, wgu_full, preferred_element_type=F32)
        gate_pre, up_pre = gate_up[:, :FF], gate_up[:, FF:]
        gate_sig = jax.nn.sigmoid(gate_pre)
        gate_act = gate_pre * gate_sig
        mlp_act = (gate_act * up_pre).astype(BF16)

        grad_act = dot_nt(grad_y, wd_full).astype(BF16).astype(F32)
        grad_gate = (grad_act * up_pre * gate_sig * (1.0 + gate_pre * (1.0 - gate_sig))).astype(BF16)
        grad_up = (grad_act * gate_act).astype(BF16)
        grad_gu = jnp.concatenate([grad_gate, grad_up], axis=1)
        grad_wgu = lax.psum_scatter(pair_grad(z_norm, grad_gu), 'sp', scatter_dimension=0, tiled=True,
                                    axis_index_groups=[[0, 2, 4, 6], [1, 3, 5, 7]])
        grad_z_b = lax.optimization_barrier(dot_nt(grad_gu, wgu_full).astype(BF16))
        grad_z = grad_z_b.astype(F32)
        grad_h = (grad_y.astype(F32) + rms_back(grad_z * gain2, normed2, inv_rms2)).astype(BF16)
        grad_o = dot_nt(grad_h, wo_full).astype(BF16)
        grad_o = exchange(grad_o.reshape(TOK, NDEV, LANES).transpose(1, 0, 2)).reshape(SEQ, LANES)
        y = (h_wide + jnp.dot(mlp_act, wd_full, preferred_element_type=F32)).astype(BF16)

        d_qkv = attn_backward(start2, lse, q, k, v, o_own, grad_o, cos_t, sin_t)
        grad_wdown, grad_wo, grad_win, grad_x, grad_gains = tail_stage(
            mlp_act.T, grad_y, o_t, grad_h, d_qkv.reshape(NDEV, TOK, 3 * LANES), x, h_res, grad_z_b,
            gain1, u_all, win_full)
        grad_q, grad_k, grad_v = (grad_win[:, :, n * LANES:(n + 1) * LANES].transpose(1, 0, 2).reshape(LANES, 16, HD)
                                  for n in range(3))
        return (y, grad_x, grad_gains[0], grad_q, grad_k, grad_v, grad_wo.reshape(2, HD, D),
                grad_gains[1], grad_wgu[:, :FF], grad_wgu[:, FF:], grad_wdown)

    return jax.shard_map(
        local_layer, mesh=mesh,
        in_specs=(row_spec, vec_spec, vec_spec, row_spec, vec_spec, cube_spec, cube_spec, cube_spec, cube_spec,
                  vec_spec, row_spec, row_spec, row_spec),
        out_specs=(row_spec, row_spec, vec_spec, cube_spec, cube_spec, cube_spec, cube_spec, vec_spec,
                   row_spec, row_spec, row_spec),
        check_vma=False)
```

```python
import jax
import jax.numpy as jnp
from jax import lax
from jax.experimental import pallas as pl
from jax.experimental.pallas import tpu as pltpu
from jax.sharding import PartitionSpec as P


NORM_EPS = 1e-5
ROPE_BASE = 10000.0
SEQ = 4096
D = 1024
HD = 64
FF = 2816
NDEV = 8
TOK = SEQ // NDEV
LANES = 128
BQ = 256
BK = 512
NQ = SEQ // BQ
NEG = -1e30
F32 = jnp.float32
BF16 = jnp.bfloat16


def dot_nt(a, b):
    return lax.dot_general(a, b, (((1,), (1,)), ((), ())), preferred_element_type=F32)


def dot_tn(a, b):
    return lax.dot_general(a, b, (((0,), (0,)), ((), ())), preferred_element_type=F32)


def head_pair(t):
    lane = lax.broadcasted_iota(jnp.int32, (1, LANES), 1)
    low = (lane < HD).astype(F32).astype(BF16)
    high = (lane >= HD).astype(F32).astype(BF16)
    return jnp.concatenate([t * low, t * high], axis=0)


def rope_back_tile(t, cos_t, sin_t):
    lane = lax.broadcasted_iota(jnp.int32, t.shape, 1)
    first_half = lax.rem(lane, HD) < HD // 2
    rotated = jnp.where(first_half, -pltpu.roll(t, LANES - HD // 2, 1), pltpu.roll(t, HD // 2, 1))
    return t * cos_t - rotated * sin_t


def attn_fwd_kernel(lo_ref, start_ref, q_ref, k_ref, v_ref, o_ref, lse_ref, acc_ref):
    q_iota = lax.rem(lax.broadcasted_iota(jnp.int32, (1, 2 * BQ), 1), BQ)

    def q_block(i, _):
        q_start = pl.multiple_of(i * BQ, BQ)
        q2 = head_pair(q_ref[pl.ds(q_start, BQ), :])
        first = start_ref[pl.ds(i, 1), :]
        q_index = q_start + q_iota
        acc_ref[...] = jnp.zeros_like(acc_ref)

        def k_block(j, carry):
            m_old, l_old = carry
            k_start = pl.multiple_of(j * BK, BK)
            k = k_ref[pl.ds(k_start, BK), :]
            v = v_ref[pl.ds(k_start, BK), :]
            s = dot_nt(k, q2)
            k_index = k_start + lax.broadcasted_iota(jnp.int32, s.shape, 0)
            s = jnp.where((k_index >= first) & (k_index <= q_index), s, NEG)
            m_new = jnp.maximum(m_old, jnp.max(s, axis=0, keepdims=True))
            p = jnp.exp(s - m_new)
            alpha = jnp.exp(m_old - m_new)
            l_new = alpha * l_old + jnp.sum(p, axis=0, keepdims=True)
            acc_ref[...] = acc_ref[...] * alpha + dot_tn(v, p.astype(BF16))
            return m_new, l_new

        init = (jnp.full((1, 2 * BQ), NEG, F32), jnp.zeros((1, 2 * BQ), F32))
        m_fin, l_fin = lax.fori_loop(lax.div(lo_ref[i, 0], BK), (q_start + BQ - 1) // BK + 1, k_block, init)
        lse_ref[pl.ds(i, 1), :] = m_fin + jnp.log(l_fin)
        out = acc_ref[...] * (1.0 / l_fin)
        out = jnp.concatenate([out[:HD, :BQ], out[HD:, BQ:]], axis=0)
        o_ref[pl.ds(q_start, BQ), :] = out.T.astype(BF16)
        return 0

    lax.fori_loop(0, NQ, q_block, 0)


def attn_bwd_kernel(lo_ref, start_ref, lse_ref, q_ref, k_ref, v_ref, o_ref, do_ref, cos_ref, sin_ref,
                    out_ref, dk_acc, dv_acc, dq_acc):
    q_iota = lax.rem(lax.broadcasted_iota(jnp.int32, (1, 2 * BQ), 1), BQ)
    dk_acc[...] = jnp.zeros_like(dk_acc)
    dv_acc[...] = jnp.zeros_like(dv_acc)

    def q_block(i, _):
        q_start = pl.multiple_of(i * BQ, BQ)
        q2 = head_pair(q_ref[pl.ds(q_start, BQ), :])
        do = do_ref[pl.ds(q_start, BQ), :]
        do2 = head_pair(do)
        prod = (do.astype(F32) * o_ref[pl.ds(q_start, BQ), :].astype(F32)).T
        delta = jnp.concatenate([jnp.sum(prod[:HD], axis=0, keepdims=True),
                                 jnp.sum(prod[HD:], axis=0, keepdims=True)], axis=1)
        first = start_ref[pl.ds(i, 1), :]
        lse = lse_ref[pl.ds(i, 1), :]
        q_index = q_start + q_iota
        dq_acc[...] = jnp.zeros_like(dq_acc)

        def k_block(j, _):
            k_start = pl.multiple_of(j * BK, BK)
            k = k_ref[pl.ds(k_start, BK), :]
            v = v_ref[pl.ds(k_start, BK), :]
            s = dot_nt(k, q2)
            k_index = k_start + lax.broadcasted_iota(jnp.int32, s.shape, 0)
            s = jnp.where((k_index >= first) & (k_index <= q_index), s, NEG)
            p = jnp.exp(s - lse)
            dp = dot_nt(v, do2).astype(BF16).astype(F32)
            ds = (p * (dp - delta)).astype(BF16)
            dv_acc[pl.ds(k_start, BK), :] += jnp.dot(p.astype(BF16), do2, preferred_element_type=F32)
            dk_acc[pl.ds(k_start, BK), :] += jnp.dot(ds, q2, preferred_element_type=F32)
            dq_acc[...] += dot_tn(k, ds)
            return 0

        lax.fori_loop(lax.div(lo_ref[i, 0], BK), (q_start + BQ - 1) // BK + 1, k_block, 0)
        dq = jnp.concatenate([dq_acc[:HD, :BQ], dq_acc[HD:, BQ:]], axis=0).T * (HD ** -0.5)
        rows = pl.ds(q_start, BQ)
        dq = dq.astype(BF16).astype(F32)
        out_ref[rows, 0:LANES] = rope_back_tile(dq, cos_ref[rows, :], sin_ref[rows, :]).astype(BF16)
        return 0

    lax.fori_loop(0, NQ, q_block, 0)

    def finish(i, _):
        rows = pl.ds(pl.multiple_of(i * BQ, BQ), BQ)
        dk = dk_acc[rows, :].astype(BF16).astype(F32)
        out_ref[rows, LANES:2 * LANES] = rope_back_tile(dk, cos_ref[rows, :], sin_ref[rows, :]).astype(BF16)
        out_ref[rows, 2 * LANES:3 * LANES] = dv_acc[rows, :].astype(BF16)
        return 0

    lax.fori_loop(0, NQ, finish, 0)


VMEM_SPEC = pl.BlockSpec(memory_space=pltpu.VMEM)
SMEM_SPEC = pl.BlockSpec(memory_space=pltpu.SMEM)


def attn_forward(start, q, k, v):
    return pl.pallas_call(
        attn_fwd_kernel,
        out_shape=(jax.ShapeDtypeStruct((SEQ, LANES), BF16), jax.ShapeDtypeStruct((NQ, 2 * BQ), F32)),
        in_specs=[SMEM_SPEC] + [VMEM_SPEC] * 4,
        out_specs=(VMEM_SPEC, VMEM_SPEC),
        scratch_shapes=[pltpu.VMEM((LANES, 2 * BQ), F32)],
        compiler_params=pltpu.CompilerParams(vmem_limit_bytes=40 * 1024 * 1024),
        cost_estimate=pl.CostEstimate(flops=20_000_000_000, bytes_accessed=5_000_000, transcendentals=20_000_000),
        name='attn_fwd',
    )(start, start, q, k, v)


def attn_backward(start, lse, q, k, v, o, do, cos_t, sin_t):
    return pl.pallas_call(
        attn_bwd_kernel,
        out_shape=jax.ShapeDtypeStruct((SEQ, 3 * LANES), BF16),
        in_specs=[SMEM_SPEC] + [VMEM_SPEC] * 9,
        out_specs=VMEM_SPEC,
        scratch_shapes=[pltpu.VMEM((SEQ, LANES), F32), pltpu.VMEM((SEQ, LANES), F32),
                        pltpu.VMEM((LANES, 2 * BQ), F32)],
        compiler_params=pltpu.CompilerParams(vmem_limit_bytes=48 * 1024 * 1024),
        cost_estimate=pl.CostEstimate(flops=50_000_000_000, bytes_accessed=12_000_000, transcendentals=20_000_000),
        name='attn_bwd',
    )(start, start, lse, q, k, v, o, do, cos_t, sin_t)


def head_kernel(x_ref, w_ref, small_ref, freq_ref, wo_ref, u_hbm, q_ref, k_ref, v_ref, cos_ref, sin_ref, all_small,
                start_ref, wo_out, x_buf, w_buf, w_ext, u_buf, small_send, small_recv, w_send, w_recv, x_send, x_recv,
                wo_send, wo_recv, u_sem):
    me = lax.axis_index('sp')
    core = lax.rem(me, 2)
    x_pos = lax.rem(me // 2, 2)
    y_pos = me // 4
    step_c, step_x, step_y = 1 - 2 * core, 2 - 4 * x_pos, 4 - 8 * y_pos
    mate, near_x, near_y, diag = me + step_c, me + step_x, me + step_y, me + step_x + step_y

    barrier = pltpu.get_barrier_semaphore()
    for n in range(1, NDEV):
        pl.semaphore_signal(barrier, inc=1, device_id=(lax.rem(me + n, NDEV),), device_id_type=pl.DeviceIdType.MESH)
    pl.semaphore_wait(barrier, NDEV - 1)

    def remote(src, dst, send_sem, recv_sem, dev):
        return pltpu.make_async_remote_copy(src_ref=src, dst_ref=dst, send_sem=send_sem, recv_sem=recv_sem,
                                            device_id=(dev,), device_id_type=pl.DeviceIdType.MESH)

    def half(ref, h):
        rows = ref.shape[0] // 2
        return ref.at[pl.ds(h * rows, rows), :]

    def x_copy(slot, src_dev, h, target, from_ref=None):
        source = half(x_buf.at[src_dev], h) if from_ref is None else half(from_ref, h)
        return remote(source, half(x_buf.at[src_dev], h), x_send.at[slot], x_recv.at[slot], target)

    def wo_copy(slot, src_dev, h, target, from_ref=None):
        source = half(wo_out.at[src_dev], h) if from_ref is None else half(from_ref, h)
        return remote(source, half(wo_out.at[src_dev], h), wo_send.at[slot], wo_recv.at[slot], target)

    def first_sends(copy, from_ref):
        return [copy(0, me, 0, near_x, from_ref), copy(3, me, 1, near_y, from_ref),
                copy(1, me, 1, near_x, from_ref), copy(2, me, 0, near_y, from_ref),
                copy(12, me, 0, mate, from_ref), copy(13, me, 1, mate, from_ref)]

    smalls = [remote(small_ref, all_small.at[me], small_send.at[n - 1], small_recv.at[n - 1], lax.rem(me + n, NDEV))
              for n in range(1, NDEV)]
    weights = [remote(w_ref.at[lax.rem(me + n, NDEV)], w_buf.at[me], w_send.at[n - 1], w_recv.at[n - 1],
                      lax.rem(me + n, NDEV)) for n in range(1, NDEV)]
    for c in smalls:
        c.start()
    for c in weights:
        c.start()
    own = first_sends(x_copy, x_ref)
    for c in own:
        c.start()

    all_small[me] = small_ref[...]
    w_buf[me] = w_ref[me]
    for c in smalls + weights:
        c.wait_recv()

    half_head = HD // 2
    for n in range(NDEV):
        cols = slice(n * LANES, (n + 1) * LANES)
        w_ext[0:3 * LANES, cols] = w_buf[n]
        for m in range(2):
            t = w_buf[n, m * LANES:(m + 1) * LANES, :].astype(F32)
            rot = jnp.concatenate([-t[half_head:HD], t[:half_head], -t[HD + half_head:], t[HD:HD + half_head]], axis=0)
            w_ext[(3 + m) * LANES:(4 + m) * LANES, cols] = rot.astype(BF16)
    gain1 = jnp.concatenate([all_small[n, 0:1, :] for n in range(NDEV)], axis=1)

    def process(order, src_ref, src_dev, h):
        def part(i, _):
            local = pl.ds(pl.multiple_of(h * (TOK // 2) + i * LANES, LANES), LANES)
            rows = pl.ds(pl.multiple_of(src_dev * TOK + h * (TOK // 2) + i * LANES, LANES), LANES)
            xv = src_ref[local, :].astype(F32)
            inv = lax.rsqrt(jnp.mean(xv * xv, axis=-1, keepdims=True) + NORM_EPS)
            u = (xv * inv * gain1).astype(BF16)
            u_buf[rows, :] = u
            proj = dot_nt(u, w_ext[...])
            angle = freq_ref[...] * all_small[src_dev, pl.ds(2 + 2 * h + i, 1), :]
            cos4, sin4 = jnp.cos(angle), jnp.sin(angle)
            cos_v = jnp.concatenate([cos4] * 4, axis=0).T
            sin_v = jnp.concatenate([sin4] * 4, axis=0).T
            cos_ref[rows, :] = cos_v
            sin_ref[rows, :] = sin_v
            q = (proj[:, :LANES] * cos_v + proj[:, 3 * LANES:4 * LANES] * sin_v).astype(BF16).astype(F32)
            q_ref[rows, :] = (q * (HD ** -0.5)).astype(BF16)
            k_ref[rows, :] = (proj[:, LANES:2 * LANES] * cos_v + proj[:, 4 * LANES:] * sin_v).astype(BF16)
            v_ref[rows, :] = proj[:, 2 * LANES:3 * LANES].astype(BF16)
            return 0

        lax.fori_loop(0, 2, part, 0)
        u_rows = pl.ds(pl.multiple_of(src_dev * TOK + h * (TOK // 2), TOK // 2), TOK // 2)
        out = pltpu.make_async_copy(u_buf.at[u_rows, :], u_hbm.at[u_rows, :], u_sem.at[order])
        out.start()
        return out

    pending = []
    copies = list(own)

    def arrive(copy, slot, src_dev, h):
        copy(slot, src_dev, h, mate).wait_recv()

    def pass_on(copy, slot, src_dev, h, target):
        c = copy(slot, src_dev, h, target)
        c.start()
        copies.append(c)

    def relay(copy, slot, src_dev, h):
        arrive(copy, slot, src_dev, h)
        if slot == 0:
            pass_on(copy, 4, src_dev, h, near_y)
        elif slot == 3:
            pass_on(copy, 5, src_dev, h, near_x)
        pass_on(copy, 6 + slot, src_dev, h, mate)

    def work(src_ref, src_dev, h):
        pending.append(process(len(pending), src_ref, src_dev, h))

    work(x_ref, me, 0)
    work(x_ref, me, 1)
    arrivals = [(0, near_x, 0), (3, near_y, 1), (1, near_x, 1), (2, near_y, 0), (4, diag, 0), (5, diag, 1)]
    late = [(12, mate, 0), (13, mate, 1)]
    for n, (slot, src_dev, h) in enumerate(arrivals):
        relay(x_copy, slot, src_dev, h)
        if n == 1:
            wo_own = first_sends(wo_copy, wo_ref)
            for c in wo_own:
                c.start()
            copies += wo_own
            wo_out[me] = wo_ref[...]
        if n >= 4:
            relay(wo_copy, *arrivals[n - 4])
        work(x_buf.at[src_dev], src_dev, h)
        mate_slot, mate_src, mate_h = late.pop(0)
        arrive(x_copy, mate_slot, mate_src, mate_h)
        work(x_buf.at[mate_src], mate_src, mate_h)
        late.append((6 + slot, src_dev + step_c, h))
    for n, (slot, src_dev, h) in enumerate(late):
        if n < 2:
            relay(wo_copy, *arrivals[n + 2])
        arrive(x_copy, slot, src_dev, h)
        work(x_buf.at[src_dev], src_dev, h)
    for n in range(NDEV):
        for h in range(2):
            row = jnp.concatenate([all_small[n, 2 + 2 * h:3 + 2 * h, :], all_small[n, 3 + 2 * h:4 + 2 * h, :]], axis=1)
            index = n * TOK + h * BQ + lax.broadcasted_iota(jnp.int32, (1, BQ), 1)
            first = index - row.astype(jnp.int32)
            start_ref[2 * n + h:2 * n + h + 1, :] = jnp.concatenate([first, first], axis=1)
    relay(wo_copy, *arrivals[4])
    relay(wo_copy, *arrivals[5])
    for slot, src_dev, h in [(12, mate, 0), (13, mate, 1)] + [(6 + m, d + step_c, h) for m, d, h in arrivals]:
        arrive(wo_copy, slot, src_dev, h)
    for c in pending:
        c.wait()
    for c in smalls + weights + copies:
        c.wait_send()


def head_stage(x, w_pieces, small, freq, w_o):
    dma = pltpu.SemaphoreType.DMA
    return pl.pallas_call(
        head_kernel,
        out_shape=(jax.ShapeDtypeStruct((SEQ, D), BF16),) + tuple(jax.ShapeDtypeStruct((SEQ, LANES), BF16) for _ in range(3))
        + tuple(jax.ShapeDtypeStruct((SEQ, LANES), F32) for _ in range(2))
        + (jax.ShapeDtypeStruct((NDEV, 8, LANES), F32), jax.ShapeDtypeStruct((NQ, 2 * BQ), jnp.int32),
           jax.ShapeDtypeStruct((NDEV, LANES, D), BF16)),
        in_specs=[VMEM_SPEC] * 5,
        out_specs=(pl.BlockSpec(memory_space=pl.ANY),) + (VMEM_SPEC,) * 8,
        scratch_shapes=[pltpu.VMEM((NDEV, TOK, D), BF16), pltpu.VMEM((NDEV, 3 * LANES, LANES), BF16),
                        pltpu.VMEM((5 * LANES, D), BF16), pltpu.VMEM((SEQ, D), BF16),
                        dma((NDEV - 1,)), dma((NDEV - 1,)), dma((NDEV - 1,)), dma((NDEV - 1,)),
                        dma((14,)), dma((14,)), dma((14,)), dma((14,)), dma((16,))],
        compiler_params=pltpu.CompilerParams(collective_id=0, has_side_effects=True,
                                             vmem_limit_bytes=48 * 1024 * 1024),
        cost_estimate=pl.CostEstimate(flops=40_000_000_000, bytes_accessed=30_000_000, transcendentals=1_000_000),
        name='head_stage',
    )(x, w_pieces, small, freq, w_o)


COLS = D // 2
DN_ROWS = FF // NDEV
OUT_ROWS = DN_ROWS + LANES


def tail_kernel(mt_ref, gy_ref, ot_ref, gh_ref, d_ref, x_ref, h_ref, gz_ref, gain_ref, u_hbm, win_hbm,
                dn_out, wo_out, gq_out, gk_out, gv_out, gx_out, gain_out,
                mt_mate, gy_mate, ot_mate, gh_mate, part, box, d_buf, win_buf, u_buf, gw_acc, gw_in, gain_mine, gain_buf,
                mate_send, mate_recv, rs_send, rs_recv, d_send, d_recv, gw_send, gw_recv, gg_send, gg_recv, win_send, win_recv, win_sem, u_sem):
    me = lax.axis_index('sp')
    core = lax.rem(me, 2)
    x_pos = lax.rem(me // 2, 2)
    y_pos = me // 4
    step_c, step_x, step_y = 1 - 2 * core, 2 - 4 * x_pos, 4 - 8 * y_pos
    mate, near_x, near_y, diag = me + step_c, me + step_x, me + step_y, me + step_x + step_y

    def win_part(q):
        return win_buf.at[:, pl.ds(pl.multiple_of((2 * q + core) * LANES, LANES), LANES)]

    win_copies = [pltpu.make_async_copy(win_hbm.at[q], win_part(q), win_sem.at[q]) for q in range(NDEV // 2)]
    for c in win_copies:
        c.start()
    u_copy = pltpu.make_async_copy(u_hbm, u_buf, u_sem)
    u_copy.start()

    barrier = pltpu.get_barrier_semaphore()
    for n in range(1, NDEV):
        pl.semaphore_signal(barrier, inc=1, device_id=(lax.rem(me + n, NDEV),), device_id_type=pl.DeviceIdType.MESH)
    pl.semaphore_wait(barrier, NDEV - 1)

    def remote(src, dst, send_sem, recv_sem, dev):
        return pltpu.make_async_remote_copy(src_ref=src, dst_ref=dst, send_sem=send_sem, recv_sem=recv_sem,
                                            device_id=(dev,), device_id_type=pl.DeviceIdType.MESH)

    def to_peers(src, dst, send_sem, recv_sem):
        return [remote(src.at[lax.rem(me + n, NDEV)], dst.at[me], send_sem.at[n - 1], recv_sem.at[n - 1],
                       lax.rem(me + n, NDEV)) for n in range(1, NDEV)]

    def dn_rows(dev):
        return pl.ds(pl.multiple_of(dev * DN_ROWS, 32), DN_ROWS)

    def wo_rows(dev):
        return pl.ds(pl.multiple_of(dev * LANES, LANES), LANES)

    swaps = []
    for q in range(NDEV // 2):
        dest = 2 * q + 1 - core
        swaps.append(remote(mt_ref.at[dn_rows(dest), :], mt_mate.at[q], mate_send.at[q], mate_recv.at[q], mate))
        swaps.append(remote(ot_ref.at[wo_rows(dest), :], ot_mate.at[q], mate_send.at[4 + q], mate_recv.at[4 + q], mate))
    swaps.append(remote(gy_ref, gy_mate, mate_send.at[8], mate_recv.at[8], mate))
    swaps.append(remote(gh_ref, gh_mate, mate_send.at[9], mate_recv.at[9], mate))
    for c in swaps:
        c.start()
    d_moves = to_peers(d_ref, d_buf, d_send, d_recv)

    def gw_cols(dev):
        return gw_acc.at[:, pl.ds(pl.multiple_of(dev * LANES, LANES), LANES)]

    gw_moves = [remote(gw_cols(lax.rem(me + n, NDEV)), gw_in.at[me], gw_send.at[n - 1], gw_recv.at[n - 1],
                       lax.rem(me + n, NDEV)) for n in range(1, NDEV)]
    gg_moves = to_peers(gain_mine, gain_buf, gg_send, gg_recv)
    for c in d_moves:
        c.start()
    win_swaps = [remote(win_hbm.at[q], win_part(q), win_send.at[q], win_recv.at[q], mate) for q in range(NDEV // 2)]
    for c in win_swaps:
        c.start()
    d_buf[me] = d_ref[me]
    for c in swaps:
        c.wait_recv()

    def compute(rel, dev, col):
        chip = dev // 2
        cols = pl.ds(col * COLS, COLS)
        part[rel, col, 0:DN_ROWS, :] = (
            jnp.dot(mt_ref[dn_rows(dev), :], gy_ref[:, cols], preferred_element_type=F32)
            + jnp.dot(mt_mate[chip], gy_mate[:, cols], preferred_element_type=F32))
        part[rel, col, DN_ROWS:OUT_ROWS, :] = (
            jnp.dot(ot_ref[wo_rows(dev), :], gh_ref[:, cols], preferred_element_type=F32)
            + jnp.dot(ot_mate[chip], gh_mate[:, cols], preferred_element_type=F32))

    moves = [remote(part.at[3, 0], box.at[0], rs_send.at[0], rs_recv.at[0], near_x),
             remote(part.at[3, 1], box.at[1], rs_send.at[1], rs_recv.at[1], near_y),
             remote(part.at[1, 0], box.at[2], rs_send.at[2], rs_recv.at[2], near_x),
             remote(part.at[2, 1], box.at[3], rs_send.at[3], rs_recv.at[3], near_y),
             remote(part.at[2, 0], box.at[4], rs_send.at[4], rs_recv.at[4], near_y),
             remote(part.at[1, 1], box.at[5], rs_send.at[5], rs_recv.at[5], near_x)]
    compute(3, diag, 0)
    moves[0].start()
    compute(3, diag, 1)
    moves[1].start()
    compute(1, near_x, 0)
    moves[2].start()
    compute(2, near_y, 1)
    moves[3].start()
    compute(2, near_y, 0)
    compute(1, near_x, 1)
    u_copy.wait()

    gw_acc[...] = dot_tn(d_ref[0], u_buf[0:TOK, :])

    def grad_win_part(g, _):
        gw_acc[...] += dot_tn(d_ref[g], u_buf[pl.ds(pl.multiple_of(g * TOK, TOK), TOK), :])
        return 0

    lax.fori_loop(1, NDEV, grad_win_part, 0)
    for c in gw_moves:
        c.start()
    gw_in[me] = gw_acc[:, pl.ds(pl.multiple_of(me * LANES, LANES), LANES)]
    compute(0, me, 0)
    compute(0, me, 1)

    def add_box(rel, col, n):
        def rows_add(i, _):
            rows = pl.ds(pl.multiple_of(i * 32, 32), 32)
            part[rel, col, rows, :] += box[n, rows, :]
            return 0

        lax.fori_loop(0, OUT_ROWS // 32, rows_add, 0)

    moves[0].wait_recv()
    add_box(2, 0, 0)
    moves[4].start()
    moves[1].wait_recv()
    add_box(1, 1, 1)
    moves[5].start()

    for c in d_moves:
        c.wait_recv()
    for c in win_copies:
        c.wait()
    for c in win_swaps:
        c.wait_recv()
    gain1 = gain_ref[...]

    def grad_rows(i, carry):
        acc, acc2 = carry
        rows = pl.ds(pl.multiple_of(i * LANES, LANES), LANES)
        gu = jnp.dot(d_buf[0, rows, :], win_buf[0:3 * LANES, :], preferred_element_type=F32)
        for g in range(1, NDEV):
            gu = gu + jnp.dot(d_buf[g, rows, :], win_buf[g * 3 * LANES:(g + 1) * 3 * LANES, :],
                              preferred_element_type=F32)
        gu = gu.astype(BF16).astype(F32)
        xv = x_ref[rows, :].astype(F32)
        inv = lax.rsqrt(jnp.mean(xv * xv, axis=-1, keepdims=True) + NORM_EPS)
        normed = xv * inv
        acc = acc + jnp.sum(gu * normed, axis=0, keepdims=True)
        scaled = gu * gain1
        mean_term = jnp.mean(scaled * normed, axis=-1, keepdims=True)
        gx_out[rows, :] = (gh_ref[rows, :].astype(F32) + inv * (scaled - normed * mean_term)).astype(BF16)
        hv = h_ref[rows, :].astype(F32)
        normed2 = hv * lax.rsqrt(jnp.mean(hv * hv, axis=-1, keepdims=True) + NORM_EPS)
        acc2 = acc2 + jnp.sum(gz_ref[rows, :].astype(F32) * normed2, axis=0, keepdims=True)
        return acc, acc2

    gg1, gg2 = lax.fori_loop(0, TOK // LANES, grad_rows, (jnp.zeros((1, D), F32), jnp.zeros((1, D), F32)))
    for n in range(NDEV):
        piece = slice(n * LANES, (n + 1) * LANES)
        gain_mine[n] = jnp.concatenate([gg1[:, piece], gg2[:, piece], jnp.zeros((6, LANES), F32)], axis=0)
    for c in gg_moves:
        c.start()
    gain_buf[me] = gain_mine[me]

    moves[2].wait_recv()
    add_box(0, 0, 2)
    moves[3].wait_recv()
    add_box(0, 1, 3)
    for c in gg_moves:
        c.wait_recv()
    total = gain_buf[0]
    for n in range(1, NDEV):
        total = total + gain_buf[n]
    gain_out[...] = total
    for col in range(2):
        moves[4 + col].wait_recv()

        def finish(i, _):
            rows = pl.ds(pl.multiple_of(i * 32, 32), 32)
            dn_out[rows, col * COLS:(col + 1) * COLS] = part[0, col, rows, :] + box[4 + col, rows, :]
            return 0

        lax.fori_loop(0, DN_ROWS // 32, finish, 0)
        wo_out[:, col * COLS:(col + 1) * COLS] = part[0, col, DN_ROWS:OUT_ROWS, :] + box[4 + col, DN_ROWS:OUT_ROWS, :]
    for c in gw_moves:
        c.wait_recv()
    for n, ref in enumerate((gq_out, gk_out, gv_out)):
        ref[...] = gw_in[:, n * LANES:(n + 1) * LANES, :]
    for c in swaps + d_moves + gw_moves + gg_moves + moves + win_swaps:
        c.wait_send()


def tail_stage(m_t, grad_y, o_t, grad_h, d_qkv, x, h_res, grad_z, gain1, u_all, win_full):
    dma = pltpu.SemaphoreType.DMA
    peers = (NDEV - 1,)
    return pl.pallas_call(
        tail_kernel,
        out_shape=(jax.ShapeDtypeStruct((DN_ROWS, D), F32), jax.ShapeDtypeStruct((LANES, D), F32),
                   *(jax.ShapeDtypeStruct((NDEV, LANES, LANES), F32),) * 3, jax.ShapeDtypeStruct((TOK, D), BF16),
                   jax.ShapeDtypeStruct((8, LANES), F32)),
        in_specs=[VMEM_SPEC] * 9 + [pl.BlockSpec(memory_space=pltpu.HBM)] * 2,
        out_specs=(VMEM_SPEC,) * 7,
        scratch_shapes=[pltpu.VMEM((4, DN_ROWS, TOK), BF16), pltpu.VMEM((TOK, D), BF16),
                        pltpu.VMEM((4, LANES, TOK), BF16), pltpu.VMEM((TOK, D), BF16),
                        pltpu.VMEM((4, 2, OUT_ROWS, COLS), F32), pltpu.VMEM((6, OUT_ROWS, COLS), F32),
                        pltpu.VMEM((NDEV, TOK, 3 * LANES), BF16), pltpu.VMEM((3 * D, D), BF16), pltpu.VMEM((SEQ, D), BF16),
                        pltpu.VMEM((3 * LANES, D), F32), pltpu.VMEM((NDEV, 3 * LANES, LANES), F32),
                        pltpu.VMEM((NDEV, 8, LANES), F32), pltpu.VMEM((NDEV, 8, LANES), F32),
                        dma((10,)), dma((10,)), dma((6,)), dma((6,)), dma(peers), dma(peers),
                        dma(peers), dma(peers), dma(peers), dma(peers), dma((4,)), dma((4,)), dma((4,)), dma],
        compiler_params=pltpu.CompilerParams(collective_id=1, has_side_effects=True,
                                             vmem_limit_bytes=60 * 1024 * 1024),
        cost_estimate=pl.CostEstimate(flops=60_000_000_000, bytes_accessed=60_000_000, transcendentals=1_000),
        name='tail_stage',
    )(m_t, grad_y, o_t, grad_h, d_qkv, x, h_res, grad_z, gain1, u_all, win_full)


UP_COLS = 256
DW_COLS = 512
DZ_COLS = 1408
SLOTS = 4


def mlp_kernel(z_ref, gy_ref, wd_hbm, w_hbm, gz_out, mt_out, gw_hbm,
               w_buf, wd_buf, g_buf, g_mate, z_mate, zt, acc, gz_acc,
               swap_send, swap_recv, load_sem, wd_sem, z_send, z_recv, g_send, g_recv, out_sem):
    me = lax.axis_index('sp')
    core = lax.rem(me, 2)
    mate = me + 1 - 2 * core
    blocks = FF // UP_COLS
    barrier = pltpu.get_barrier_semaphore()
    pl.semaphore_signal(barrier, inc=1, device_id=(mate,), device_id_type=pl.DeviceIdType.MESH)
    pl.semaphore_wait(barrier, 1)

    def to_mate(src, dst, send_sem, recv_sem):
        return pltpu.make_async_remote_copy(src_ref=src, dst_ref=dst, send_sem=send_sem, recv_sem=recv_sem,
                                            device_id=(mate,), device_id_type=pl.DeviceIdType.MESH)

    def cols(n, width):
        return pl.ds(pl.multiple_of(n * width, LANES), width)

    def w_swap(n):
        return to_mate(w_hbm.at[:, :, cols(n, UP_COLS)], w_buf.at[:, core, :, cols(n, UP_COLS)],
                       swap_send.at[n], swap_recv.at[n])

    def w_load(n):
        return pltpu.make_async_copy(w_hbm.at[:, :, cols(n, UP_COLS)], w_buf.at[:, core, :, cols(n, UP_COLS)],
                                     load_sem.at[n])

    def wd_load(b):
        return pltpu.make_async_copy(wd_hbm.at[cols(b, UP_COLS), :], wd_buf.at[cols(b, UP_COLS), :], wd_sem.at[b])

    def g_swap(n):
        return to_mate(g_buf.at[:, cols(n, UP_COLS)], g_mate.at[:, cols(n, UP_COLS)], g_send.at[n], g_recv.at[n])

    def out_copy(n):
        slot = lax.rem(n, SLOTS)
        return pltpu.make_async_copy(acc.at[slot], gw_hbm.at[:, cols(n, DW_COLS)], out_sem.at[slot])

    def start(b, _):
        for n in (b, b + blocks):
            w_swap(n).start()
            w_load(n).start()
        wd_load(b).start()
        return 0

    lax.fori_loop(0, blocks, start, 0)
    z_swap = to_mate(z_ref, z_mate, z_send, z_recv)
    z_swap.start()

    def dest_cols(q):
        return pl.ds(pl.multiple_of((2 * q + core) * LANES, LANES), LANES)

    for q in range(NDEV // 2):
        zt[q * LANES:(q + 1) * LANES, 0:TOK] = z_ref[:, dest_cols(q)].T

    def up_block(b, _):
        for n in (b, b + blocks):
            w_load(n).wait()
            w_swap(n).wait_recv()
        wd_load(b).wait()
        rows = cols(b, UP_COLS)
        low, high = cols(b, UP_COLS), cols(b + blocks, UP_COLS)
        z = z_ref[...]
        gate = jnp.dot(z, w_buf[:, :, :, low].reshape(D, UP_COLS), preferred_element_type=F32)
        up = jnp.dot(z, w_buf[:, :, :, high].reshape(D, UP_COLS), preferred_element_type=F32)
        g_act = dot_nt(gy_ref[...], wd_buf[rows, :]).astype(BF16).astype(F32)
        sig = jax.nn.sigmoid(gate)
        act = gate * sig
        mt_out[rows, :] = (act * up).T.astype(BF16)
        g_buf[:, low] = (g_act * up * sig * (1.0 + gate * (1.0 - sig))).astype(BF16)
        g_buf[:, high] = (g_act * act).astype(BF16)
        g_swap(b).start()
        g_swap(b + blocks).start()
        return 0

    lax.fori_loop(0, blocks, up_block, 0)
    z_swap.wait_recv()
    for q in range(NDEV // 2):
        zt[q * LANES:(q + 1) * LANES, TOK:2 * TOK] = z_mate[:, dest_cols(q)].T

    def grad_block(n, _):
        @pl.when(n >= SLOTS)
        def _():
            out_copy(n - SLOTS).wait()

        g_swap(2 * n).wait_recv()
        g_swap(2 * n + 1).wait_recv()
        block = cols(n, DW_COLS)
        acc[lax.rem(n, SLOTS)] = (jnp.dot(zt[:, 0:TOK], g_buf[:, block], preferred_element_type=F32)
                                  + jnp.dot(zt[:, TOK:2 * TOK], g_mate[:, block], preferred_element_type=F32))
        out_copy(n).start()
        return 0

    lax.fori_loop(0, blocks, grad_block, 0)
    gz_acc[...] = jnp.zeros_like(gz_acc)

    def gz_block(n, _):
        block = cols(n, DZ_COLS)
        gz_acc[...] += dot_nt(g_buf[:, block], w_buf[:, :, :, block].reshape(D, DZ_COLS))
        return 0

    lax.fori_loop(0, 2 * FF // DZ_COLS, gz_block, 0)
    gz_out[...] = gz_acc[...].astype(BF16)
    for n in range(blocks - SLOTS, blocks):
        out_copy(n).wait()

    def finish(n, _):
        w_swap(n).wait_send()
        g_swap(n).wait_send()
        return 0

    lax.fori_loop(0, 2 * blocks, finish, 0)
    z_swap.wait_send()


def mlp_stage(z, grad_y, wd_full, w_half):
    dma = pltpu.SemaphoreType.DMA
    count = 2 * FF // UP_COLS
    hbm = pl.BlockSpec(memory_space=pltpu.HBM)
    return pl.pallas_call(
        mlp_kernel,
        out_shape=(jax.ShapeDtypeStruct((TOK, D), BF16), jax.ShapeDtypeStruct((FF, TOK), BF16),
                   jax.ShapeDtypeStruct((D // 2, 2 * FF), F32)),
        in_specs=[VMEM_SPEC] * 2 + [hbm] * 2,
        out_specs=(VMEM_SPEC, VMEM_SPEC, hbm),
        scratch_shapes=[pltpu.VMEM((NDEV // 2, 2, LANES, 2 * FF), BF16), pltpu.VMEM((FF, D), BF16),
                        pltpu.VMEM((TOK, 2 * FF), BF16), pltpu.VMEM((TOK, 2 * FF), BF16), pltpu.VMEM((TOK, D), BF16),
                        pltpu.VMEM((D // 2, 2 * TOK), BF16), pltpu.VMEM((SLOTS, D // 2, DW_COLS), F32),
                        pltpu.VMEM((TOK, D), F32),
                        dma((count,)), dma((count,)), dma((count,)), dma((count // 2,)), dma, dma,
                        dma((count,)), dma((count,)), dma((SLOTS,))],
        compiler_params=pltpu.CompilerParams(collective_id=3, has_side_effects=True,
                                             vmem_limit_bytes=58 * 1024 * 1024),
        cost_estimate=pl.CostEstimate(flops=21_000_000_000, bytes_accessed=40_000_000, transcendentals=1_500_000),
        name='mlp_stage',
    )(z, grad_y, wd_full, w_half)


def rms_back(grad_out, normed, inv_rms):
    mean_term = jnp.mean(grad_out * normed, axis=-1, keepdims=True)
    return inv_rms * (grad_out - normed * mean_term)


def solution(mesh):
    row_spec = P('sp', None)
    cube_spec = P('sp', None, None)
    vec_spec = P('sp')

    def gather(t):
        return lax.all_gather(t, 'sp', axis=0, tiled=True)

    same_core = [[0, 2, 4, 6], [1, 3, 5, 7]]

    def gather_same_core(t):
        full = lax.all_gather(t, 'sp', axis=0, tiled=True, axis_index_groups=same_core)
        return full.reshape((NDEV // 2,) + t.shape)

    def exchange(t):
        return lax.all_to_all(t, 'sp', 0, 0)

    def local_layer(x, seg_ids, positions, grad_y, norm1_gain, w_q, w_k, w_v, w_o, norm2_gain, w_gate, w_up, w_down):
        half = HD // 2
        inv_freq = (ROPE_BASE ** (-jnp.arange(half, dtype=F32) * 2.0 / HD))[:, None]
        freq = jnp.broadcast_to(inv_freq, (half, LANES))
        small = jnp.concatenate([norm1_gain.astype(F32)[None, :], norm2_gain.astype(F32)[None, :],
                                 positions.astype(F32).reshape(4, LANES), jnp.zeros((2, LANES), F32)])
        w_in = jnp.concatenate([t.transpose(1, 2, 0).reshape(NDEV, LANES, LANES) for t in (w_q, w_k, w_v)], axis=1)
        u_all, q, k, v, cos_t, sin_t, small, start2, wo_full = head_stage(
            x, w_in, small, freq, w_o.reshape(LANES, D))
        wo_full = wo_full.reshape(D, D)
        gain1 = small[:, 0].reshape(1, D)
        gain2 = small[:, 1].reshape(D)
        o_own, lse = attn_forward(start2, q, k, v)
        o_heads = exchange(o_own.reshape(NDEV, TOK, LANES))
        o_loc = o_heads.transpose(1, 0, 2).reshape(TOK, D)
        o_t = o_heads.transpose(0, 2, 1).reshape(D, TOK)

        wd_full = gather(w_down)
        wgu_half = gather_same_core(jnp.concatenate([w_gate, w_up], axis=1))
        win_half = gather_same_core(w_in.reshape(3 * D, LANES))

        x_wide = x.astype(F32)
        h_res = (x_wide + jnp.dot(o_loc, wo_full, preferred_element_type=F32)).astype(BF16)
        h_wide = h_res.astype(F32)
        inv_rms2 = lax.rsqrt(jnp.mean(h_wide * h_wide, axis=-1, keepdims=True) + NORM_EPS)
        normed2 = h_wide * inv_rms2
        z_norm = (normed2 * gain2).astype(BF16)
        grad_z_b, m_t, grad_wgu = mlp_stage(z_norm, grad_y, wd_full, wgu_half)
        grad_wgu = lax.psum_scatter(grad_wgu, 'sp', scatter_dimension=0, tiled=True, axis_index_groups=same_core)
        grad_z = grad_z_b.astype(F32)
        grad_h = (grad_y.astype(F32) + rms_back(grad_z * gain2, normed2, inv_rms2)).astype(BF16)
        grad_o = dot_nt(grad_h, wo_full).astype(BF16)
        grad_o = exchange(grad_o.reshape(TOK, NDEV, LANES).transpose(1, 0, 2)).reshape(SEQ, LANES)
        y = (h_wide + dot_tn(m_t, wd_full)).astype(BF16)

        d_qkv = attn_backward(start2, lse, q, k, v, o_own, grad_o, cos_t, sin_t)
        grad_wdown, grad_wo, *grad_qkv, grad_x, grad_gains = tail_stage(
            m_t, grad_y, o_t, grad_h, d_qkv.reshape(NDEV, TOK, 3 * LANES), x, h_res, grad_z_b,
            gain1, u_all, win_half)
        grad_q, grad_k, grad_v = (t.reshape(16, HD, LANES).transpose(2, 0, 1) for t in grad_qkv)
        return (y, grad_x, grad_gains[0], grad_q, grad_k, grad_v, grad_wo.reshape(2, HD, D),
                grad_gains[1], grad_wgu[:, :FF], grad_wgu[:, FF:], grad_wdown)

    return jax.shard_map(
        local_layer, mesh=mesh,
        in_specs=(row_spec, vec_spec, vec_spec, row_spec, vec_spec, cube_spec, cube_spec, cube_spec, cube_spec,
                  vec_spec, row_spec, row_spec, row_spec),
        out_specs=(row_spec, row_spec, vec_spec, cube_spec, cube_spec, cube_spec, cube_spec, vec_spec,
                   row_spec, row_spec, row_spec),
        check_vma=False)
```

```python
import jax
import jax.numpy as jnp
from jax import lax
from jax.experimental import pallas as pl
from jax.experimental.pallas import tpu as pltpu
from jax.sharding import PartitionSpec as P


NORM_EPS = 1e-5
ROPE_BASE = 10000.0
SEQ = 4096
D = 1024
HD = 64
FF = 2816
NDEV = 8
TOK = SEQ // NDEV
LANES = 128
BQ = 256
BK = 512
NQ = SEQ // BQ
NEG = -1e30
F32 = jnp.float32
BF16 = jnp.bfloat16


def dot_nt(a, b):
    return lax.dot_general(a, b, (((1,), (1,)), ((), ())), preferred_element_type=F32)


def dot_tn(a, b):
    return lax.dot_general(a, b, (((0,), (0,)), ((), ())), preferred_element_type=F32)


def head_pair(t):
    lane = lax.broadcasted_iota(jnp.int32, (1, LANES), 1)
    low = (lane < HD).astype(F32).astype(BF16)
    high = (lane >= HD).astype(F32).astype(BF16)
    return jnp.concatenate([t * low, t * high], axis=0)


def rope_back_tile(t, cos_t, sin_t):
    lane = lax.broadcasted_iota(jnp.int32, t.shape, 1)
    first_half = lax.rem(lane, HD) < HD // 2
    rotated = jnp.where(first_half, -pltpu.roll(t, LANES - HD // 2, 1), pltpu.roll(t, HD // 2, 1))
    return t * cos_t - rotated * sin_t


def attn_fwd_kernel(lo_ref, start_ref, q_ref, k_ref, v_ref, o_ref, lse_ref, acc_ref):
    q_iota = lax.rem(lax.broadcasted_iota(jnp.int32, (1, 2 * BQ), 1), BQ)

    def q_block(i, _):
        q_start = pl.multiple_of(i * BQ, BQ)
        q2 = head_pair(q_ref[pl.ds(q_start, BQ), :])
        first = start_ref[pl.ds(i, 1), :]
        q_index = q_start + q_iota
        acc_ref[...] = jnp.zeros_like(acc_ref)

        def k_block(j, carry):
            m_old, l_old = carry
            k_start = pl.multiple_of(j * BK, BK)
            k = k_ref[pl.ds(k_start, BK), :]
            v = v_ref[pl.ds(k_start, BK), :]
            s = dot_nt(k, q2)
            k_index = k_start + lax.broadcasted_iota(jnp.int32, s.shape, 0)
            s = jnp.where((k_index >= first) & (k_index <= q_index), s, NEG)
            m_new = jnp.maximum(m_old, jnp.max(s, axis=0, keepdims=True))
            p = jnp.exp(s - m_new)
            alpha = jnp.exp(m_old - m_new)
            l_new = alpha * l_old + jnp.sum(p, axis=0, keepdims=True)
            acc_ref[...] = acc_ref[...] * alpha + dot_tn(v, p.astype(BF16))
            return m_new, l_new

        init = (jnp.full((1, 2 * BQ), NEG, F32), jnp.zeros((1, 2 * BQ), F32))
        m_fin, l_fin = lax.fori_loop(lax.div(lo_ref[i, 0], BK), (q_start + BQ - 1) // BK + 1, k_block, init)
        lse_ref[pl.ds(i, 1), :] = m_fin + jnp.log(l_fin)
        out = acc_ref[...] * (1.0 / l_fin)
        out = jnp.concatenate([out[:HD, :BQ], out[HD:, BQ:]], axis=0)
        o_ref[pl.ds(q_start, BQ), :] = out.T.astype(BF16)
        return 0

    lax.fori_loop(0, NQ, q_block, 0)


def attn_bwd_kernel(lo_ref, start_ref, lse_ref, q_ref, k_ref, v_ref, o_ref, do_ref, cos_ref, sin_ref,
                    out_ref, dk_acc, dv_acc, dq_acc):
    q_iota = lax.rem(lax.broadcasted_iota(jnp.int32, (1, 2 * BQ), 1), BQ)
    dk_acc[...] = jnp.zeros_like(dk_acc)
    dv_acc[...] = jnp.zeros_like(dv_acc)

    def q_block(i, _):
        q_start = pl.multiple_of(i * BQ, BQ)
        q2 = head_pair(q_ref[pl.ds(q_start, BQ), :])
        do = do_ref[pl.ds(q_start, BQ), :]
        do2 = head_pair(do)
        prod = (do.astype(F32) * o_ref[pl.ds(q_start, BQ), :].astype(F32)).T
        delta = jnp.concatenate([jnp.sum(prod[:HD], axis=0, keepdims=True),
                                 jnp.sum(prod[HD:], axis=0, keepdims=True)], axis=1)
        first = start_ref[pl.ds(i, 1), :]
        lse = lse_ref[pl.ds(i, 1), :]
        q_index = q_start + q_iota
        dq_acc[...] = jnp.zeros_like(dq_acc)

        def k_block(j, _):
            k_start = pl.multiple_of(j * BK, BK)
            k = k_ref[pl.ds(k_start, BK), :]
            v = v_ref[pl.ds(k_start, BK), :]
            s = dot_nt(k, q2)
            k_index = k_start + lax.broadcasted_iota(jnp.int32, s.shape, 0)
            s = jnp.where((k_index >= first) & (k_index <= q_index), s, NEG)
            p = jnp.exp(s - lse)
            dp = dot_nt(v, do2).astype(BF16).astype(F32)
            ds = (p * (dp - delta)).astype(BF16)
            dv_acc[pl.ds(k_start, BK), :] += jnp.dot(p.astype(BF16), do2, preferred_element_type=F32)
            dk_acc[pl.ds(k_start, BK), :] += jnp.dot(ds, q2, preferred_element_type=F32)
            dq_acc[...] += dot_tn(k, ds)
            return 0

        lax.fori_loop(lax.div(lo_ref[i, 0], BK), (q_start + BQ - 1) // BK + 1, k_block, 0)
        dq = jnp.concatenate([dq_acc[:HD, :BQ], dq_acc[HD:, BQ:]], axis=0).T * (HD ** -0.5)
        rows = pl.ds(q_start, BQ)
        dq = dq.astype(BF16).astype(F32)
        out_ref[rows, 0:LANES] = rope_back_tile(dq, cos_ref[rows, :], sin_ref[rows, :]).astype(BF16)
        return 0

    lax.fori_loop(0, NQ, q_block, 0)

    def finish(i, _):
        rows = pl.ds(pl.multiple_of(i * BQ, BQ), BQ)
        dk = dk_acc[rows, :].astype(BF16).astype(F32)
        out_ref[rows, LANES:2 * LANES] = rope_back_tile(dk, cos_ref[rows, :], sin_ref[rows, :]).astype(BF16)
        out_ref[rows, 2 * LANES:3 * LANES] = dv_acc[rows, :].astype(BF16)
        return 0

    lax.fori_loop(0, NQ, finish, 0)


VMEM_SPEC = pl.BlockSpec(memory_space=pltpu.VMEM)
SMEM_SPEC = pl.BlockSpec(memory_space=pltpu.SMEM)


def attn_forward(start, q, k, v):
    return pl.pallas_call(
        attn_fwd_kernel,
        out_shape=(jax.ShapeDtypeStruct((SEQ, LANES), BF16), jax.ShapeDtypeStruct((NQ, 2 * BQ), F32)),
        in_specs=[SMEM_SPEC] + [VMEM_SPEC] * 4,
        out_specs=(VMEM_SPEC, VMEM_SPEC),
        scratch_shapes=[pltpu.VMEM((LANES, 2 * BQ), F32)],
        compiler_params=pltpu.CompilerParams(vmem_limit_bytes=40 * 1024 * 1024),
        cost_estimate=pl.CostEstimate(flops=20_000_000_000, bytes_accessed=5_000_000, transcendentals=20_000_000),
        name='attn_fwd',
    )(start, start, q, k, v)


def attn_backward(start, lse, q, k, v, o, do, cos_t, sin_t):
    return pl.pallas_call(
        attn_bwd_kernel,
        out_shape=jax.ShapeDtypeStruct((SEQ, 3 * LANES), BF16),
        in_specs=[SMEM_SPEC] + [VMEM_SPEC] * 9,
        out_specs=VMEM_SPEC,
        scratch_shapes=[pltpu.VMEM((SEQ, LANES), F32), pltpu.VMEM((SEQ, LANES), F32),
                        pltpu.VMEM((LANES, 2 * BQ), F32)],
        compiler_params=pltpu.CompilerParams(vmem_limit_bytes=48 * 1024 * 1024),
        cost_estimate=pl.CostEstimate(flops=50_000_000_000, bytes_accessed=12_000_000, transcendentals=20_000_000),
        name='attn_bwd',
    )(start, start, lse, q, k, v, o, do, cos_t, sin_t)


def head_kernel(x_ref, w_ref, small_ref, freq_ref, wo_ref, u_hbm, q_ref, k_ref, v_ref, cos_ref, sin_ref, all_small,
                start_ref, wo_out, x_buf, w_buf, w_ext, u_buf, small_send, small_recv, w_send, w_recv, x_send, x_recv,
                wo_send, wo_recv, u_sem):
    me = lax.axis_index('sp')
    core = lax.rem(me, 2)
    x_pos = lax.rem(me // 2, 2)
    y_pos = me // 4
    step_c, step_x, step_y = 1 - 2 * core, 2 - 4 * x_pos, 4 - 8 * y_pos
    mate, near_x, near_y, diag = me + step_c, me + step_x, me + step_y, me + step_x + step_y

    barrier = pltpu.get_barrier_semaphore()
    for n in range(1, NDEV):
        pl.semaphore_signal(barrier, inc=1, device_id=(lax.rem(me + n, NDEV),), device_id_type=pl.DeviceIdType.MESH)
    pl.semaphore_wait(barrier, NDEV - 1)

    def remote(src, dst, send_sem, recv_sem, dev):
        return pltpu.make_async_remote_copy(src_ref=src, dst_ref=dst, send_sem=send_sem, recv_sem=recv_sem,
                                            device_id=(dev,), device_id_type=pl.DeviceIdType.MESH)

    def half(ref, h):
        rows = ref.shape[0] // 2
        return ref.at[pl.ds(h * rows, rows), :]

    def x_copy(slot, src_dev, h, target, from_ref=None):
        source = half(x_buf.at[src_dev], h) if from_ref is None else half(from_ref, h)
        return remote(source, half(x_buf.at[src_dev], h), x_send.at[slot], x_recv.at[slot], target)

    def wo_copy(slot, src_dev, h, target, from_ref=None):
        source = half(wo_out.at[src_dev], h) if from_ref is None else half(from_ref, h)
        return remote(source, half(wo_out.at[src_dev], h), wo_send.at[slot], wo_recv.at[slot], target)

    def first_sends(copy, from_ref):
        return [copy(0, me, 0, near_x, from_ref), copy(3, me, 1, near_y, from_ref),
                copy(1, me, 1, near_x, from_ref), copy(2, me, 0, near_y, from_ref),
                copy(12, me, 0, mate, from_ref), copy(13, me, 1, mate, from_ref)]

    smalls = [remote(small_ref, all_small.at[me], small_send.at[n - 1], small_recv.at[n - 1], lax.rem(me + n, NDEV))
              for n in range(1, NDEV)]
    weights = [remote(w_ref.at[lax.rem(me + n, NDEV)], w_buf.at[me], w_send.at[n - 1], w_recv.at[n - 1],
                      lax.rem(me + n, NDEV)) for n in range(1, NDEV)]
    for c in smalls:
        c.start()
    for c in weights:
        c.start()
    own = first_sends(x_copy, x_ref)
    for c in own:
        c.start()

    all_small[me] = small_ref[...]
    w_buf[me] = w_ref[me]
    for c in smalls + weights:
        c.wait_recv()

    half_head = HD // 2
    for n in range(NDEV):
        cols = slice(n * LANES, (n + 1) * LANES)
        w_ext[0:3 * LANES, cols] = w_buf[n]
        for m in range(2):
            t = w_buf[n, m * LANES:(m + 1) * LANES, :].astype(F32)
            rot = jnp.concatenate([-t[half_head:HD], t[:half_head], -t[HD + half_head:], t[HD:HD + half_head]], axis=0)
            w_ext[(3 + m) * LANES:(4 + m) * LANES, cols] = rot.astype(BF16)
    gain1 = jnp.concatenate([all_small[n, 0:1, :] for n in range(NDEV)], axis=1)

    def process(order, src_ref, src_dev, h):
        def part(i, _):
            local = pl.ds(pl.multiple_of(h * (TOK // 2) + i * LANES, LANES), LANES)
            rows = pl.ds(pl.multiple_of(src_dev * TOK + h * (TOK // 2) + i * LANES, LANES), LANES)
            xv = src_ref[local, :].astype(F32)
            inv = lax.rsqrt(jnp.mean(xv * xv, axis=-1, keepdims=True) + NORM_EPS)
            u = (xv * inv * gain1).astype(BF16)
            u_buf[rows, :] = u
            proj = dot_nt(u, w_ext[...])
            angle = freq_ref[...] * all_small[src_dev, pl.ds(2 + 2 * h + i, 1), :]
            cos4, sin4 = jnp.cos(angle), jnp.sin(angle)
            cos_v = jnp.concatenate([cos4] * 4, axis=0).T
            sin_v = jnp.concatenate([sin4] * 4, axis=0).T
            cos_ref[rows, :] = cos_v
            sin_ref[rows, :] = sin_v
            q = (proj[:, :LANES] * cos_v + proj[:, 3 * LANES:4 * LANES] * sin_v).astype(BF16).astype(F32)
            q_ref[rows, :] = (q * (HD ** -0.5)).astype(BF16)
            k_ref[rows, :] = (proj[:, LANES:2 * LANES] * cos_v + proj[:, 4 * LANES:] * sin_v).astype(BF16)
            v_ref[rows, :] = proj[:, 2 * LANES:3 * LANES].astype(BF16)
            return 0

        lax.fori_loop(0, 2, part, 0)
        u_rows = pl.ds(pl.multiple_of(src_dev * TOK + h * (TOK // 2), TOK // 2), TOK // 2)
        out = pltpu.make_async_copy(u_buf.at[u_rows, :], u_hbm.at[u_rows, :], u_sem.at[order])
        out.start()
        return out

    pending = []
    copies = list(own)

    def arrive(copy, slot, src_dev, h):
        copy(slot, src_dev, h, mate).wait_recv()

    def pass_on(copy, slot, src_dev, h, target):
        c = copy(slot, src_dev, h, target)
        c.start()
        copies.append(c)

    def relay(copy, slot, src_dev, h):
        arrive(copy, slot, src_dev, h)
        if slot == 0:
            pass_on(copy, 4, src_dev, h, near_y)
        elif slot == 3:
            pass_on(copy, 5, src_dev, h, near_x)
        pass_on(copy, 6 + slot, src_dev, h, mate)

    def work(src_ref, src_dev, h):
        pending.append(process(len(pending), src_ref, src_dev, h))

    work(x_ref, me, 0)
    work(x_ref, me, 1)
    arrivals = [(0, near_x, 0), (3, near_y, 1), (1, near_x, 1), (2, near_y, 0), (4, diag, 0), (5, diag, 1)]
    late = [(12, mate, 0), (13, mate, 1)]
    for n, (slot, src_dev, h) in enumerate(arrivals):
        relay(x_copy, slot, src_dev, h)
        if n == 1:
            wo_own = first_sends(wo_copy, wo_ref)
            for c in wo_own:
                c.start()
            copies += wo_own
            wo_out[me] = wo_ref[...]
        if n >= 4:
            relay(wo_copy, *arrivals[n - 4])
        work(x_buf.at[src_dev], src_dev, h)
        mate_slot, mate_src, mate_h = late.pop(0)
        arrive(x_copy, mate_slot, mate_src, mate_h)
        work(x_buf.at[mate_src], mate_src, mate_h)
        late.append((6 + slot, src_dev + step_c, h))
    for n, (slot, src_dev, h) in enumerate(late):
        if n < 2:
            relay(wo_copy, *arrivals[n + 2])
        arrive(x_copy, slot, src_dev, h)
        work(x_buf.at[src_dev], src_dev, h)
    for n in range(NDEV):
        for h in range(2):
            row = jnp.concatenate([all_small[n, 2 + 2 * h:3 + 2 * h, :], all_small[n, 3 + 2 * h:4 + 2 * h, :]], axis=1)
            index = n * TOK + h * BQ + lax.broadcasted_iota(jnp.int32, (1, BQ), 1)
            first = index - row.astype(jnp.int32)
            start_ref[2 * n + h:2 * n + h + 1, :] = jnp.concatenate([first, first], axis=1)
    relay(wo_copy, *arrivals[4])
    relay(wo_copy, *arrivals[5])
    for slot, src_dev, h in [(12, mate, 0), (13, mate, 1)] + [(6 + m, d + step_c, h) for m, d, h in arrivals]:
        arrive(wo_copy, slot, src_dev, h)
    for c in pending:
        c.wait()
    for c in smalls + weights + copies:
        c.wait_send()


def head_stage(x, w_pieces, small, freq, w_o):
    dma = pltpu.SemaphoreType.DMA
    return pl.pallas_call(
        head_kernel,
        out_shape=(jax.ShapeDtypeStruct((SEQ, D), BF16),) + tuple(jax.ShapeDtypeStruct((SEQ, LANES), BF16) for _ in range(3))
        + tuple(jax.ShapeDtypeStruct((SEQ, LANES), F32) for _ in range(2))
        + (jax.ShapeDtypeStruct((NDEV, 8, LANES), F32), jax.ShapeDtypeStruct((NQ, 2 * BQ), jnp.int32),
           jax.ShapeDtypeStruct((NDEV, LANES, D), BF16)),
        in_specs=[VMEM_SPEC] * 5,
        out_specs=(pl.BlockSpec(memory_space=pl.ANY),) + (VMEM_SPEC,) * 8,
        scratch_shapes=[pltpu.VMEM((NDEV, TOK, D), BF16), pltpu.VMEM((NDEV, 3 * LANES, LANES), BF16),
                        pltpu.VMEM((5 * LANES, D), BF16), pltpu.VMEM((SEQ, D), BF16),
                        dma((NDEV - 1,)), dma((NDEV - 1,)), dma((NDEV - 1,)), dma((NDEV - 1,)),
                        dma((14,)), dma((14,)), dma((14,)), dma((14,)), dma((16,))],
        compiler_params=pltpu.CompilerParams(collective_id=0, has_side_effects=True,
                                             vmem_limit_bytes=48 * 1024 * 1024),
        cost_estimate=pl.CostEstimate(flops=40_000_000_000, bytes_accessed=30_000_000, transcendentals=1_000_000),
        name='head_stage',
    )(x, w_pieces, small, freq, w_o)


COLS = D // 2
DN_ROWS = FF // NDEV
OUT_ROWS = DN_ROWS + LANES


def tail_kernel(mt_ref, gy_ref, ot_ref, gh_ref, d_ref, x_ref, h_ref, gz_ref, gain_ref, u_hbm, win_hbm,
                dn_out, wo_out, gq_out, gk_out, gv_out, gx_out, gain1_out, gain2_out,
                mt_mate, gy_mate, ot_mate, gh_mate, part, box, d_buf, win_buf, u_buf, gw_acc, gw_in, gain_mine, gain_buf,
                mate_send, mate_recv, rs_send, rs_recv, d_send, d_recv, gw_send, gw_recv, gg_send, gg_recv, win_send, win_recv, win_sem, u_sem):
    me = lax.axis_index('sp')
    core = lax.rem(me, 2)
    x_pos = lax.rem(me // 2, 2)
    y_pos = me // 4
    step_c, step_x, step_y = 1 - 2 * core, 2 - 4 * x_pos, 4 - 8 * y_pos
    mate, near_x, near_y, diag = me + step_c, me + step_x, me + step_y, me + step_x + step_y

    def win_part(q):
        return win_buf.at[:, pl.ds(pl.multiple_of((2 * q + core) * LANES, LANES), LANES)]

    win_copies = [pltpu.make_async_copy(win_hbm.at[q], win_part(q), win_sem.at[q]) for q in range(NDEV // 2)]
    for c in win_copies:
        c.start()
    u_copy = pltpu.make_async_copy(u_hbm, u_buf, u_sem)
    u_copy.start()

    barrier = pltpu.get_barrier_semaphore()
    for n in range(1, NDEV):
        pl.semaphore_signal(barrier, inc=1, device_id=(lax.rem(me + n, NDEV),), device_id_type=pl.DeviceIdType.MESH)
    pl.semaphore_wait(barrier, NDEV - 1)

    def remote(src, dst, send_sem, recv_sem, dev):
        return pltpu.make_async_remote_copy(src_ref=src, dst_ref=dst, send_sem=send_sem, recv_sem=recv_sem,
                                            device_id=(dev,), device_id_type=pl.DeviceIdType.MESH)

    def to_peers(src, dst, send_sem, recv_sem):
        return [remote(src.at[lax.rem(me + n, NDEV)], dst.at[me], send_sem.at[n - 1], recv_sem.at[n - 1],
                       lax.rem(me + n, NDEV)) for n in range(1, NDEV)]

    def dn_rows(dev):
        return pl.ds(pl.multiple_of(dev * DN_ROWS, 32), DN_ROWS)

    def wo_rows(dev):
        return pl.ds(pl.multiple_of(dev * LANES, LANES), LANES)

    swaps = []
    for q in range(NDEV // 2):
        dest = 2 * q + 1 - core
        swaps.append(remote(mt_ref.at[dn_rows(dest), :], mt_mate.at[q], mate_send.at[q], mate_recv.at[q], mate))
        swaps.append(remote(ot_ref.at[wo_rows(dest), :], ot_mate.at[q], mate_send.at[4 + q], mate_recv.at[4 + q], mate))
    swaps.append(remote(gy_ref, gy_mate, mate_send.at[8], mate_recv.at[8], mate))
    swaps.append(remote(gh_ref, gh_mate, mate_send.at[9], mate_recv.at[9], mate))
    for c in swaps:
        c.start()
    d_moves = to_peers(d_ref, d_buf, d_send, d_recv)

    def gw_cols(dev):
        return gw_acc.at[:, pl.ds(pl.multiple_of(dev * LANES, LANES), LANES)]

    gw_moves = [remote(gw_cols(lax.rem(me + n, NDEV)), gw_in.at[me], gw_send.at[n - 1], gw_recv.at[n - 1],
                       lax.rem(me + n, NDEV)) for n in range(1, NDEV)]
    gg_moves = to_peers(gain_mine, gain_buf, gg_send, gg_recv)
    for c in d_moves:
        c.start()
    win_swaps = [remote(win_hbm.at[q], win_part(q), win_send.at[q], win_recv.at[q], mate) for q in range(NDEV // 2)]
    for c in win_swaps:
        c.start()
    d_buf[me] = d_ref[me]
    for c in swaps:
        c.wait_recv()

    def compute(rel, dev, col):
        chip = dev // 2
        cols = pl.ds(col * COLS, COLS)
        part[rel, col, 0:DN_ROWS, :] = (
            jnp.dot(mt_ref[dn_rows(dev), :], gy_ref[:, cols], preferred_element_type=F32)
            + jnp.dot(mt_mate[chip], gy_mate[:, cols], preferred_element_type=F32))
        part[rel, col, DN_ROWS:OUT_ROWS, :] = (
            jnp.dot(ot_ref[wo_rows(dev), :], gh_ref[:, cols], preferred_element_type=F32)
            + jnp.dot(ot_mate[chip], gh_mate[:, cols], preferred_element_type=F32))

    moves = [remote(part.at[3, 0], box.at[0], rs_send.at[0], rs_recv.at[0], near_x),
             remote(part.at[3, 1], box.at[1], rs_send.at[1], rs_recv.at[1], near_y),
             remote(part.at[1, 0], box.at[2], rs_send.at[2], rs_recv.at[2], near_x),
             remote(part.at[2, 1], box.at[3], rs_send.at[3], rs_recv.at[3], near_y),
             remote(part.at[2, 0], box.at[4], rs_send.at[4], rs_recv.at[4], near_y),
             remote(part.at[1, 1], box.at[5], rs_send.at[5], rs_recv.at[5], near_x)]
    compute(3, diag, 0)
    moves[0].start()
    compute(3, diag, 1)
    moves[1].start()
    compute(1, near_x, 0)
    moves[2].start()
    compute(2, near_y, 1)
    moves[3].start()
    compute(2, near_y, 0)
    compute(1, near_x, 1)
    u_copy.wait()

    gw_acc[...] = dot_tn(d_ref[0], u_buf[0:TOK, :])

    def grad_win_part(g, _):
        gw_acc[...] += dot_tn(d_ref[g], u_buf[pl.ds(pl.multiple_of(g * TOK, TOK), TOK), :])
        return 0

    lax.fori_loop(1, NDEV, grad_win_part, 0)
    for c in gw_moves:
        c.start()
    gw_in[me] = gw_acc[:, pl.ds(pl.multiple_of(me * LANES, LANES), LANES)]
    compute(0, me, 0)
    compute(0, me, 1)

    def add_box(rel, col, n):
        def rows_add(i, _):
            rows = pl.ds(pl.multiple_of(i * 32, 32), 32)
            part[rel, col, rows, :] += box[n, rows, :]
            return 0

        lax.fori_loop(0, OUT_ROWS // 32, rows_add, 0)

    moves[0].wait_recv()
    add_box(2, 0, 0)
    moves[4].start()
    moves[1].wait_recv()
    add_box(1, 1, 1)
    moves[5].start()

    for c in d_moves:
        c.wait_recv()
    for c in win_copies:
        c.wait()
    for c in win_swaps:
        c.wait_recv()
    gain1 = gain_ref[...]

    def grad_rows(i, carry):
        acc, acc2 = carry
        rows = pl.ds(pl.multiple_of(i * LANES, LANES), LANES)
        gu = jnp.dot(d_buf[0, rows, :], win_buf[0:3 * LANES, :], preferred_element_type=F32)
        for g in range(1, NDEV):
            gu = gu + jnp.dot(d_buf[g, rows, :], win_buf[g * 3 * LANES:(g + 1) * 3 * LANES, :],
                              preferred_element_type=F32)
        gu = gu.astype(BF16).astype(F32)
        xv = x_ref[rows, :].astype(F32)
        inv = lax.rsqrt(jnp.mean(xv * xv, axis=-1, keepdims=True) + NORM_EPS)
        normed = xv * inv
        acc = acc + jnp.sum(gu * normed, axis=0, keepdims=True)
        scaled = gu * gain1
        mean_term = jnp.mean(scaled * normed, axis=-1, keepdims=True)
        gx_out[rows, :] = (gh_ref[rows, :].astype(F32) + inv * (scaled - normed * mean_term)).astype(BF16)
        hv = h_ref[rows, :].astype(F32)
        normed2 = hv * lax.rsqrt(jnp.mean(hv * hv, axis=-1, keepdims=True) + NORM_EPS)
        acc2 = acc2 + jnp.sum(gz_ref[rows, :].astype(F32) * normed2, axis=0, keepdims=True)
        return acc, acc2

    gg1, gg2 = lax.fori_loop(0, TOK // LANES, grad_rows, (jnp.zeros((1, D), F32), jnp.zeros((1, D), F32)))
    for n in range(NDEV):
        piece = slice(n * LANES, (n + 1) * LANES)
        gain_mine[n] = jnp.concatenate([gg1[:, piece], gg2[:, piece], jnp.zeros((6, LANES), F32)], axis=0)
    for c in gg_moves:
        c.start()
    gain_buf[me] = gain_mine[me]

    moves[2].wait_recv()
    add_box(0, 0, 2)
    moves[3].wait_recv()
    add_box(0, 1, 3)
    for c in gg_moves:
        c.wait_recv()
    total = gain_buf[0]
    for n in range(1, NDEV):
        total = total + gain_buf[n]
    gain1_out[...] = total[0:1]
    gain2_out[...] = total[1:2]
    for col in range(2):
        moves[4 + col].wait_recv()

        def finish(i, _):
            rows = pl.ds(pl.multiple_of(i * 32, 32), 32)
            dn_out[rows, col * COLS:(col + 1) * COLS] = part[0, col, rows, :] + box[4 + col, rows, :]
            return 0

        lax.fori_loop(0, DN_ROWS // 32, finish, 0)
        wo_out[:, col * COLS:(col + 1) * COLS] = part[0, col, DN_ROWS:OUT_ROWS, :] + box[4 + col, DN_ROWS:OUT_ROWS, :]
    for c in gw_moves:
        c.wait_recv()
    for n, ref in enumerate((gq_out, gk_out, gv_out)):
        ref[...] = gw_in[:, n * LANES:(n + 1) * LANES, :]
    for c in swaps + d_moves + gw_moves + gg_moves + moves + win_swaps:
        c.wait_send()


def tail_stage(m_t, grad_y, o_t, grad_h, d_qkv, x, h_res, grad_z, gain1, u_all, win_full):
    dma = pltpu.SemaphoreType.DMA
    peers = (NDEV - 1,)
    return pl.pallas_call(
        tail_kernel,
        out_shape=(jax.ShapeDtypeStruct((DN_ROWS, D), F32), jax.ShapeDtypeStruct((LANES, D), F32),
                   *(jax.ShapeDtypeStruct((NDEV, LANES, LANES), F32),) * 3, jax.ShapeDtypeStruct((TOK, D), BF16),
                   *(jax.ShapeDtypeStruct((1, LANES), F32),) * 2),
        in_specs=[VMEM_SPEC] * 9 + [pl.BlockSpec(memory_space=pltpu.HBM)] * 2,
        out_specs=(VMEM_SPEC,) * 8,
        scratch_shapes=[pltpu.VMEM((4, DN_ROWS, TOK), BF16), pltpu.VMEM((TOK, D), BF16),
                        pltpu.VMEM((4, LANES, TOK), BF16), pltpu.VMEM((TOK, D), BF16),
                        pltpu.VMEM((4, 2, OUT_ROWS, COLS), F32), pltpu.VMEM((6, OUT_ROWS, COLS), F32),
                        pltpu.VMEM((NDEV, TOK, 3 * LANES), BF16), pltpu.VMEM((3 * D, D), BF16), pltpu.VMEM((SEQ, D), BF16),
                        pltpu.VMEM((3 * LANES, D), F32), pltpu.VMEM((NDEV, 3 * LANES, LANES), F32),
                        pltpu.VMEM((NDEV, 8, LANES), F32), pltpu.VMEM((NDEV, 8, LANES), F32),
                        dma((10,)), dma((10,)), dma((6,)), dma((6,)), dma(peers), dma(peers),
                        dma(peers), dma(peers), dma(peers), dma(peers), dma((4,)), dma((4,)), dma((4,)), dma],
        compiler_params=pltpu.CompilerParams(collective_id=1, has_side_effects=True,
                                             vmem_limit_bytes=60 * 1024 * 1024),
        cost_estimate=pl.CostEstimate(flops=60_000_000_000, bytes_accessed=60_000_000, transcendentals=1_000),
        name='tail_stage',
    )(m_t, grad_y, o_t, grad_h, d_qkv, x, h_res, grad_z, gain1, u_all, win_full)


UP_COLS = 256
DW_COLS = 512
DZ_COLS = 1408
SLOTS = 4


def mlp_kernel(z_ref, gy_ref, wd_hbm, w_hbm, gz_out, mt_out, gw_hbm,
               w_buf, wd_buf, g_buf, g_mate, z_mate, zt, acc, gz_acc,
               swap_send, swap_recv, load_sem, wd_sem, z_send, z_recv, g_send, g_recv, out_sem):
    me = lax.axis_index('sp')
    core = lax.rem(me, 2)
    mate = me + 1 - 2 * core
    blocks = FF // UP_COLS
    barrier = pltpu.get_barrier_semaphore()
    pl.semaphore_signal(barrier, inc=1, device_id=(mate,), device_id_type=pl.DeviceIdType.MESH)
    pl.semaphore_wait(barrier, 1)

    def to_mate(src, dst, send_sem, recv_sem):
        return pltpu.make_async_remote_copy(src_ref=src, dst_ref=dst, send_sem=send_sem, recv_sem=recv_sem,
                                            device_id=(mate,), device_id_type=pl.DeviceIdType.MESH)

    def cols(n, width):
        return pl.ds(pl.multiple_of(n * width, LANES), width)

    def w_swap(n):
        return to_mate(w_hbm.at[:, :, cols(n, UP_COLS)], w_buf.at[:, core, :, cols(n, UP_COLS)],
                       swap_send.at[n], swap_recv.at[n])

    def w_load(n):
        return pltpu.make_async_copy(w_hbm.at[:, :, cols(n, UP_COLS)], w_buf.at[:, core, :, cols(n, UP_COLS)],
                                     load_sem.at[n])

    def wd_load(b):
        return pltpu.make_async_copy(wd_hbm.at[cols(b, UP_COLS), :], wd_buf.at[cols(b, UP_COLS), :], wd_sem.at[b])

    def g_swap(n):
        return to_mate(g_buf.at[:, cols(n, UP_COLS)], g_mate.at[:, cols(n, UP_COLS)], g_send.at[n], g_recv.at[n])

    def out_copy(n):
        slot = lax.rem(n, SLOTS)
        return pltpu.make_async_copy(acc.at[slot], gw_hbm.at[:, cols(n, DW_COLS)], out_sem.at[slot])

    def start(b, _):
        for n in (b, b + blocks):
            w_swap(n).start()
            w_load(n).start()
        wd_load(b).start()
        return 0

    lax.fori_loop(0, blocks, start, 0)
    z_swap = to_mate(z_ref, z_mate, z_send, z_recv)
    z_swap.start()

    def dest_cols(q):
        return pl.ds(pl.multiple_of((2 * q + core) * LANES, LANES), LANES)

    for q in range(NDEV // 2):
        zt[q * LANES:(q + 1) * LANES, 0:TOK] = z_ref[:, dest_cols(q)].T

    def up_block(b, _):
        for n in (b, b + blocks):
            w_load(n).wait()
            w_swap(n).wait_recv()
        wd_load(b).wait()
        rows = cols(b, UP_COLS)
        low, high = cols(b, UP_COLS), cols(b + blocks, UP_COLS)
        z = z_ref[...]
        gate = jnp.dot(z, w_buf[:, :, :, low].reshape(D, UP_COLS), preferred_element_type=F32)
        up = jnp.dot(z, w_buf[:, :, :, high].reshape(D, UP_COLS), preferred_element_type=F32)
        g_act = dot_nt(gy_ref[...], wd_buf[rows, :]).astype(BF16).astype(F32)
        sig = jax.nn.sigmoid(gate)
        act = gate * sig
        mt_out[rows, :] = (act * up).T.astype(BF16)
        g_buf[:, low] = (g_act * up * sig * (1.0 + gate * (1.0 - sig))).astype(BF16)
        g_buf[:, high] = (g_act * act).astype(BF16)
        g_swap(b).start()
        g_swap(b + blocks).start()
        return 0

    lax.fori_loop(0, blocks, up_block, 0)
    z_swap.wait_recv()
    for q in range(NDEV // 2):
        zt[q * LANES:(q + 1) * LANES, TOK:2 * TOK] = z_mate[:, dest_cols(q)].T

    def grad_block(n, _):
        @pl.when(n >= SLOTS)
        def _():
            out_copy(n - SLOTS).wait()

        g_swap(2 * n).wait_recv()
        g_swap(2 * n + 1).wait_recv()
        block = cols(n, DW_COLS)
        acc[lax.rem(n, SLOTS)] = (jnp.dot(zt[:, 0:TOK], g_buf[:, block], preferred_element_type=F32)
                                  + jnp.dot(zt[:, TOK:2 * TOK], g_mate[:, block], preferred_element_type=F32))
        out_copy(n).start()
        return 0

    lax.fori_loop(0, blocks, grad_block, 0)
    gz_acc[...] = jnp.zeros_like(gz_acc)

    def gz_block(n, _):
        block = cols(n, DZ_COLS)
        gz_acc[...] += dot_nt(g_buf[:, block], w_buf[:, :, :, block].reshape(D, DZ_COLS))
        return 0

    lax.fori_loop(0, 2 * FF // DZ_COLS, gz_block, 0)
    gz_out[...] = gz_acc[...].astype(BF16)
    for n in range(blocks - SLOTS, blocks):
        out_copy(n).wait()

    def finish(n, _):
        w_swap(n).wait_send()
        g_swap(n).wait_send()
        return 0

    lax.fori_loop(0, 2 * blocks, finish, 0)
    z_swap.wait_send()


def mlp_stage(z, grad_y, wd_full, w_half):
    dma = pltpu.SemaphoreType.DMA
    count = 2 * FF // UP_COLS
    hbm = pl.BlockSpec(memory_space=pltpu.HBM)
    return pl.pallas_call(
        mlp_kernel,
        out_shape=(jax.ShapeDtypeStruct((TOK, D), BF16), jax.ShapeDtypeStruct((FF, TOK), BF16),
                   jax.ShapeDtypeStruct((D // 2, 2 * FF), F32)),
        in_specs=[VMEM_SPEC] * 2 + [hbm] * 2,
        out_specs=(VMEM_SPEC, VMEM_SPEC, hbm),
        scratch_shapes=[pltpu.VMEM((NDEV // 2, 2, LANES, 2 * FF), BF16), pltpu.VMEM((FF, D), BF16),
                        pltpu.VMEM((TOK, 2 * FF), BF16), pltpu.VMEM((TOK, 2 * FF), BF16), pltpu.VMEM((TOK, D), BF16),
                        pltpu.VMEM((D // 2, 2 * TOK), BF16), pltpu.VMEM((SLOTS, D // 2, DW_COLS), F32),
                        pltpu.VMEM((TOK, D), F32),
                        dma((count,)), dma((count,)), dma((count,)), dma((count // 2,)), dma, dma,
                        dma((count,)), dma((count,)), dma((SLOTS,))],
        compiler_params=pltpu.CompilerParams(collective_id=3, has_side_effects=True,
                                             vmem_limit_bytes=58 * 1024 * 1024),
        cost_estimate=pl.CostEstimate(flops=21_000_000_000, bytes_accessed=40_000_000, transcendentals=1_500_000),
        name='mlp_stage',
    )(z, grad_y, wd_full, w_half)


def emit_kernel(*refs):
    count = (len(refs) - 1) // 3
    sources, targets, bufs = refs[:count - 1], refs[count - 1:2 * count - 1], refs[2 * count - 1:3 * count - 1]
    load_sem, store_sem = refs[-2:]
    gu = sources[0]
    views = [gu.at[:, 0:FF], gu.at[:, FF:2 * FF]] + list(sources[1:])
    loads = [pltpu.make_async_copy(v, b, load_sem.at[n]) for n, (v, b) in enumerate(zip(views, bufs))]
    stores = [pltpu.make_async_copy(b, t, store_sem.at[n]) for n, (b, t) in enumerate(zip(bufs, targets))]
    order = list(range(2, count)) + [0, 1]
    for n in order:
        loads[n].start()
    for n in order:
        loads[n].wait()
        stores[n].start()
    for n in order:
        stores[n].wait()


def emit(grad_gu, *rest):
    shapes = [jax.ShapeDtypeStruct((LANES, FF), F32)] * 2 + [jax.ShapeDtypeStruct(t.shape, t.dtype) for t in rest]
    dma = pltpu.SemaphoreType.DMA
    return pl.pallas_call(
        emit_kernel,
        out_shape=tuple(shapes),
        in_specs=[pl.BlockSpec(memory_space=pl.ANY)] * (1 + len(rest)),
        out_specs=(pl.BlockSpec(memory_space=pl.ANY),) * len(shapes),
        scratch_shapes=[pltpu.VMEM(t.shape, t.dtype) for t in shapes] + [dma((len(shapes),)), dma((len(shapes),))],
        compiler_params=pltpu.CompilerParams(vmem_limit_bytes=60 * 1024 * 1024),
        cost_estimate=pl.CostEstimate(flops=1_000_000, bytes_accessed=15_000_000, transcendentals=0),
        name='emit',
    )(grad_gu, *rest)


def rms_back(grad_out, normed, inv_rms):
    mean_term = jnp.mean(grad_out * normed, axis=-1, keepdims=True)
    return inv_rms * (grad_out - normed * mean_term)


def solution(mesh):
    row_spec = P('sp', None)
    cube_spec = P('sp', None, None)
    vec_spec = P('sp')

    def gather(t):
        return lax.all_gather(t, 'sp', axis=0, tiled=True)

    same_core = [[0, 2, 4, 6], [1, 3, 5, 7]]

    def gather_same_core(t):
        full = lax.all_gather(t, 'sp', axis=0, tiled=True, axis_index_groups=same_core)
        return full.reshape((NDEV // 2,) + t.shape)

    def exchange(t):
        return lax.all_to_all(t, 'sp', 0, 0)

    def local_layer(x, seg_ids, positions, grad_y, norm1_gain, w_q, w_k, w_v, w_o, norm2_gain, w_gate, w_up, w_down):
        half = HD // 2
        inv_freq = (ROPE_BASE ** (-jnp.arange(half, dtype=F32) * 2.0 / HD))[:, None]
        freq = jnp.broadcast_to(inv_freq, (half, LANES))
        small = jnp.concatenate([norm1_gain.astype(F32)[None, :], norm2_gain.astype(F32)[None, :],
                                 positions.astype(F32).reshape(4, LANES), jnp.zeros((2, LANES), F32)])
        w_in = jnp.concatenate([t.transpose(1, 2, 0).reshape(NDEV, LANES, LANES) for t in (w_q, w_k, w_v)], axis=1)
        u_all, q, k, v, cos_t, sin_t, small, start2, wo_full = head_stage(
            x, w_in, small, freq, w_o.reshape(LANES, D))
        wo_full = wo_full.reshape(D, D)
        gain1 = small[:, 0].reshape(1, D)
        gain2 = small[:, 1].reshape(D)
        o_own, lse = attn_forward(start2, q, k, v)
        o_heads = exchange(o_own.reshape(NDEV, TOK, LANES))
        o_loc = o_heads.transpose(1, 0, 2).reshape(TOK, D)
        o_t = o_heads.transpose(0, 2, 1).reshape(D, TOK)

        wd_full = gather(w_down)
        wgu_half = gather_same_core(jnp.concatenate([w_gate, w_up], axis=1))
        win_half = gather_same_core(w_in.reshape(3 * D, LANES))

        x_wide = x.astype(F32)
        h_res = (x_wide + jnp.dot(o_loc, wo_full, preferred_element_type=F32)).astype(BF16)
        h_wide = h_res.astype(F32)
        inv_rms2 = lax.rsqrt(jnp.mean(h_wide * h_wide, axis=-1, keepdims=True) + NORM_EPS)
        normed2 = h_wide * inv_rms2
        z_norm = (normed2 * gain2).astype(BF16)
        grad_z_b, m_t, grad_wgu = mlp_stage(z_norm, grad_y, wd_full, wgu_half)
        grad_wgu = lax.psum_scatter(grad_wgu, 'sp', scatter_dimension=0, tiled=True, axis_index_groups=same_core)
        grad_z = grad_z_b.astype(F32)
        grad_h = (grad_y.astype(F32) + rms_back(grad_z * gain2, normed2, inv_rms2)).astype(BF16)
        grad_o = dot_nt(grad_h, wo_full).astype(BF16)
        grad_o = exchange(grad_o.reshape(TOK, NDEV, LANES).transpose(1, 0, 2)).reshape(SEQ, LANES)
        y = (h_wide + dot_tn(m_t, wd_full)).astype(BF16)

        d_qkv = attn_backward(start2, lse, q, k, v, o_own, grad_o, cos_t, sin_t)
        grad_wdown, grad_wo, *grad_qkv, grad_x, grad_gain1, grad_gain2 = tail_stage(
            m_t, grad_y, o_t, grad_h, d_qkv.reshape(NDEV, TOK, 3 * LANES), x, h_res, grad_z_b,
            gain1, u_all, win_half)
        grad_wgate, grad_wup, grad_wdown, grad_wo, *grad_qkv, grad_x, grad_gain1, grad_gain2 = emit(
            grad_wgu, grad_wdown, grad_wo, *grad_qkv, grad_x, grad_gain1, grad_gain2)
        grad_q, grad_k, grad_v = (t.reshape(16, HD, LANES).transpose(2, 0, 1) for t in grad_qkv)
        return (y, grad_x, grad_gain1.reshape(LANES), grad_q, grad_k, grad_v, grad_wo.reshape(2, HD, D),
                grad_gain2.reshape(LANES), grad_wgate, grad_wup, grad_wdown)

    return jax.shard_map(
        local_layer, mesh=mesh,
        in_specs=(row_spec, vec_spec, vec_spec, row_spec, vec_spec, cube_spec, cube_spec, cube_spec, cube_spec,
                  vec_spec, row_spec, row_spec, row_spec),
        out_specs=(row_spec, row_spec, vec_spec, cube_spec, cube_spec, cube_spec, cube_spec, vec_spec,
                   row_spec, row_spec, row_spec),
        check_vma=False)
```

```python
import jax
import jax.numpy as jnp
from jax import lax
from jax.experimental import pallas as pl
from jax.experimental.pallas import tpu as pltpu
from jax.sharding import PartitionSpec as P


NORM_EPS = 1e-5
ROPE_BASE = 10000.0
SEQ = 4096
D = 1024
HD = 64
FF = 2816
NDEV = 8
TOK = SEQ // NDEV
LANES = 128
BQ = 256
BK = 512
BK_BWD = 256
NQ = SEQ // BQ
NEG = -1e30
F32 = jnp.float32
BF16 = jnp.bfloat16


def dot_nt(a, b):
    return lax.dot_general(a, b, (((1,), (1,)), ((), ())), preferred_element_type=F32)


def dot_tn(a, b):
    return lax.dot_general(a, b, (((0,), (0,)), ((), ())), preferred_element_type=F32)


def head_pair(t):
    lane = lax.broadcasted_iota(jnp.int32, (1, LANES), 1)
    low = (lane < HD).astype(F32).astype(BF16)
    high = (lane >= HD).astype(F32).astype(BF16)
    return jnp.concatenate([t * low, t * high], axis=0)


def rope_back_tile(t, cos_t, sin_t):
    lane = lax.broadcasted_iota(jnp.int32, t.shape, 1)
    first_half = lax.rem(lane, HD) < HD // 2
    rotated = jnp.where(first_half, -pltpu.roll(t, LANES - HD // 2, 1), pltpu.roll(t, HD // 2, 1))
    return t * cos_t - rotated * sin_t


def attn_fwd_kernel(lo_ref, start_ref, q_ref, k_ref, v_ref, o_ref, lse_ref, acc_ref):
    q_iota = lax.rem(lax.broadcasted_iota(jnp.int32, (1, 2 * BQ), 1), BQ)

    def q_block(i, _):
        q_start = pl.multiple_of(i * BQ, BQ)
        q2 = head_pair(q_ref[pl.ds(q_start, BQ), :])
        first = start_ref[pl.ds(i, 1), :]
        q_index = q_start + q_iota
        acc_ref[...] = jnp.zeros_like(acc_ref)

        def k_block(j, carry):
            m_old, l_old = carry
            k_start = pl.multiple_of(j * BK, BK)
            k = k_ref[pl.ds(k_start, BK), :]
            v = v_ref[pl.ds(k_start, BK), :]
            s = dot_nt(k, q2)
            k_index = k_start + lax.broadcasted_iota(jnp.int32, s.shape, 0)
            s = jnp.where((k_index >= first) & (k_index <= q_index), s, NEG)
            m_new = jnp.maximum(m_old, jnp.max(s, axis=0, keepdims=True))
            p = jnp.exp(s - m_new)
            alpha = jnp.exp(m_old - m_new)
            l_new = alpha * l_old + jnp.sum(p, axis=0, keepdims=True)
            acc_ref[...] = acc_ref[...] * alpha + dot_tn(v, p.astype(BF16))
            return m_new, l_new

        init = (jnp.full((1, 2 * BQ), NEG, F32), jnp.zeros((1, 2 * BQ), F32))
        m_fin, l_fin = lax.fori_loop(lax.div(lo_ref[i, 0], BK), (q_start + BQ - 1) // BK + 1, k_block, init)
        lse_ref[pl.ds(i, 1), :] = m_fin + jnp.log(l_fin)
        out = acc_ref[...] * (1.0 / l_fin)
        out = jnp.concatenate([out[:HD, :BQ], out[HD:, BQ:]], axis=0)
        o_ref[pl.ds(q_start, BQ), :] = out.T.astype(BF16)
        return 0

    lax.fori_loop(0, NQ, q_block, 0)


def attn_bwd_kernel(lo_ref, start_ref, lse_ref, q_ref, k_ref, v_ref, o_ref, do_ref, cos_ref, sin_ref,
                    out_ref, dk_acc, dv_acc, dq_acc):
    q_iota = lax.rem(lax.broadcasted_iota(jnp.int32, (1, 2 * BQ), 1), BQ)
    dk_acc[...] = jnp.zeros_like(dk_acc)
    dv_acc[...] = jnp.zeros_like(dv_acc)

    def q_block(i, _):
        q_start = pl.multiple_of(i * BQ, BQ)
        q2 = head_pair(q_ref[pl.ds(q_start, BQ), :])
        do = do_ref[pl.ds(q_start, BQ), :]
        do2 = head_pair(do)
        prod = (do.astype(F32) * o_ref[pl.ds(q_start, BQ), :].astype(F32)).T
        delta = jnp.concatenate([jnp.sum(prod[:HD], axis=0, keepdims=True),
                                 jnp.sum(prod[HD:], axis=0, keepdims=True)], axis=1)
        first = start_ref[pl.ds(i, 1), :]
        lse = lse_ref[pl.ds(i, 1), :]
        q_index = q_start + q_iota
        dq_acc[...] = jnp.zeros_like(dq_acc)

        def k_block(j, _):
            k_start = pl.multiple_of(j * BK_BWD, BK_BWD)
            k = k_ref[pl.ds(k_start, BK_BWD), :]
            v = v_ref[pl.ds(k_start, BK_BWD), :]
            s = dot_nt(k, q2)
            k_index = k_start + lax.broadcasted_iota(jnp.int32, s.shape, 0)
            s = jnp.where((k_index >= first) & (k_index <= q_index), s, NEG)
            p = jnp.exp(s - lse)
            dp = dot_nt(v, do2).astype(BF16).astype(F32)
            ds = (p * (dp - delta)).astype(BF16)
            dv_acc[pl.ds(k_start, BK_BWD), :] += jnp.dot(p.astype(BF16), do2, preferred_element_type=F32)
            dk_acc[pl.ds(k_start, BK_BWD), :] += jnp.dot(ds, q2, preferred_element_type=F32)
            dq_acc[...] += dot_tn(k, ds)
            return 0

        lax.fori_loop(lax.div(lo_ref[i, 0], BK_BWD), (q_start + BQ - 1) // BK_BWD + 1, k_block, 0)
        dq = jnp.concatenate([dq_acc[:HD, :BQ], dq_acc[HD:, BQ:]], axis=0).T * (HD ** -0.5)
        rows = pl.ds(q_start, BQ)
        dq = dq.astype(BF16).astype(F32)
        out_ref[rows, 0:LANES] = rope_back_tile(dq, cos_ref[rows, :], sin_ref[rows, :]).astype(BF16)
        return 0

    lax.fori_loop(0, NQ, q_block, 0)

    def finish(i, _):
        rows = pl.ds(pl.multiple_of(i * BQ, BQ), BQ)
        dk = dk_acc[rows, :].astype(BF16).astype(F32)
        out_ref[rows, LANES:2 * LANES] = rope_back_tile(dk, cos_ref[rows, :], sin_ref[rows, :]).astype(BF16)
        out_ref[rows, 2 * LANES:3 * LANES] = dv_acc[rows, :].astype(BF16)
        return 0

    lax.fori_loop(0, NQ, finish, 0)


VMEM_SPEC = pl.BlockSpec(memory_space=pltpu.VMEM)
SMEM_SPEC = pl.BlockSpec(memory_space=pltpu.SMEM)


def attn_forward(start, q, k, v):
    return pl.pallas_call(
        attn_fwd_kernel,
        out_shape=(jax.ShapeDtypeStruct((SEQ, LANES), BF16), jax.ShapeDtypeStruct((NQ, 2 * BQ), F32)),
        in_specs=[SMEM_SPEC] + [VMEM_SPEC] * 4,
        out_specs=(VMEM_SPEC, VMEM_SPEC),
        scratch_shapes=[pltpu.VMEM((LANES, 2 * BQ), F32)],
        compiler_params=pltpu.CompilerParams(vmem_limit_bytes=40 * 1024 * 1024),
        cost_estimate=pl.CostEstimate(flops=20_000_000_000, bytes_accessed=5_000_000, transcendentals=20_000_000),
        name='attn_fwd',
    )(start, start, q, k, v)


def attn_backward(start, lse, q, k, v, o, do, cos_t, sin_t):
    return pl.pallas_call(
        attn_bwd_kernel,
        out_shape=jax.ShapeDtypeStruct((SEQ, 3 * LANES), BF16),
        in_specs=[SMEM_SPEC] + [VMEM_SPEC] * 9,
        out_specs=VMEM_SPEC,
        scratch_shapes=[pltpu.VMEM((SEQ, LANES), F32), pltpu.VMEM((SEQ, LANES), F32),
                        pltpu.VMEM((LANES, 2 * BQ), F32)],
        compiler_params=pltpu.CompilerParams(vmem_limit_bytes=48 * 1024 * 1024),
        cost_estimate=pl.CostEstimate(flops=50_000_000_000, bytes_accessed=12_000_000, transcendentals=20_000_000),
        name='attn_bwd',
    )(start, start, lse, q, k, v, o, do, cos_t, sin_t)


def head_kernel(x_ref, w_ref, small_ref, freq_ref, wo_ref, u_hbm, q_ref, k_ref, v_ref, cos_ref, sin_ref, all_small,
                start_ref, wo_out, x_buf, w_buf, w_ext, u_buf, small_send, small_recv, w_send, w_recv, x_send, x_recv,
                wo_send, wo_recv, u_sem):
    me = lax.axis_index('sp')
    core = lax.rem(me, 2)
    x_pos = lax.rem(me // 2, 2)
    y_pos = me // 4
    step_c, step_x, step_y = 1 - 2 * core, 2 - 4 * x_pos, 4 - 8 * y_pos
    mate, near_x, near_y, diag = me + step_c, me + step_x, me + step_y, me + step_x + step_y

    barrier = pltpu.get_barrier_semaphore()
    for n in range(1, NDEV):
        pl.semaphore_signal(barrier, inc=1, device_id=(lax.rem(me + n, NDEV),), device_id_type=pl.DeviceIdType.MESH)
    pl.semaphore_wait(barrier, NDEV - 1)

    def remote(src, dst, send_sem, recv_sem, dev):
        return pltpu.make_async_remote_copy(src_ref=src, dst_ref=dst, send_sem=send_sem, recv_sem=recv_sem,
                                            device_id=(dev,), device_id_type=pl.DeviceIdType.MESH)

    def half(ref, h):
        rows = ref.shape[0] // 2
        return ref.at[pl.ds(h * rows, rows), :]

    def x_copy(slot, src_dev, h, target, from_ref=None):
        source = half(x_buf.at[src_dev], h) if from_ref is None else half(from_ref, h)
        return remote(source, half(x_buf.at[src_dev], h), x_send.at[slot], x_recv.at[slot], target)

    def wo_copy(slot, src_dev, h, target, from_ref=None):
        source = half(wo_out.at[src_dev], h) if from_ref is None else half(from_ref, h)
        return remote(source, half(wo_out.at[src_dev], h), wo_send.at[slot], wo_recv.at[slot], target)

    def first_sends(copy, from_ref):
        return [copy(0, me, 0, near_x, from_ref), copy(3, me, 1, near_y, from_ref),
                copy(1, me, 1, near_x, from_ref), copy(2, me, 0, near_y, from_ref),
                copy(12, me, 0, mate, from_ref), copy(13, me, 1, mate, from_ref)]

    smalls = [remote(small_ref, all_small.at[me], small_send.at[n - 1], small_recv.at[n - 1], lax.rem(me + n, NDEV))
              for n in range(1, NDEV)]
    weights = [remote(w_ref.at[lax.rem(me + n, NDEV)], w_buf.at[me], w_send.at[n - 1], w_recv.at[n - 1],
                      lax.rem(me + n, NDEV)) for n in range(1, NDEV)]
    for c in smalls:
        c.start()
    for c in weights:
        c.start()
    own = first_sends(x_copy, x_ref)
    for c in own:
        c.start()

    all_small[me] = small_ref[...]
    w_buf[me] = w_ref[me]
    for c in smalls + weights:
        c.wait_recv()

    half_head = HD // 2
    for n in range(NDEV):
        cols = slice(n * LANES, (n + 1) * LANES)
        w_ext[0:3 * LANES, cols] = w_buf[n]
        for m in range(2):
            t = w_buf[n, m * LANES:(m + 1) * LANES, :].astype(F32)
            rot = jnp.concatenate([-t[half_head:HD], t[:half_head], -t[HD + half_head:], t[HD:HD + half_head]], axis=0)
            w_ext[(3 + m) * LANES:(4 + m) * LANES, cols] = rot.astype(BF16)
    gain1 = jnp.concatenate([all_small[n, 0:1, :] for n in range(NDEV)], axis=1)

    def process(order, src_ref, src_dev, h):
        def part(i, _):
            local = pl.ds(pl.multiple_of(h * (TOK // 2) + i * LANES, LANES), LANES)
            rows = pl.ds(pl.multiple_of(src_dev * TOK + h * (TOK // 2) + i * LANES, LANES), LANES)
            xv = src_ref[local, :].astype(F32)
            inv = lax.rsqrt(jnp.mean(xv * xv, axis=-1, keepdims=True) + NORM_EPS)
            u = (xv * inv * gain1).astype(BF16)
            u_buf[rows, :] = u
            proj = dot_nt(u, w_ext[...])
            angle = freq_ref[...] * all_small[src_dev, pl.ds(2 + 2 * h + i, 1), :]
            cos4, sin4 = jnp.cos(angle), jnp.sin(angle)
            cos_v = jnp.concatenate([cos4] * 4, axis=0).T
            sin_v = jnp.concatenate([sin4] * 4, axis=0).T
            cos_ref[rows, :] = cos_v
            sin_ref[rows, :] = sin_v
            q = (proj[:, :LANES] * cos_v + proj[:, 3 * LANES:4 * LANES] * sin_v).astype(BF16).astype(F32)
            q_ref[rows, :] = (q * (HD ** -0.5)).astype(BF16)
            k_ref[rows, :] = (proj[:, LANES:2 * LANES] * cos_v + proj[:, 4 * LANES:] * sin_v).astype(BF16)
            v_ref[rows, :] = proj[:, 2 * LANES:3 * LANES].astype(BF16)
            return 0

        lax.fori_loop(0, 2, part, 0)
        u_rows = pl.ds(pl.multiple_of(src_dev * TOK + h * (TOK // 2), TOK // 2), TOK // 2)
        out = pltpu.make_async_copy(u_buf.at[u_rows, :], u_hbm.at[u_rows, :], u_sem.at[order])
        out.start()
        return out

    pending = []
    copies = list(own)

    def arrive(copy, slot, src_dev, h):
        copy(slot, src_dev, h, mate).wait_recv()

    def pass_on(copy, slot, src_dev, h, target):
        c = copy(slot, src_dev, h, target)
        c.start()
        copies.append(c)

    def relay(copy, slot, src_dev, h):
        arrive(copy, slot, src_dev, h)
        if slot == 0:
            pass_on(copy, 4, src_dev, h, near_y)
        elif slot == 3:
            pass_on(copy, 5, src_dev, h, near_x)
        pass_on(copy, 6 + slot, src_dev, h, mate)

    def work(src_ref, src_dev, h):
        pending.append(process(len(pending), src_ref, src_dev, h))

    work(x_ref, me, 0)
    work(x_ref, me, 1)
    arrivals = [(0, near_x, 0), (3, near_y, 1), (1, near_x, 1), (2, near_y, 0), (4, diag, 0), (5, diag, 1)]
    late = [(12, mate, 0), (13, mate, 1)]
    for n, (slot, src_dev, h) in enumerate(arrivals):
        relay(x_copy, slot, src_dev, h)
        if n == 1:
            wo_own = first_sends(wo_copy, wo_ref)
            for c in wo_own:
                c.start()
            copies += wo_own
            wo_out[me] = wo_ref[...]
        if n >= 4:
            relay(wo_copy, *arrivals[n - 4])
        work(x_buf.at[src_dev], src_dev, h)
        mate_slot, mate_src, mate_h = late.pop(0)
        arrive(x_copy, mate_slot, mate_src, mate_h)
        work(x_buf.at[mate_src], mate_src, mate_h)
        late.append((6 + slot, src_dev + step_c, h))
    for n, (slot, src_dev, h) in enumerate(late):
        if n < 2:
            relay(wo_copy, *arrivals[n + 2])
        arrive(x_copy, slot, src_dev, h)
        work(x_buf.at[src_dev], src_dev, h)
    for n in range(NDEV):
        for h in range(2):
            row = jnp.concatenate([all_small[n, 2 + 2 * h:3 + 2 * h, :], all_small[n, 3 + 2 * h:4 + 2 * h, :]], axis=1)
            index = n * TOK + h * BQ + lax.broadcasted_iota(jnp.int32, (1, BQ), 1)
            first = index - row.astype(jnp.int32)
            start_ref[2 * n + h:2 * n + h + 1, :] = jnp.concatenate([first, first], axis=1)
    relay(wo_copy, *arrivals[4])
    relay(wo_copy, *arrivals[5])
    for slot, src_dev, h in [(12, mate, 0), (13, mate, 1)] + [(6 + m, d + step_c, h) for m, d, h in arrivals]:
        arrive(wo_copy, slot, src_dev, h)
    for c in pending:
        c.wait()
    for c in smalls + weights + copies:
        c.wait_send()


def head_stage(x, w_pieces, small, freq, w_o):
    dma = pltpu.SemaphoreType.DMA
    return pl.pallas_call(
        head_kernel,
        out_shape=(jax.ShapeDtypeStruct((SEQ, D), BF16),) + tuple(jax.ShapeDtypeStruct((SEQ, LANES), BF16) for _ in range(3))
        + tuple(jax.ShapeDtypeStruct((SEQ, LANES), F32) for _ in range(2))
        + (jax.ShapeDtypeStruct((NDEV, 8, LANES), F32), jax.ShapeDtypeStruct((NQ, 2 * BQ), jnp.int32),
           jax.ShapeDtypeStruct((NDEV, LANES, D), BF16)),
        in_specs=[VMEM_SPEC] * 5,
        out_specs=(pl.BlockSpec(memory_space=pl.ANY),) + (VMEM_SPEC,) * 8,
        scratch_shapes=[pltpu.VMEM((NDEV, TOK, D), BF16), pltpu.VMEM((NDEV, 3 * LANES, LANES), BF16),
                        pltpu.VMEM((5 * LANES, D), BF16), pltpu.VMEM((SEQ, D), BF16),
                        dma((NDEV - 1,)), dma((NDEV - 1,)), dma((NDEV - 1,)), dma((NDEV - 1,)),
                        dma((14,)), dma((14,)), dma((14,)), dma((14,)), dma((16,))],
        compiler_params=pltpu.CompilerParams(collective_id=0, has_side_effects=True,
                                             vmem_limit_bytes=48 * 1024 * 1024),
        cost_estimate=pl.CostEstimate(flops=40_000_000_000, bytes_accessed=30_000_000, transcendentals=1_000_000),
        name='head_stage',
    )(x, w_pieces, small, freq, w_o)


COLS = D // 2
DN_ROWS = FF // NDEV
OUT_ROWS = DN_ROWS + LANES


def tail_kernel(mt_ref, gy_ref, ot_ref, gh_ref, d_ref, x_ref, h_ref, gz_ref, gain_ref, u_hbm, win_hbm,
                dn_out, wo_out, gq_out, gk_out, gv_out, gx_out, gain1_out, gain2_out,
                mt_mate, gy_mate, ot_mate, gh_mate, part, box, d_buf, win_buf, u_buf, gw_acc, gw_in, gain_mine, gain_buf,
                mate_send, mate_recv, rs_send, rs_recv, d_send, d_recv, gw_send, gw_recv, gg_send, gg_recv, win_send, win_recv, win_sem, u_sem):
    me = lax.axis_index('sp')
    core = lax.rem(me, 2)
    x_pos = lax.rem(me // 2, 2)
    y_pos = me // 4
    step_c, step_x, step_y = 1 - 2 * core, 2 - 4 * x_pos, 4 - 8 * y_pos
    mate, near_x, near_y, diag = me + step_c, me + step_x, me + step_y, me + step_x + step_y

    def win_part(q):
        return win_buf.at[:, pl.ds(pl.multiple_of((2 * q + core) * LANES, LANES), LANES)]

    win_copies = [pltpu.make_async_copy(win_hbm.at[q], win_part(q), win_sem.at[q]) for q in range(NDEV // 2)]
    for c in win_copies:
        c.start()
    u_copy = pltpu.make_async_copy(u_hbm, u_buf, u_sem)
    u_copy.start()

    barrier = pltpu.get_barrier_semaphore()
    for n in range(1, NDEV):
        pl.semaphore_signal(barrier, inc=1, device_id=(lax.rem(me + n, NDEV),), device_id_type=pl.DeviceIdType.MESH)
    pl.semaphore_wait(barrier, NDEV - 1)

    def remote(src, dst, send_sem, recv_sem, dev):
        return pltpu.make_async_remote_copy(src_ref=src, dst_ref=dst, send_sem=send_sem, recv_sem=recv_sem,
                                            device_id=(dev,), device_id_type=pl.DeviceIdType.MESH)

    def to_peers(src, dst, send_sem, recv_sem):
        return [remote(src.at[lax.rem(me + n, NDEV)], dst.at[me], send_sem.at[n - 1], recv_sem.at[n - 1],
                       lax.rem(me + n, NDEV)) for n in range(1, NDEV)]

    def dn_rows(dev):
        return pl.ds(pl.multiple_of(dev * DN_ROWS, 32), DN_ROWS)

    def wo_rows(dev):
        return pl.ds(pl.multiple_of(dev * LANES, LANES), LANES)

    swaps = []
    for q in range(NDEV // 2):
        dest = 2 * q + 1 - core
        swaps.append(remote(mt_ref.at[dn_rows(dest), :], mt_mate.at[q], mate_send.at[q], mate_recv.at[q], mate))
        swaps.append(remote(ot_ref.at[wo_rows(dest), :], ot_mate.at[q], mate_send.at[4 + q], mate_recv.at[4 + q], mate))
    swaps.append(remote(gy_ref, gy_mate, mate_send.at[8], mate_recv.at[8], mate))
    swaps.append(remote(gh_ref, gh_mate, mate_send.at[9], mate_recv.at[9], mate))
    for c in swaps:
        c.start()
    d_moves = to_peers(d_ref, d_buf, d_send, d_recv)

    def gw_cols(dev):
        return gw_acc.at[:, pl.ds(pl.multiple_of(dev * LANES, LANES), LANES)]

    gw_moves = [remote(gw_cols(lax.rem(me + n, NDEV)), gw_in.at[me], gw_send.at[n - 1], gw_recv.at[n - 1],
                       lax.rem(me + n, NDEV)) for n in range(1, NDEV)]
    gg_moves = to_peers(gain_mine, gain_buf, gg_send, gg_recv)
    for c in d_moves:
        c.start()
    win_swaps = [remote(win_hbm.at[q], win_part(q), win_send.at[q], win_recv.at[q], mate) for q in range(NDEV // 2)]
    for c in win_swaps:
        c.start()
    d_buf[me] = d_ref[me]
    for c in swaps:
        c.wait_recv()

    def compute(rel, dev, col):
        chip = dev // 2
        cols = pl.ds(col * COLS, COLS)
        part[rel, col, 0:DN_ROWS, :] = (
            jnp.dot(mt_ref[dn_rows(dev), :], gy_ref[:, cols], preferred_element_type=F32)
            + jnp.dot(mt_mate[chip], gy_mate[:, cols], preferred_element_type=F32))
        part[rel, col, DN_ROWS:OUT_ROWS, :] = (
            jnp.dot(ot_ref[wo_rows(dev), :], gh_ref[:, cols], preferred_element_type=F32)
            + jnp.dot(ot_mate[chip], gh_mate[:, cols], preferred_element_type=F32))

    moves = [remote(part.at[3, 0], box.at[0], rs_send.at[0], rs_recv.at[0], near_x),
             remote(part.at[3, 1], box.at[1], rs_send.at[1], rs_recv.at[1], near_y),
             remote(part.at[1, 0], box.at[2], rs_send.at[2], rs_recv.at[2], near_x),
             remote(part.at[2, 1], box.at[3], rs_send.at[3], rs_recv.at[3], near_y),
             remote(part.at[2, 0], box.at[4], rs_send.at[4], rs_recv.at[4], near_y),
             remote(part.at[1, 1], box.at[5], rs_send.at[5], rs_recv.at[5], near_x)]
    compute(3, diag, 0)
    moves[0].start()
    compute(3, diag, 1)
    moves[1].start()
    compute(1, near_x, 0)
    moves[2].start()
    compute(2, near_y, 1)
    moves[3].start()
    compute(2, near_y, 0)
    compute(1, near_x, 1)
    u_copy.wait()

    gw_acc[...] = dot_tn(d_ref[0], u_buf[0:TOK, :])

    def grad_win_part(g, _):
        gw_acc[...] += dot_tn(d_ref[g], u_buf[pl.ds(pl.multiple_of(g * TOK, TOK), TOK), :])
        return 0

    lax.fori_loop(1, NDEV, grad_win_part, 0)
    for c in gw_moves:
        c.start()
    gw_in[me] = gw_acc[:, pl.ds(pl.multiple_of(me * LANES, LANES), LANES)]
    compute(0, me, 0)
    compute(0, me, 1)

    def add_box(rel, col, n):
        def rows_add(i, _):
            rows = pl.ds(pl.multiple_of(i * 32, 32), 32)
            part[rel, col, rows, :] += box[n, rows, :]
            return 0

        lax.fori_loop(0, OUT_ROWS // 32, rows_add, 0)

    moves[0].wait_recv()
    add_box(2, 0, 0)
    moves[4].start()
    moves[1].wait_recv()
    add_box(1, 1, 1)
    moves[5].start()

    for c in d_moves:
        c.wait_recv()
    for c in win_copies:
        c.wait()
    for c in win_swaps:
        c.wait_recv()
    gain1 = gain_ref[...]

    def grad_rows(i, carry):
        acc, acc2 = carry
        rows = pl.ds(pl.multiple_of(i * LANES, LANES), LANES)
        gu = jnp.dot(d_buf[0, rows, :], win_buf[0:3 * LANES, :], preferred_element_type=F32)
        for g in range(1, NDEV):
            gu = gu + jnp.dot(d_buf[g, rows, :], win_buf[g * 3 * LANES:(g + 1) * 3 * LANES, :],
                              preferred_element_type=F32)
        gu = gu.astype(BF16).astype(F32)
        xv = x_ref[rows, :].astype(F32)
        inv = lax.rsqrt(jnp.mean(xv * xv, axis=-1, keepdims=True) + NORM_EPS)
        normed = xv * inv
        acc = acc + jnp.sum(gu * normed, axis=0, keepdims=True)
        scaled = gu * gain1
        mean_term = jnp.mean(scaled * normed, axis=-1, keepdims=True)
        gx_out[rows, :] = (gh_ref[rows, :].astype(F32) + inv * (scaled - normed * mean_term)).astype(BF16)
        hv = h_ref[rows, :].astype(F32)
        normed2 = hv * lax.rsqrt(jnp.mean(hv * hv, axis=-1, keepdims=True) + NORM_EPS)
        acc2 = acc2 + jnp.sum(gz_ref[rows, :].astype(F32) * normed2, axis=0, keepdims=True)
        return acc, acc2

    gg1, gg2 = lax.fori_loop(0, TOK // LANES, grad_rows, (jnp.zeros((1, D), F32), jnp.zeros((1, D), F32)))
    for n in range(NDEV):
        piece = slice(n * LANES, (n + 1) * LANES)
        gain_mine[n] = jnp.concatenate([gg1[:, piece], gg2[:, piece], jnp.zeros((6, LANES), F32)], axis=0)
    for c in gg_moves:
        c.start()
    gain_buf[me] = gain_mine[me]

    moves[2].wait_recv()
    add_box(0, 0, 2)
    moves[3].wait_recv()
    add_box(0, 1, 3)
    for c in gg_moves:
        c.wait_recv()
    total = gain_buf[0]
    for n in range(1, NDEV):
        total = total + gain_buf[n]
    gain1_out[...] = total[0:1]
    gain2_out[...] = total[1:2]
    for col in range(2):
        moves[4 + col].wait_recv()

        def finish(i, _):
            rows = pl.ds(pl.multiple_of(i * 32, 32), 32)
            dn_out[rows, col * COLS:(col + 1) * COLS] = part[0, col, rows, :] + box[4 + col, rows, :]
            return 0

        lax.fori_loop(0, DN_ROWS // 32, finish, 0)
        wo_out[:, col * COLS:(col + 1) * COLS] = part[0, col, DN_ROWS:OUT_ROWS, :] + box[4 + col, DN_ROWS:OUT_ROWS, :]
    for c in gw_moves:
        c.wait_recv()
    for n, ref in enumerate((gq_out, gk_out, gv_out)):
        ref[...] = gw_in[:, n * LANES:(n + 1) * LANES, :]
    for c in swaps + d_moves + gw_moves + gg_moves + moves + win_swaps:
        c.wait_send()


def tail_stage(m_t, grad_y, o_t, grad_h, d_qkv, x, h_res, grad_z, gain1, u_all, win_full):
    dma = pltpu.SemaphoreType.DMA
    peers = (NDEV - 1,)
    return pl.pallas_call(
        tail_kernel,
        out_shape=(jax.ShapeDtypeStruct((DN_ROWS, D), F32), jax.ShapeDtypeStruct((LANES, D), F32),
                   *(jax.ShapeDtypeStruct((NDEV, LANES, LANES), F32),) * 3, jax.ShapeDtypeStruct((TOK, D), BF16),
                   *(jax.ShapeDtypeStruct((1, LANES), F32),) * 2),
        in_specs=[VMEM_SPEC] * 9 + [pl.BlockSpec(memory_space=pltpu.HBM)] * 2,
        out_specs=(VMEM_SPEC,) * 8,
        scratch_shapes=[pltpu.VMEM((4, DN_ROWS, TOK), BF16), pltpu.VMEM((TOK, D), BF16),
                        pltpu.VMEM((4, LANES, TOK), BF16), pltpu.VMEM((TOK, D), BF16),
                        pltpu.VMEM((4, 2, OUT_ROWS, COLS), F32), pltpu.VMEM((6, OUT_ROWS, COLS), F32),
                        pltpu.VMEM((NDEV, TOK, 3 * LANES), BF16), pltpu.VMEM((3 * D, D), BF16), pltpu.VMEM((SEQ, D), BF16),
                        pltpu.VMEM((3 * LANES, D), F32), pltpu.VMEM((NDEV, 3 * LANES, LANES), F32),
                        pltpu.VMEM((NDEV, 8, LANES), F32), pltpu.VMEM((NDEV, 8, LANES), F32),
                        dma((10,)), dma((10,)), dma((6,)), dma((6,)), dma(peers), dma(peers),
                        dma(peers), dma(peers), dma(peers), dma(peers), dma((4,)), dma((4,)), dma((4,)), dma],
        compiler_params=pltpu.CompilerParams(collective_id=1, has_side_effects=True,
                                             vmem_limit_bytes=60 * 1024 * 1024),
        cost_estimate=pl.CostEstimate(flops=60_000_000_000, bytes_accessed=60_000_000, transcendentals=1_000),
        name='tail_stage',
    )(m_t, grad_y, o_t, grad_h, d_qkv, x, h_res, grad_z, gain1, u_all, win_full)


UP_COLS = 256
DW_COLS = 512
DZ_COLS = 1408
SLOTS = 4


def mlp_kernel(z_ref, gy_ref, wd_hbm, w_hbm, gz_out, mt_out, gw_hbm,
               w_buf, wd_buf, g_buf, g_mate, z_mate, zt, acc, gz_acc,
               swap_send, swap_recv, load_sem, wd_sem, z_send, z_recv, g_send, g_recv, out_sem):
    me = lax.axis_index('sp')
    core = lax.rem(me, 2)
    mate = me + 1 - 2 * core
    blocks = FF // UP_COLS
    barrier = pltpu.get_barrier_semaphore()
    pl.semaphore_signal(barrier, inc=1, device_id=(mate,), device_id_type=pl.DeviceIdType.MESH)
    pl.semaphore_wait(barrier, 1)

    def to_mate(src, dst, send_sem, recv_sem):
        return pltpu.make_async_remote_copy(src_ref=src, dst_ref=dst, send_sem=send_sem, recv_sem=recv_sem,
                                            device_id=(mate,), device_id_type=pl.DeviceIdType.MESH)

    def cols(n, width):
        return pl.ds(pl.multiple_of(n * width, LANES), width)

    def w_swap(n):
        return to_mate(w_hbm.at[:, :, cols(n, UP_COLS)], w_buf.at[:, core, :, cols(n, UP_COLS)],
                       swap_send.at[n], swap_recv.at[n])

    def w_load(n):
        return pltpu.make_async_copy(w_hbm.at[:, :, cols(n, UP_COLS)], w_buf.at[:, core, :, cols(n, UP_COLS)],
                                     load_sem.at[n])

    def wd_load(b):
        return pltpu.make_async_copy(wd_hbm.at[cols(b, UP_COLS), :], wd_buf.at[cols(b, UP_COLS), :], wd_sem.at[b])

    def g_swap(n):
        return to_mate(g_buf.at[:, cols(n, UP_COLS)], g_mate.at[:, cols(n, UP_COLS)], g_send.at[n], g_recv.at[n])

    def out_copy(n):
        slot = lax.rem(n, SLOTS)
        return pltpu.make_async_copy(acc.at[slot], gw_hbm.at[:, cols(n, DW_COLS)], out_sem.at[slot])

    def start(b, _):
        for n in (b, b + blocks):
            w_swap(n).start()
            w_load(n).start()
        wd_load(b).start()
        return 0

    lax.fori_loop(0, blocks, start, 0)
    z_swap = to_mate(z_ref, z_mate, z_send, z_recv)
    z_swap.start()

    def dest_cols(q):
        return pl.ds(pl.multiple_of((2 * q + core) * LANES, LANES), LANES)

    for q in range(NDEV // 2):
        zt[q * LANES:(q + 1) * LANES, 0:TOK] = z_ref[:, dest_cols(q)].T

    def up_block(b, _):
        for n in (b, b + blocks):
            w_load(n).wait()
            w_swap(n).wait_recv()
        wd_load(b).wait()
        rows = cols(b, UP_COLS)
        low, high = cols(b, UP_COLS), cols(b + blocks, UP_COLS)
        z = z_ref[...]
        gate = jnp.dot(z, w_buf[:, :, :, low].reshape(D, UP_COLS), preferred_element_type=F32)
        up = jnp.dot(z, w_buf[:, :, :, high].reshape(D, UP_COLS), preferred_element_type=F32)
        g_act = dot_nt(gy_ref[...], wd_buf[rows, :]).astype(BF16).astype(F32)
        sig = jax.nn.sigmoid(gate)
        act = gate * sig
        mt_out[rows, :] = (act * up).T.astype(BF16)
        g_buf[:, low] = (g_act * up * sig * (1.0 + gate * (1.0 - sig))).astype(BF16)
        g_buf[:, high] = (g_act * act).astype(BF16)
        g_swap(b).start()
        g_swap(b + blocks).start()
        return 0

    lax.fori_loop(0, blocks, up_block, 0)
    z_swap.wait_recv()
    for q in range(NDEV // 2):
        zt[q * LANES:(q + 1) * LANES, TOK:2 * TOK] = z_mate[:, dest_cols(q)].T

    def grad_block(n, _):
        @pl.when(n >= SLOTS)
        def _():
            out_copy(n - SLOTS).wait()

        g_swap(2 * n).wait_recv()
        g_swap(2 * n + 1).wait_recv()
        block = cols(n, DW_COLS)
        acc[lax.rem(n, SLOTS)] = (jnp.dot(zt[:, 0:TOK], g_buf[:, block], preferred_element_type=F32)
                                  + jnp.dot(zt[:, TOK:2 * TOK], g_mate[:, block], preferred_element_type=F32))
        out_copy(n).start()
        return 0

    lax.fori_loop(0, blocks, grad_block, 0)
    gz_acc[...] = jnp.zeros_like(gz_acc)

    def gz_block(n, _):
        block = cols(n, DZ_COLS)
        gz_acc[...] += dot_nt(g_buf[:, block], w_buf[:, :, :, block].reshape(D, DZ_COLS))
        return 0

    lax.fori_loop(0, 2 * FF // DZ_COLS, gz_block, 0)
    gz_out[...] = gz_acc[...].astype(BF16)
    for n in range(blocks - SLOTS, blocks):
        out_copy(n).wait()

    def finish(n, _):
        w_swap(n).wait_send()
        g_swap(n).wait_send()
        return 0

    lax.fori_loop(0, 2 * blocks, finish, 0)
    z_swap.wait_send()


def mlp_stage(z, grad_y, wd_full, w_half):
    dma = pltpu.SemaphoreType.DMA
    count = 2 * FF // UP_COLS
    hbm = pl.BlockSpec(memory_space=pltpu.HBM)
    return pl.pallas_call(
        mlp_kernel,
        out_shape=(jax.ShapeDtypeStruct((TOK, D), BF16), jax.ShapeDtypeStruct((FF, TOK), BF16),
                   jax.ShapeDtypeStruct((D // 2, 2 * FF), F32)),
        in_specs=[VMEM_SPEC] * 2 + [hbm] * 2,
        out_specs=(VMEM_SPEC, VMEM_SPEC, hbm),
        scratch_shapes=[pltpu.VMEM((NDEV // 2, 2, LANES, 2 * FF), BF16), pltpu.VMEM((FF, D), BF16),
                        pltpu.VMEM((TOK, 2 * FF), BF16), pltpu.VMEM((TOK, 2 * FF), BF16), pltpu.VMEM((TOK, D), BF16),
                        pltpu.VMEM((D // 2, 2 * TOK), BF16), pltpu.VMEM((SLOTS, D // 2, DW_COLS), F32),
                        pltpu.VMEM((TOK, D), F32),
                        dma((count,)), dma((count,)), dma((count,)), dma((count // 2,)), dma, dma,
                        dma((count,)), dma((count,)), dma((SLOTS,))],
        compiler_params=pltpu.CompilerParams(collective_id=3, has_side_effects=True,
                                             vmem_limit_bytes=58 * 1024 * 1024),
        cost_estimate=pl.CostEstimate(flops=21_000_000_000, bytes_accessed=40_000_000, transcendentals=1_500_000),
        name='mlp_stage',
    )(z, grad_y, wd_full, w_half)


def emit_kernel(*refs):
    count = (len(refs) - 1) // 3
    sources, targets, bufs = refs[:count - 1], refs[count - 1:2 * count - 1], refs[2 * count - 1:3 * count - 1]
    load_sem, store_sem = refs[-2:]
    gu = sources[0]
    views = [gu.at[:, 0:FF], gu.at[:, FF:2 * FF]] + list(sources[1:])
    loads = [pltpu.make_async_copy(v, b, load_sem.at[n]) for n, (v, b) in enumerate(zip(views, bufs))]
    stores = [pltpu.make_async_copy(b, t, store_sem.at[n]) for n, (b, t) in enumerate(zip(bufs, targets))]
    order = list(range(2, count)) + [0, 1]
    for n in order:
        loads[n].start()
    for n in order:
        loads[n].wait()
        stores[n].start()
    for n in order:
        stores[n].wait()


def emit(grad_gu, *rest):
    shapes = [jax.ShapeDtypeStruct((LANES, FF), F32)] * 2 + [jax.ShapeDtypeStruct(t.shape, t.dtype) for t in rest]
    dma = pltpu.SemaphoreType.DMA
    return pl.pallas_call(
        emit_kernel,
        out_shape=tuple(shapes),
        in_specs=[pl.BlockSpec(memory_space=pl.ANY)] * (1 + len(rest)),
        out_specs=(pl.BlockSpec(memory_space=pl.ANY),) * len(shapes),
        scratch_shapes=[pltpu.VMEM(t.shape, t.dtype) for t in shapes] + [dma((len(shapes),)), dma((len(shapes),))],
        compiler_params=pltpu.CompilerParams(vmem_limit_bytes=60 * 1024 * 1024),
        cost_estimate=pl.CostEstimate(flops=1_000_000, bytes_accessed=15_000_000, transcendentals=0),
        name='emit',
    )(grad_gu, *rest)


def rms_back(grad_out, normed, inv_rms):
    mean_term = jnp.mean(grad_out * normed, axis=-1, keepdims=True)
    return inv_rms * (grad_out - normed * mean_term)


def solution(mesh):
    row_spec = P('sp', None)
    cube_spec = P('sp', None, None)
    vec_spec = P('sp')

    def gather(t):
        return lax.all_gather(t, 'sp', axis=0, tiled=True)

    same_core = [[0, 2, 4, 6], [1, 3, 5, 7]]

    def gather_same_core(t):
        full = lax.all_gather(t, 'sp', axis=0, tiled=True, axis_index_groups=same_core)
        return full.reshape((NDEV // 2,) + t.shape)

    def exchange(t):
        return lax.all_to_all(t, 'sp', 0, 0)

    def local_layer(x, seg_ids, positions, grad_y, norm1_gain, w_q, w_k, w_v, w_o, norm2_gain, w_gate, w_up, w_down):
        half = HD // 2
        inv_freq = (ROPE_BASE ** (-jnp.arange(half, dtype=F32) * 2.0 / HD))[:, None]
        freq = jnp.broadcast_to(inv_freq, (half, LANES))
        small = jnp.concatenate([norm1_gain.astype(F32)[None, :], norm2_gain.astype(F32)[None, :],
                                 positions.astype(F32).reshape(4, LANES), jnp.zeros((2, LANES), F32)])
        w_in = jnp.concatenate([t.transpose(1, 2, 0).reshape(NDEV, LANES, LANES) for t in (w_q, w_k, w_v)], axis=1)
        u_all, q, k, v, cos_t, sin_t, small, start2, wo_full = head_stage(
            x, w_in, small, freq, w_o.reshape(LANES, D))
        wo_full = wo_full.reshape(D, D)
        gain1 = small[:, 0].reshape(1, D)
        gain2 = small[:, 1].reshape(D)
        o_own, lse = attn_forward(start2, q, k, v)
        o_heads = exchange(o_own.reshape(NDEV, TOK, LANES))
        o_loc = o_heads.transpose(1, 0, 2).reshape(TOK, D)
        o_t = o_heads.transpose(0, 2, 1).reshape(D, TOK)

        wd_full = gather(w_down)
        wgu_half = gather_same_core(jnp.concatenate([w_gate, w_up], axis=1))
        win_half = gather_same_core(w_in.reshape(3 * D, LANES))

        x_wide = x.astype(F32)
        h_res = (x_wide + jnp.dot(o_loc, wo_full, preferred_element_type=F32)).astype(BF16)
        h_wide = h_res.astype(F32)
        inv_rms2 = lax.rsqrt(jnp.mean(h_wide * h_wide, axis=-1, keepdims=True) + NORM_EPS)
        normed2 = h_wide * inv_rms2
        z_norm = (normed2 * gain2).astype(BF16)
        grad_z_b, m_t, grad_wgu = mlp_stage(z_norm, grad_y, wd_full, wgu_half)
        grad_wgu = lax.psum_scatter(grad_wgu, 'sp', scatter_dimension=0, tiled=True, axis_index_groups=same_core)
        grad_z = grad_z_b.astype(F32)
        grad_h = (grad_y.astype(F32) + rms_back(grad_z * gain2, normed2, inv_rms2)).astype(BF16)
        grad_o = dot_nt(grad_h, wo_full).astype(BF16)
        grad_o = exchange(grad_o.reshape(TOK, NDEV, LANES).transpose(1, 0, 2)).reshape(SEQ, LANES)
        y = (h_wide + dot_tn(m_t, wd_full)).astype(BF16)

        d_qkv = attn_backward(start2, lse, q, k, v, o_own, grad_o, cos_t, sin_t)
        grad_wdown, grad_wo, *grad_qkv, grad_x, grad_gain1, grad_gain2 = tail_stage(
            m_t, grad_y, o_t, grad_h, d_qkv.reshape(NDEV, TOK, 3 * LANES), x, h_res, grad_z_b,
            gain1, u_all, win_half)
        grad_wgate, grad_wup, grad_wdown, grad_wo, *grad_qkv, grad_x, grad_gain1, grad_gain2 = emit(
            grad_wgu, grad_wdown, grad_wo, *grad_qkv, grad_x, grad_gain1, grad_gain2)
        grad_q, grad_k, grad_v = (t.reshape(16, HD, LANES).transpose(2, 0, 1) for t in grad_qkv)
        return (y, grad_x, grad_gain1.reshape(LANES), grad_q, grad_k, grad_v, grad_wo.reshape(2, HD, D),
                grad_gain2.reshape(LANES), grad_wgate, grad_wup, grad_wdown)

    return jax.shard_map(
        local_layer, mesh=mesh,
        in_specs=(row_spec, vec_spec, vec_spec, row_spec, vec_spec, cube_spec, cube_spec, cube_spec, cube_spec,
                  vec_spec, row_spec, row_spec, row_spec),
        out_specs=(row_spec, row_spec, vec_spec, cube_spec, cube_spec, cube_spec, cube_spec, vec_spec,
                   row_spec, row_spec, row_spec),
        check_vma=False)
```
